16 devices in a mesh: dp: 1, tp: 16 (over x, y, z, core).
Axes of the slice: x: 2, y: 2, z: 2, core: 2. Of those that a mesh axis runs over, the one named last changes fastest.
Arguments:
- x: bfloat16 [2048, 8192], P(('dp', 'tp'))
- dy: bfloat16 [2048, 8192], P(('dp', 'tp'))
- pre: bfloat16 [2048, 32768], P('dp', 'tp')
- w_in: bfloat16 [8192, 32768], P(None, 'tp')
- w_down: bfloat16 [32768, 8192], P('tp')
Outputs:
- output 1: bfloat16 [2048, 8192], P(('dp', 'tp'))
- output 2: bfloat16 [8192, 32768], P('dp', 'tp')
- output 3: bfloat16 [32768, 8192], P(('dp', 'tp'))
All inputs are finite; a program needn't handle non-finite values.
Results may differ from the reference program's by a relative error of at most 0.012.
Values are sent between devices in bfloat16 or wider.
A program may use at most 2 GiB of HBM per device.

```python
import jax
import jax.numpy as jnp

ROWS = 2048
D = 8192
FF = 32768


def act(pre):
    return jax.nn.gelu(pre)


def setup_inputs(seed: int = 0, part: int = 0) -> dict:
    kx, ky, ka, ki, kd = jax.random.split(jax.random.key(seed), 5)
    kx, ky, ka = (jax.random.fold_in(k, part) for k in (kx, ky, ka))
    drawn = {
        "x": jax.random.normal(kx, (ROWS, D), jnp.float32),
        "dy": jax.random.normal(ky, (ROWS, D), jnp.float32),
        "pre": jax.random.normal(ka, (ROWS, FF), jnp.float32),
        "w_in": jax.random.normal(ki, (D, FF), jnp.float32) * D**-0.5,
        "w_down": jax.random.normal(kd, (FF, D), jnp.float32) * FF**-0.5,
    }
    return {k: v.astype(jnp.bfloat16) for k, v in drawn.items()}


def reference(x, dy, pre, w_in, w_down):
    hidden, back = jax.vjp(act, pre.astype(jnp.float32))
    d_hidden = jnp.dot(dy, w_down.T, preferred_element_type=jnp.float32)
    d_pre = back(d_hidden)[0].astype(jnp.bfloat16)
    dx = jnp.dot(d_pre, w_in.T, preferred_element_type=jnp.float32)
    dw_in = jnp.dot(x.T, d_pre, preferred_element_type=jnp.float32)
    dw_down = jnp.dot(hidden.astype(jnp.bfloat16).T, dy, preferred_element_type=jnp.float32)
    return tuple(g.astype(jnp.bfloat16) for g in (dx, dw_in, dw_down))
```

```python
import functools

import jax
import jax.numpy as jnp
from jax import lax
from jax.experimental import pallas as pl
from jax.experimental.pallas import tpu as pltpu
from jax.sharding import PartitionSpec as P

VMEM_LIMIT = 60 * 1024 * 1024


def act(pre):
    return jax.nn.gelu(pre)


def params(*semantics):
    return pltpu.CompilerParams(dimension_semantics=semantics, vmem_limit_bytes=VMEM_LIMIT)


def cost(m, n, k):
    return pl.CostEstimate(flops=2 * m * n * k, bytes_accessed=2 * (m * k + k * n + m * n), transcendentals=0)


def pre_kernel(dy_ref, w_ref, pre_ref, d_pre_ref, hidden_ref):
    d_hidden = lax.dot_general(dy_ref[...], w_ref[...], (((1,), (1,)), ((), ())), preferred_element_type=jnp.float32)
    hidden, back = jax.vjp(act, pre_ref[...].astype(jnp.float32))
    d_pre_ref[...] = back(d_hidden)[0].astype(jnp.bfloat16)
    hidden_ref[...] = hidden.astype(jnp.bfloat16)


def pre_grad(dy, w_down, pre, tm=512, tn=512):
    (m, k), n = dy.shape, w_down.shape[0]
    return pl.pallas_call(
        pre_kernel,
        grid=(n // tn, m // tm),
        in_specs=[
            pl.BlockSpec((tm, k), lambda j, i: (i, 0)),
            pl.BlockSpec((tn, k), lambda j, i: (j, 0)),
            pl.BlockSpec((tm, tn), lambda j, i: (i, j)),
        ],
        out_specs=[pl.BlockSpec((tm, tn), lambda j, i: (i, j))] * 2,
        out_shape=[jax.ShapeDtypeStruct((m, n), jnp.bfloat16)] * 2,
        compiler_params=params("arbitrary", "arbitrary"),
        cost_estimate=cost(m, n, k),
        name="pre_grad",
    )(dy, w_down, pre)


def dot_kernel(dims, a_ref, b_ref, o_ref):
    o_ref[...] = lax.dot_general(a_ref[...], b_ref[...], (dims, ((), ())), preferred_element_type=jnp.float32).astype(jnp.bfloat16)


def matmul_nt(a, b, tm=1024, tn=1024):
    (m, k), n = a.shape, b.shape[0]
    return pl.pallas_call(
        functools.partial(dot_kernel, ((1,), (1,))),
        grid=(m // tm, n // tn),
        in_specs=[pl.BlockSpec((tm, k), lambda i, j: (i, 0)), pl.BlockSpec((tn, k), lambda i, j: (j, 0))],
        out_specs=pl.BlockSpec((tm, tn), lambda i, j: (i, j)),
        out_shape=jax.ShapeDtypeStruct((m, n), jnp.bfloat16),
        compiler_params=params("arbitrary", "arbitrary"),
        cost_estimate=cost(m, n, k),
        name="nt",
    )(a, b)


def matmul_tn(a, b, name, tm=1024, tn=1024):
    (k, m), n = a.shape, b.shape[1]
    return pl.pallas_call(
        functools.partial(dot_kernel, ((0,), (0,))),
        grid=(m // tm, n // tn),
        in_specs=[pl.BlockSpec((k, tm), lambda i, j: (0, i)), pl.BlockSpec((k, tn), lambda i, j: (0, j))],
        out_specs=pl.BlockSpec((tm, tn), lambda i, j: (i, j)),
        out_shape=jax.ShapeDtypeStruct((m, n), jnp.bfloat16),
        compiler_params=params("arbitrary", "arbitrary"),
        cost_estimate=cost(m, n, k),
        name=name,
    )(a, b)


def solution(mesh):
    def body(x, dy, pre, w_in, w_down):
        dy_all = lax.all_gather(dy, "tp", axis=0, tiled=True)
        x_all = lax.all_gather(x, "tp", axis=0, tiled=True)
        d_pre, hidden = pre_grad(dy_all, w_down, pre)
        dx = lax.psum_scatter(matmul_nt(d_pre, w_in), "tp", scatter_dimension=0, tiled=True)
        dw_down = matmul_tn(hidden, dy_all, "dw_down")
        dw_in = matmul_tn(x_all, d_pre, "dw_in")
        return dx, dw_in, dw_down

    return jax.shard_map(
        body,
        mesh=mesh,
        in_specs=(P(("dp", "tp")), P(("dp", "tp")), P("dp", "tp"), P(None, "tp"), P("tp", None)),
        out_specs=(P(("dp", "tp")), P("dp", "tp"), P(("dp", "tp"))),
        check_vma=False,
    )
```

```python
import functools

import jax
import jax.numpy as jnp
from jax import lax
from jax.experimental import pallas as pl
from jax.experimental.pallas import tpu as pltpu
from jax.sharding import PartitionSpec as P

VMEM_LIMIT = 66_000_000
WEIGHT = (4, 2, 1)
F32, BF16 = jnp.float32, jnp.bfloat16
ANY = pl.BlockSpec(memory_space=pl.ANY)
CHIPS = [(a, b, c) for a in (0, 1) for b in (0, 1) for c in (0, 1)]


def act(pre):
    return jax.nn.gelu(pre)


def dot(a, b, dims):
    return lax.dot_general(a, b, (dims, ((), ())), preferred_element_type=F32)


NT, TN = ((1,), (1,)), ((0,), (0,))


def rows(start, size):
    return pl.ds(pl.multiple_of(start, 16), size)


def lanes(start, size):
    return pl.ds(pl.multiple_of(start, 128), size)


class Place:
    def __init__(self):
        me = lax.axis_index("tp")
        self.chip, self.core = lax.div(me, 2), lax.rem(me, 2)
        self.step = [w * (1 - 2 * lax.rem(lax.div(self.chip, w), 2)) for w in WEIGHT]
        self.sibling = self.device(self.chip, 1 - self.core)

    def chip_at(self, r):
        return self.chip + sum(self.step[d] * r[d] for d in range(3) if isinstance(r[d], jax.Array) or r[d])

    def device(self, chip, core):
        return {"tp": 2 * chip + core}

    def across(self, d):
        if isinstance(d, int):
            return self.device(self.chip + self.step[d], self.core)
        r = (lax.div(2 - d, 2), lax.rem(d, 2), lax.div(d, 2))
        return self.device(self.chip_at(r), self.core)

    def barrier(self):
        sem = pltpu.get_barrier_semaphore()
        for peer in [self.sibling] + [self.across(d) for d in range(3)]:
            pl.semaphore_signal(sem, inc=1, device_id=peer, device_id_type=pl.DeviceIdType.MESH)
        pl.semaphore_wait(sem, 4)


def remote(src, dst, send, recv, device):
    return pltpu.make_async_remote_copy(src, dst, send, recv, device_id=device, device_id_type=pl.DeviceIdType.MESH)


def order(p):
    return p, (p + 1) % 3, (p + 2) % 3


def across(*dims):
    return tuple(int(d in dims) for d in range(3))


class Gather:
    def __init__(self, place, src, dst, sems, base):
        self.place, self.src, self.dst = place, src, dst
        self.shard, width = src.shape
        self.send, self.recv, self.out, self.back = (functools.partial(lambda s, i: s.at[base + i], s) for s in sems)
        tiles = width // 128
        ends = [128 * (tiles * k // 3) for k in range(4)]
        self.columns = [pl.ds(ends[k], ends[k + 1] - ends[k]) for k in range(3)]

    def rows_of(self, r, core):
        return rows((2 * self.place.chip_at(r) + core) * self.shard, self.shard)

    def piece(self, p, r, core):
        return self.dst.at[self.rows_of(r, core), self.columns[p]]

    @staticmethod
    def index(p, r):
        return 8 * p + 4 * r[0] + 2 * r[1] + r[2]

    def hop(self, p, r):
        d = [d for d in order(p) if r[d]][-1]
        q = tuple(r[e] * (e != d) for e in range(3))
        dst = self.piece(p, q, self.place.core)
        src = dst if any(q) else self.src.at[:, self.columns[p]]
        i = self.index(p, r)
        return remote(src, dst, self.send(i), self.recv(i), self.place.across(d))

    def arrive(self, p, r):
        view, i = self.piece(p, r, self.place.core), self.index(p, r)
        remote(view, view, self.send(i), self.recv(i), self.place.sibling).wait_recv()

    def share(self, p, r):
        view, i = self.piece(p, r, self.place.core), self.index(p, r)
        return remote(view, view, self.out(i), self.back(i), self.place.sibling)

    def shared(self, p, r):
        view, i = self.piece(p, r, 1 - self.place.core), self.index(p, r)
        remote(view, view, self.out(i), self.back(i), self.place.sibling).wait_recv()

    def share_own(self):
        return remote(self.src, self.dst.at[self.rows_of((0, 0, 0), self.place.core)], self.out(0), self.back(0), self.place.sibling)

    def shared_own(self):
        view = self.dst.at[self.rows_of((0, 0, 0), 1 - self.place.core)]
        remote(view, view, self.out(0), self.back(0), self.place.sibling).wait_recv()

    def begin(self):
        self.share_own().start()
        for k in range(3):
            for d in range(3):
                self.hop((d - k) % 3, across(d)).start()

    def act(self, n):
        for p in range(3):
            a, b, c = order(p)
            seq = [across(a), across(b), across(c), across(a, b), across(a, c), across(b, c), across(a, b, c)]
            follow = {0: [across(a, b), across(a, c)], 1: [across(b, c)], 3: [across(a, b, c)]}
            self.arrive(p, seq[n])
            for r in follow.get(n, []):
                self.hop(p, r).start()
            self.share(p, seq[n]).start()

    def drain(self):
        self.share_own().wait_send()
        for p in range(3):
            for r in CHIPS[1:]:
                self.hop(p, r).wait_send()
                self.share(p, r).wait_send()


NEAR = [(1, 0, 0), (0, 1, 0), (0, 0, 1)]
MIDDLE = [(1, 1, 0), (0, 1, 1), (1, 0, 1)]
FAR = [(1, 1, 1)]


def forward_kernel(x, dy, pre, w_down, x_all, dy_all, d_pre, hidden, slope, dw_down, send, recv, out, back, w_sem, load_sem, store_sem):
    place = Place()
    shard, width = dy.shape
    tokens, ff = pre.shape
    block = ff // 4
    place.barrier()
    sems = (send, recv, out, back)
    gather_dy = Gather(place, dy, dy_all, sems, 0)
    gather_x = Gather(place, x, x_all, sems, 24)
    gather_dy.begin()
    here = (0, 0, 0)

    def gradient(weights):
        def load_weights(j):
            part = pl.ds(j * block, block)
            return pltpu.make_async_copy(w_down.at[part], weights.at[part], w_sem.at[j])

        for j in range(4):
            load_weights(j).start()

        def gelu(pre_ref, hidden_ref, slope_ref):
            value, pull = jax.vjp(act, pre_ref[...].astype(F32))
            hidden_ref[...] = value.astype(BF16)
            slope_ref[...] = pull(jnp.ones_like(value))[0]

        spec = pl.BlockSpec((shard, ff), lambda i: (i, 0))
        pltpu.emit_pipeline(gelu, grid=(tokens // shard,), in_specs=[spec], out_specs=[spec, spec])(pre, hidden, slope)

        def chunks(lhs, slopes, result):
            def part(k):
                return pl.ds(k * shard, shard)

            def stores(chips):
                parts = [(r, core) for r in chips for core in (0, 1)]
                return [
                    pltpu.make_async_copy(
                        result.at[part(k)], d_pre.at[gather_dy.rows_of(r, place.core + core - 2 * core * place.core)], store_sem.at[k]
                    )
                    for k, (r, core) in enumerate(parts)
                ]

            def chunk(chips, before, first=False):
                shards = [(r, place.core + core - 2 * core * place.core) for r in chips for core in (0, 1)]
                copies = []
                for k, (r, core) in enumerate(shards):
                    src = dy if (first and k == 0) else dy_all.at[gather_dy.rows_of(r, core)]
                    copies.append(pltpu.make_async_copy(src, lhs.at[part(k)], load_sem.at[k]))
                    copies.append(pltpu.make_async_copy(slope.at[gather_dy.rows_of(r, core)], slopes.at[part(k)], load_sem.at[6 + k]))
                for copy in copies:
                    copy.start()
                for copy in copies:
                    copy.wait()
                if first:
                    own = pltpu.make_async_copy(lhs.at[part(0)], dy_all.at[gather_dy.rows_of(here, place.core)], load_sem.at[0])
                    own.start()
                    for j in range(4):
                        load_weights(j).wait()
                for copy in before:
                    copy.wait()
                size = len(shards) * shard

                @pl.loop(0, 4)
                def _(j):
                    columns = lanes(j * block, block)
                    d_hidden = dot(lhs[:size], weights[rows(j * block, block), :], NT)
                    result[:size, columns] = (d_hidden * slopes[:size, columns]).astype(BF16)

                if first:
                    own.wait()
                done = stores(chips)
                for copy in done:
                    copy.start()
                return done

            gather_dy.act(0)
            gather_dy.shared_own()
            done = chunk([here], [], first=True)
            gather_dy.act(1)
            gather_dy.act(2)
            for p in range(3):
                for r in NEAR:
                    gather_dy.shared(p, r)
            done = chunk(NEAR, done)
            gather_dy.act(3)
            gather_x.begin()
            gather_dy.act(4)
            gather_dy.act(5)
            for p in range(3):
                for r in MIDDLE:
                    gather_dy.shared(p, r)
            done = chunk(MIDDLE, done)
            gather_dy.act(6)
            for p in range(3):
                gather_dy.shared(p, FAR[0])
            done = chunk(FAR, done)
            own = [
                pltpu.make_async_copy(x, lhs.at[part(0)], load_sem.at[0]),
                pltpu.make_async_copy(lhs.at[part(0)], x_all.at[gather_dy.rows_of(here, place.core)], load_sem.at[0]),
            ]
            for copy in own:
                copy.start()
                copy.wait()
            for copy in done:
                copy.wait()

        pl.run_scoped(chunks, pltpu.VMEM((6 * shard, width), BF16), pltpu.VMEM((6 * shard, ff), F32), pltpu.VMEM((6 * shard, ff), BF16))

    pl.run_scoped(gradient, pltpu.VMEM((ff, width), BF16))

    tm, tn = ff // 2, width // 8

    def product(h_ref, dy_ref, o_ref):
        at = pl.program_id(0) * 8 + pl.program_id(1)
        for n, when in enumerate((1, 2, 5, 8, 11, 14)):
            @pl.when(at == when)
            def _():
                gather_x.act(n)

        o_ref[...] = dot(h_ref[...], dy_ref[...], TN).astype(BF16)

    pltpu.emit_pipeline(
        product,
        grid=(2, 8),
        in_specs=[pl.BlockSpec((tokens, tm), lambda i, j: (0, i)), pl.BlockSpec((tokens, tn), lambda i, j: (0, j))],
        out_specs=[pl.BlockSpec((tm, tn), lambda i, j: (i, j))],
    )(hidden, dy_all, dw_down)
    gather_x.act(6)
    gather_x.shared_own()
    for p in range(3):
        for r in CHIPS[1:]:
            gather_x.shared(p, r)
    gather_dy.drain()
    gather_x.drain()


def forward(x, dy, pre, w_down):
    shard, width = dy.shape
    tokens, ff = pre.shape
    dma = pltpu.SemaphoreType.DMA
    whole = jax.ShapeDtypeStruct((tokens, width), BF16)
    return pl.pallas_call(
        forward_kernel,
        in_specs=[ANY] * 4,
        out_specs=[ANY] * 6,
        out_shape=[
            whole,
            whole,
            jax.ShapeDtypeStruct((tokens, ff), BF16),
            jax.ShapeDtypeStruct((tokens, ff), BF16),
            jax.ShapeDtypeStruct((tokens, ff), F32),
            jax.ShapeDtypeStruct((ff, width), BF16),
        ],
        scratch_shapes=[dma((48,)), dma((48,)), dma((48,)), dma((48,)), dma((4,)), dma((12,)), dma((6,))],
        compiler_params=pltpu.CompilerParams(collective_id=0, has_side_effects=True, vmem_limit_bytes=VMEM_LIMIT),
        cost_estimate=pl.CostEstimate(flops=4 * tokens * ff * width, bytes_accessed=400_000_000, transcendentals=tokens * ff),
        name="gather_gradient",
    )(x, dy, pre, w_down)


def scatter_kernel(x_all, d_pre, w_in, dx, dw_in, ici, d2d, out1, out2, out3, out4, lhs2, lhs3, lhs4, weights,
                   ici_send, ici_recv, d2d_send, d2d_recv, w_sem, load_sem, stage_sem, dx_sem, x_sem, dw_sem):
    place = Place()
    chip, core = place.chip, place.core
    shard, width = dx.shape
    tokens, ff = d_pre.shape
    n1, n2 = width // 16, width // 8

    def pick(i, group):
        k = lax.div(i, 3 * group)
        p = (1 - k) * lax.rem(i, 3) + k * lax.rem(i, 2)
        t = (1 - k) * lax.div(i, 3) + k * (group + lax.div(i - 3 * group, 2))
        return p, t

    def unpick(p, t, group):
        k = lax.div(t, group)
        return (1 - k) * (3 * t + p) + k * (3 * group + 2 * (t - group) + p)

    def turn(p, k):
        return lax.rem(p + k, 3)

    def narrow(i):
        p, t = pick(i, 4)
        return p, t, p * (3 * n2) + t * n1

    def wide(i):
        p, t = pick(i, 2)
        return p, t, p * (3 * n2) + t * n2

    def narrow_weights(i):
        slot = lax.rem(i, 4)
        return [pltpu.make_async_copy(w_in.at[rows(narrow(i)[2], n1)], weights.at[rows(slot * n1, n1)], w_sem.at[slot])]

    def wide_weights(i):
        start, slot = wide(i)[2], lax.rem(i, 2)
        return [
            pltpu.make_async_copy(w_in.at[rows(start + h * n1, n1)], weights.at[rows(slot * n2 + h * n1, n1)], w_sem.at[2 * slot + h])
            for h in (0, 1)
        ]

    def go(copies):
        for copy in copies:
            copy.start()

    def wait(copies):
        for copy in copies:
            copy.wait()

    def lhs_loads(ref, p, chips, base):
        loads = []
        for half, c in enumerate((1 - core, core)):
            for k, r in enumerate(chips):
                src = d_pre.at[rows((2 * place.chip_at(r) + c) * shard, shard)]
                n = half * len(chips) + k
                view = ref if p is None else ref.at[p]
                loads.append(pltpu.make_async_copy(src, view.at[pl.ds(n * shard, shard)], load_sem.at[base + n]))
        return loads

    place.barrier()
    for i in range(4):
        go(narrow_weights(i))

    def exchange(k, i, count, size, columns, base, part):
        region = (0, 4, 6, 7)[k]
        dst = d2d.at[pl.ds(region * shard, count * shard), columns]
        return remote(part, dst, d2d_send.at[base + i], d2d_recv.at[base + i], place.sibling)

    def onward(k, i, count, p, columns, base, part):
        region = (0, 4, 6)[k]
        dst = ici.at[pl.ds(region * shard, count * shard), columns]
        return remote(part, dst, ici_send.at[base + i], ici_recv.at[base + i], place.across(turn(p, k)))

    def stage_chips(p, k):
        a, b, c = order(p)
        tail = [(0, 0), (0, 1), (1, 0), (1, 1)]
        if k == 0:
            return [tuple(across(a)[d] + s * across(b)[d] + t * across(c)[d] for d in range(3)) for s, t in tail]
        if k == 1:
            return [across(b), across(b, c)]
        return [across(c)] if k == 2 else [(0, 0, 0)]

    def stage(k, items, lhs, out, group, lag_b, lag_c, filler=None):
        count = (4, 2, 1, 1)[k]
        size = n1 if k == 0 else n2
        base = (0, 16, 24, 32)[k]
        locate = narrow if k == 0 else wide
        slots = lag_c + 1
        n_in = 1 + k
        from_ici = [(), ((2, 4),), ((1, 2), (5, 6)), ((0, 1), (4, 5), (6, 7))][k]

        def body(acc, term, staged):
            def columns(i):
                return lanes(locate(i)[2], size)

            def sources(i):
                region = (0, 4, 6, 7)[k]
                views = [d2d.at[pl.ds(region * shard, count * shard), columns(i)]]
                views += [ici.at[pl.ds(a * shard, (b - a) * shard), columns(i)] for a, b in from_ici]
                slot = lax.rem(i, slots)
                return [
                    pltpu.make_async_copy(view, staged.at[slot, n], stage_sem.at[slot * n_in + n]) for n, view in enumerate(views)
                ]

            def send(i):
                slot = lax.rem(i, slots)
                return exchange(k, i, count, size, columns(i), base, term.at[slot])

            def leave(i):
                if k < 3:
                    return onward(k, i, count, locate(i)[0], columns(i), base, out.at[i])
                return pltpu.make_async_copy(out.at[i], dx.at[:, columns(i)], dx_sem.at[i])

            @pl.loop(0, items + lag_c)
            def _(i):
                @pl.when(i < items)
                def _():
                    p, _, start = locate(i)
                    slot = lax.rem(i, slots)
                    if k == 0:
                        wait(narrow_weights(i))
                        w = weights[rows(lax.rem(i, 4) * n1, n1), :]
                    else:
                        wait(wide_weights(i))
                        w = weights[rows(lax.rem(i, 2) * n2, n2), :]

                    @pl.when(i >= slots)
                    def _():
                        send(i - slots).wait_send()

                    left = lhs[...] if k == 3 else lhs[p]
                    value = dot(left, w, NT)
                    term[slot] = value[: count * shard].astype(BF16)
                    acc[slot] = value[count * shard :]
                    send(i).start()
                    if k == 0:
                        @pl.when(i + 4 < items)
                        def _():
                            go(narrow_weights(i + 4))

                        @pl.when(i == items - 3)
                        def _():
                            go(wide_weights(0))

                        @pl.when(i == items - 1)
                        def _():
                            go(wide_weights(1))
                    elif k < 3:
                        go(wide_weights(lax.rem(i + 2, 8)))
                    else:
                        @pl.when(i + 2 < items)
                        def _():
                            go(wide_weights(i + 2))

                    if filler is not None:
                        filler(i)

                @pl.when((i >= lag_b) & (i < items + lag_b))
                def _():
                    j = i - lag_b
                    view = d2d.at[pl.ds(0, count * shard), columns(j)]
                    remote(view, view, d2d_send.at[base + j], d2d_recv.at[base + j], place.sibling).wait_recv()
                    p, t, _ = locate(j)
                    if k == 1:
                        for h in (0, 1):
                            n = unpick(p, 2 * t + h, 4)
                            view = ici.at[pl.ds(0, 4 * shard), lanes(locate(j)[2] + h * n1, n1)]
                            remote(view, view, ici_send.at[n], ici_recv.at[n], place.sibling).wait_recv()
                    elif k > 1:
                        n = (16, 24)[k - 2] + j
                        view = ici.at[pl.ds(0, (2, 1)[k - 2] * shard), columns(j)]
                        remote(view, view, ici_send.at[n], ici_recv.at[n], place.sibling).wait_recv()
                    go(sources(j))

                @pl.when(i >= lag_c)
                def _():
                    j = i - lag_c
                    slot = lax.rem(j, slots)
                    wait(sources(j))
                    total = acc[slot]
                    for n in range(n_in):
                        total = total + staged[slot, n].astype(F32)
                    out[j] = total.astype(BF16)
                    leave(j).start()

            for i in range(max(items - slots, 0), items):
                send(i).wait_send()

        pl.run_scoped(
            body,
            pltpu.VMEM((slots, count * shard, size), F32),
            pltpu.VMEM((slots, count * shard, size), BF16),
            pltpu.VMEM((slots, n_in, count * shard, size), BF16),
        )

    def first(lhs1):
        loads = [lhs_loads(lhs1, p, stage_chips(p, 0), 8 * p) for p in range(3)]
        loads.append([c for p in range(3) for c in lhs_loads(lhs2, p, stage_chips(p, 1), 24 + 4 * p)])
        loads.append([c for p in range(3) for c in lhs_loads(lhs3, p, stage_chips(p, 2), 36 + 2 * p)])
        loads.append(lhs_loads(lhs4, None, stage_chips(0, 3), 42))
        for some in loads:
            go(some)
        for some in loads:
            wait(some)
        stage(0, 16, lhs1, out1, 4, 1, 2)

    pl.run_scoped(first, pltpu.VMEM((3, 8 * shard, ff), BF16))

    def second(right, x_buf, dw_buf, right_sem):
        copy = pltpu.make_async_copy(d_pre, right, right_sem.at[0])
        copy.start()

        def x_load(i):
            slot = lax.rem(i, 2)
            return pltpu.make_async_copy(x_all.at[:, lanes(i * n1, n1)], x_buf.at[slot], x_sem.at[slot])

        def dw_store(i):
            slot = lax.rem(i, 2)
            return pltpu.make_async_copy(dw_buf.at[slot], dw_in.at[rows(i * n1, n1)], dw_sem.at[slot])

        x_load(0).start()
        x_load(1).start()
        copy.wait()

        def tile(i):
            slot = lax.rem(i, 2)
            x_load(i).wait()

            @pl.when(i >= 2)
            def _():
                dw_store(i - 2).wait()

            @pl.loop(0, 2)
            def _(h):
                half = lanes(h * (ff // 2), ff // 2)
                dw_buf[slot, :, half] = dot(x_buf[slot], right[:, half], TN).astype(BF16)

            dw_store(i).start()

            @pl.when(i + 2 < 8)
            def _():
                x_load(i + 2).start()

        stage(1, 8, lhs2, out2, 2, 0, 1, filler=tile)
        dw_store(6).wait()
        dw_store(7).wait()

    pl.run_scoped(
        second,
        pltpu.VMEM((tokens, ff), BF16),
        pltpu.VMEM((2, tokens, n1), BF16),
        pltpu.VMEM((2, n1, ff), BF16),
        pltpu.SemaphoreType.DMA((1,)),
    )
    stage(2, 8, lhs3, out3, 2, 2, 4)
    stage(3, 8, lhs4, out4, 2, 2, 4)
    for i in range(16):
        onward(0, i, 4, narrow(i)[0], lanes(narrow(i)[2], n1), 0, out1.at[i]).wait_send()
    for i in range(8):
        onward(1, i, 2, wide(i)[0], lanes(wide(i)[2], n2), 16, out2.at[i]).wait_send()
        onward(2, i, 1, wide(i)[0], lanes(wide(i)[2], n2), 24, out3.at[i]).wait_send()
        pltpu.make_async_copy(out4.at[i], dx.at[:, lanes(wide(i)[2], n2)], dx_sem.at[i]).wait()


def scatter(x_all, d_pre, w_in, shard):
    tokens, ff = d_pre.shape
    width = x_all.shape[1]
    n1, n2 = width // 16, width // 8
    dma, vmem = pltpu.SemaphoreType.DMA, pltpu.VMEM
    return pl.pallas_call(
        scatter_kernel,
        in_specs=[ANY] * 3,
        out_specs=[ANY] * 4,
        out_shape=[
            jax.ShapeDtypeStruct((shard, width), BF16),
            jax.ShapeDtypeStruct((width // 2, ff), BF16),
            jax.ShapeDtypeStruct((7 * shard, width), BF16),
            jax.ShapeDtypeStruct((8 * shard, width), BF16),
        ],
        scratch_shapes=[
            vmem((16, 4 * shard, n1), BF16),
            vmem((8, 2 * shard, n2), BF16),
            vmem((8, shard, n2), BF16),
            vmem((8, shard, n2), BF16),
            vmem((3, 4 * shard, ff), BF16),
            vmem((3, 2 * shard, ff), BF16),
            vmem((2 * shard, ff), BF16),
            vmem((4 * n1, ff), BF16),
            dma((32,)), dma((32,)), dma((40,)), dma((40,)), dma((4,)), dma((44,)), dma((20,)), dma((8,)), dma((2,)), dma((2,)),
        ],
        compiler_params=pltpu.CompilerParams(collective_id=1, has_side_effects=True, vmem_limit_bytes=VMEM_LIMIT),
        cost_estimate=pl.CostEstimate(flops=3 * tokens * ff * width, bytes_accessed=400_000_000, transcendentals=0),
        name="scatter_dx",
    )(x_all, d_pre, w_in)[:2]


def finish_kernel(x_ref, d_pre_ref, part_ref, down_ref, dw_in, dw_down, buf, copy_sem, buf_sem):
    i = pl.program_id(0)
    n, ff = part_ref.shape
    count = pl.num_programs(0)
    slot = lax.rem(i, 2)
    copies = [
        pltpu.make_async_copy(part_ref, dw_in.at[rows(i * n, n)], copy_sem.at[0]),
        pltpu.make_async_copy(down_ref, dw_down.at[rows(i * down_ref.shape[0], down_ref.shape[0])], copy_sem.at[1]),
    ]

    def store(i):
        slot = lax.rem(i, 2)
        return pltpu.make_async_copy(buf.at[slot], dw_in.at[rows((count + i) * n, n)], buf_sem.at[slot])

    for copy in copies:
        copy.start()

    @pl.when(i >= 2)
    def _():
        store(i - 2).wait()

    @pl.loop(0, 2)
    def _(h):
        half = lanes(h * (ff // 2), ff // 2)
        buf[slot, :, half] = dot(x_ref[...], d_pre_ref[:, half], TN).astype(BF16)

    store(i).start()
    for copy in copies:
        copy.wait()

    @pl.when(i == count - 1)
    def _():
        store(i - 1).wait()
        store(i).wait()


def finish(x_all, d_pre, dw_in_part, dw_down_part):
    tokens, ff = d_pre.shape
    width = x_all.shape[1]
    n = width // 16
    return pl.pallas_call(
        finish_kernel,
        grid=(8,),
        in_specs=[
            pl.BlockSpec((tokens, n), lambda i: (0, 8 + i)),
            pl.BlockSpec((tokens, ff), lambda i: (0, 0)),
            pl.BlockSpec((n, ff), lambda i: (i, 0)),
            pl.BlockSpec((ff // 8, width), lambda i: (i, 0)),
        ],
        out_specs=[ANY] * 2,
        out_shape=[jax.ShapeDtypeStruct((width, ff), BF16), jax.ShapeDtypeStruct((ff, width), BF16)],
        scratch_shapes=[pltpu.VMEM((2, n, ff), BF16), pltpu.SemaphoreType.DMA((2,)), pltpu.SemaphoreType.DMA((2,))],
        compiler_params=pltpu.CompilerParams(dimension_semantics=("arbitrary",), vmem_limit_bytes=VMEM_LIMIT),
        cost_estimate=pl.CostEstimate(flops=tokens * ff * width, bytes_accessed=140_000_000, transcendentals=0),
        name="finish",
    )(x_all, d_pre, dw_in_part, dw_down_part)


def solution(mesh):
    def body(x, dy, pre, w_in, w_down):
        x_all, _, d_pre, _, _, dw_down = forward(x, dy, pre, w_down)
        dx, dw_in = scatter(x_all, d_pre, w_in, x.shape[0])
        dw_in, dw_down = finish(x_all, d_pre, dw_in, dw_down)
        return dx, dw_in, dw_down

    return jax.shard_map(
        body,
        mesh=mesh,
        in_specs=(P(("dp", "tp")), P(("dp", "tp")), P("dp", "tp"), P(None, "tp"), P("tp", None)),
        out_specs=(P(("dp", "tp")), P("dp", "tp"), P(("dp", "tp"))),
        check_vma=False,
    )
```

```python
import functools

import jax
import jax.numpy as jnp
from jax import lax
from jax.experimental import pallas as pl
from jax.experimental.pallas import tpu as pltpu
from jax.sharding import PartitionSpec as P

VMEM_LIMIT = 66_000_000
WEIGHT = (4, 2, 1)
F32, BF16 = jnp.float32, jnp.bfloat16
ANY = pl.BlockSpec(memory_space=pl.ANY)
CHIPS = [(a, b, c) for a in (0, 1) for b in (0, 1) for c in (0, 1)]


def act(pre):
    return jax.nn.gelu(pre)


def dot(a, b, dims):
    return lax.dot_general(a, b, (dims, ((), ())), preferred_element_type=F32)


NT, TN = ((1,), (1,)), ((0,), (0,))


def rows(start, size):
    return pl.ds(pl.multiple_of(start, 16), size)


def lanes(start, size):
    return pl.ds(pl.multiple_of(start, 128), size)


class Place:
    def __init__(self):
        me = lax.axis_index("tp")
        self.chip, self.core = lax.div(me, 2), lax.rem(me, 2)
        self.step = [w * (1 - 2 * lax.rem(lax.div(self.chip, w), 2)) for w in WEIGHT]
        self.sibling = self.device(self.chip, 1 - self.core)

    def chip_at(self, r):
        return self.chip + sum(self.step[d] * r[d] for d in range(3) if isinstance(r[d], jax.Array) or r[d])

    def device(self, chip, core):
        return {"tp": 2 * chip + core}

    def across(self, d):
        if isinstance(d, int):
            return self.device(self.chip + self.step[d], self.core)
        r = (lax.div(2 - d, 2), lax.rem(d, 2), lax.div(d, 2))
        return self.device(self.chip_at(r), self.core)

    def barrier(self):
        sem = pltpu.get_barrier_semaphore()
        for peer in [self.sibling] + [self.across(d) for d in range(3)]:
            pl.semaphore_signal(sem, inc=1, device_id=peer, device_id_type=pl.DeviceIdType.MESH)
        pl.semaphore_wait(sem, 4)


def remote(src, dst, send, recv, device):
    return pltpu.make_async_remote_copy(src, dst, send, recv, device_id=device, device_id_type=pl.DeviceIdType.MESH)


def order(p):
    return p, (p + 1) % 3, (p + 2) % 3


def across(*dims):
    return tuple(int(d in dims) for d in range(3))


class Gather:
    def __init__(self, place, src, dst, sems, base, halves):
        self.place, self.src, self.dst, self.halves = place, src, dst, halves
        self.shard, width = src.shape
        self.size = self.shard // halves
        self.send, self.recv, self.out, self.back = (functools.partial(lambda s, i: s.at[base + i], s) for s in sems)
        tiles = width // 128
        ends = [128 * (tiles * k // 3) for k in range(4)]
        self.columns = [pl.ds(ends[k], ends[k + 1] - ends[k]) for k in range(3)]

    def rows_of(self, r, core, h=None):
        start = (2 * self.place.chip_at(r) + core) * self.shard
        return rows(start, self.shard) if h is None else rows(start + h * self.size, self.size)

    def piece(self, p, r, core, h):
        return self.dst.at[self.rows_of(r, core, h), self.columns[p]]

    @staticmethod
    def index(p, r, h):
        return 24 * h + 8 * p + 4 * r[0] + 2 * r[1] + r[2]

    def hop(self, p, r, h):
        d = [d for d in order(p) if r[d]][-1]
        q = tuple(r[e] * (e != d) for e in range(3))
        dst = self.piece(p, q, self.place.core, h)
        src = dst if any(q) else self.src.at[pl.ds(h * self.size, self.size), self.columns[p]]
        i = self.index(p, r, h)
        return remote(src, dst, self.send(i), self.recv(i), self.place.across(d))

    def arrive(self, p, r, h):
        view, i = self.piece(p, r, self.place.core, h), self.index(p, r, h)
        remote(view, view, self.send(i), self.recv(i), self.place.sibling).wait_recv()

    def share(self, p, r, h):
        view, i = self.piece(p, r, self.place.core, h), self.index(p, r, h)
        return remote(view, view, self.out(i), self.back(i), self.place.sibling)

    def shared(self, p, r, h):
        view, i = self.piece(p, r, 1 - self.place.core, h), self.index(p, r, h)
        remote(view, view, self.out(i), self.back(i), self.place.sibling).wait_recv()

    def share_own(self):
        return remote(self.src, self.dst.at[self.rows_of((0, 0, 0), self.place.core)], self.out(0), self.back(0), self.place.sibling)

    def shared_own(self):
        view = self.dst.at[self.rows_of((0, 0, 0), 1 - self.place.core)]
        remote(view, view, self.out(0), self.back(0), self.place.sibling).wait_recv()

    def shared_all(self, chips, h):
        for p in range(3):
            for r in chips:
                self.shared(p, r, h)

    def begin(self):
        self.share_own().start()
        for h in range(self.halves):
            for k in range(3):
                for d in range(3):
                    self.hop((d - k) % 3, across(d), h).start()

    def act(self, n, h=0):
        for p in range(3):
            a, b, c = order(p)
            seq = [across(a), across(b), across(c), across(a, b), across(a, c), across(b, c), across(a, b, c)]
            follow = {0: [across(a, b), across(a, c)], 1: [across(b, c)], 3: [across(a, b, c)]}
            self.arrive(p, seq[n], h)
            for r in follow.get(n, []):
                self.hop(p, r, h).start()
            self.share(p, seq[n], h).start()

    def drain(self):
        self.share_own().wait_send()
        for h in range(self.halves):
            for p in range(3):
                for r in CHIPS[1:]:
                    self.hop(p, r, h).wait_send()
                    self.share(p, r, h).wait_send()


NEAR = [(1, 0, 0), (0, 1, 0), (0, 0, 1)]
MIDDLE = [(1, 1, 0), (0, 1, 1), (1, 0, 1)]
FAR = [(1, 1, 1)]
HERE = [(0, 0, 0)]


def forward_kernel(x, dy, pre, w_down, x_all, dy_all, d_pre, hidden, slope, dw_down, send, recv, out, back, w_sem, load_sem, store_sem, own_sem):
    place = Place()
    shard, width = dy.shape
    half = shard // 2
    tokens, ff = pre.shape
    block = ff // 4
    place.barrier()
    sems = (send, recv, out, back)
    gather_dy = Gather(place, dy, dy_all, sems, 0, 2)
    gather_x = Gather(place, x, x_all, sems, 48, 1)
    gather_dy.begin()
    mine = gather_dy.rows_of(HERE[0], place.core)

    def gradient(weights):
        def load_weights(j):
            part = pl.ds(j * block, block)
            return pltpu.make_async_copy(w_down.at[part], weights.at[part], w_sem.at[j])

        for j in range(4):
            load_weights(j).start()

        def before(x_buf):
            taken = pltpu.make_async_copy(x, x_buf, own_sem.at[0])
            taken.start()

            def gelu(pre_ref, hidden_ref, slope_ref):
                value, pull = jax.vjp(act, pre_ref[...].astype(F32))
                hidden_ref[...] = value.astype(BF16)
                slope_ref[...] = pull(jnp.ones_like(value))[0]

            spec = pl.BlockSpec((shard, ff), lambda i: (i, 0))
            pltpu.emit_pipeline(gelu, grid=(tokens // shard,), in_specs=[spec], out_specs=[spec, spec])(pre, hidden, slope)
            taken.wait()
            put = pltpu.make_async_copy(x_buf, x_all.at[mine], own_sem.at[1])
            put.start()
            for n in range(3):
                gather_dy.act(n, 0)
            gather_dy.shared_own()
            put.wait()

        pl.run_scoped(before, pltpu.VMEM((shard, width), BF16))

        def chunks(lhs, slopes, result):
            batches = [(HERE, None), (NEAR, 0), (NEAR, 1), (MIDDLE, 0), (MIDDLE, 1), (FAR, None)]

            def parts(n):
                chips, h = batches[n]
                size = shard if h is None else half
                cores = (place.core, 1 - place.core)
                return [(gather_dy.rows_of(r, c, h), pl.ds(k * size, size)) for k, (r, c) in enumerate((r, c) for r in chips for c in cores)]

            def rows_in(n):
                return sum(part.size for _, part in parts(n))

            def loads(n):
                copies = []
                for k, (src, part) in enumerate(parts(n)):
                    at = 12 * (n % 2) + k
                    there = dy if (n == 0 and k == 0) else dy_all.at[src]
                    copies.append(pltpu.make_async_copy(there, lhs.at[n % 2, part], load_sem.at[at]))
                    copies.append(pltpu.make_async_copy(slope.at[src], slopes.at[n % 2, part], load_sem.at[at + 6]))
                return copies

            def stores(n):
                return [
                    pltpu.make_async_copy(result.at[n % 2, part], d_pre.at[dst], store_sem.at[6 * (n % 2) + k])
                    for k, (dst, part) in enumerate(parts(n))
                ]

            own = pltpu.make_async_copy(lhs.at[0, pl.ds(0, shard)], dy_all.at[mine], own_sem.at[0])

            def ready(n):
                chips, h = batches[n]
                if n == 2:
                    for k in range(3):
                        gather_dy.act(k, 1)
                if n in (3, 4):
                    for k in (3, 4, 5):
                        gather_dy.act(k, h)
                if n == 5:
                    gather_dy.act(6, 0)
                    gather_dy.act(6, 1)
                for h in (0, 1) if h is None else (h,):
                    gather_dy.shared_all(chips, h)
                if n == 2:
                    own.wait()
                for copy in loads(n):
                    copy.start()

            when = (2, 3, 4, 4, 3)
            for copy in loads(0):
                copy.start()
            for n in range(6):
                for copy in loads(n):
                    copy.wait()
                if n == 0:
                    own.start()
                    for j in range(4):
                        load_weights(j).wait()
                if n >= 2:
                    for copy in stores(n - 2):
                        copy.wait()
                size, slot = rows_in(n), n % 2

                @pl.loop(0, 4)
                def _(j):
                    if n < 5 and when[n] < 4:
                        @pl.when(j == when[n])
                        def _():
                            ready(n + 1)

                    columns = lanes(j * block, block)
                    d_hidden = dot(lhs[slot, :size], weights[rows(j * block, block), :], NT)
                    result[slot, :size, columns] = (d_hidden * slopes[slot, :size, columns]).astype(BF16)

                for copy in stores(n):
                    copy.start()
                if n < 5 and when[n] == 4:
                    ready(n + 1)
                if n == 3:
                    gather_x.begin()
            for n in (4, 5):
                for copy in stores(n):
                    copy.wait()

        pl.run_scoped(chunks, pltpu.VMEM((2, 6 * half, width), BF16), pltpu.VMEM((2, 6 * half, ff), F32), pltpu.VMEM((2, 6 * half, ff), BF16))

    pl.run_scoped(gradient, pltpu.VMEM((ff, width), BF16))

    tm, tn = ff // 2, width // 8

    def product(h_ref, dy_ref, o_ref):
        at = pl.program_id(0) * 8 + pl.program_id(1)
        for n, when in enumerate((1, 4, 7, 10, 13, 15)):
            @pl.when(at == when)
            def _():
                gather_x.act(n)

        o_ref[...] = dot(h_ref[...], dy_ref[...], TN).astype(BF16)

    pltpu.emit_pipeline(
        product,
        grid=(2, 8),
        in_specs=[pl.BlockSpec((tokens, tm), lambda i, j: (0, i)), pl.BlockSpec((tokens, tn), lambda i, j: (0, j))],
        out_specs=[pl.BlockSpec((tm, tn), lambda i, j: (i, j))],
    )(hidden, dy_all, dw_down)
    gather_x.act(6)
    gather_x.shared_own()
    gather_x.shared_all(CHIPS[1:], 0)
    gather_dy.drain()
    gather_x.drain()


def forward(x, dy, pre, w_down):
    shard, width = dy.shape
    tokens, ff = pre.shape
    dma = pltpu.SemaphoreType.DMA
    whole = jax.ShapeDtypeStruct((tokens, width), BF16)
    return pl.pallas_call(
        forward_kernel,
        in_specs=[ANY] * 4,
        out_specs=[ANY] * 6,
        out_shape=[
            whole,
            whole,
            jax.ShapeDtypeStruct((tokens, ff), BF16),
            jax.ShapeDtypeStruct((tokens, ff), BF16),
            jax.ShapeDtypeStruct((tokens, ff), F32),
            jax.ShapeDtypeStruct((ff, width), BF16),
        ],
        scratch_shapes=[dma((72,)), dma((72,)), dma((72,)), dma((72,)), dma((4,)), dma((24,)), dma((12,)), dma((2,))],
        compiler_params=pltpu.CompilerParams(collective_id=0, has_side_effects=True, vmem_limit_bytes=VMEM_LIMIT),
        cost_estimate=pl.CostEstimate(flops=4 * tokens * ff * width, bytes_accessed=400_000_000, transcendentals=tokens * ff),
        name="gather_gradient",
    )(x, dy, pre, w_down)


def scatter_kernel(x_all, d_pre, w_in, dx, dw_in, ici, d2d, out1, out2, lhs2, lhs3, lhs4, weights,
                   ici_send, ici_recv, d2d_send, d2d_recv, w_sem, load_sem, stage_sem, dx_sem, x_sem, dw_sem):
    place = Place()
    chip, core = place.chip, place.core
    shard, width = dx.shape
    tokens, ff = d_pre.shape
    n1, n2 = width // 16, width // 8

    def pick(i, group):
        k = lax.div(i, 3 * group)
        p = (1 - k) * lax.rem(i, 3) + k * lax.rem(i, 2)
        t = (1 - k) * lax.div(i, 3) + k * (group + lax.div(i - 3 * group, 2))
        return p, t

    def unpick(p, t, group):
        k = lax.div(t, group)
        return (1 - k) * (3 * t + p) + k * (3 * group + 2 * (t - group) + p)

    def turn(p, k):
        return lax.rem(p + k, 3)

    def narrow(i):
        p, t = pick(i, 4)
        return p, t, p * (3 * n2) + t * n1

    def wide(i):
        p, t = pick(i, 2)
        return p, t, p * (3 * n2) + t * n2

    def narrow_weights(i):
        slot = lax.rem(i, 4)
        return [pltpu.make_async_copy(w_in.at[rows(narrow(i)[2], n1)], weights.at[rows(slot * n1, n1)], w_sem.at[slot])]

    def wide_weights(i):
        start, slot = wide(i)[2], lax.rem(i, 2)
        return [
            pltpu.make_async_copy(w_in.at[rows(start + h * n1, n1)], weights.at[rows(slot * n2 + h * n1, n1)], w_sem.at[2 * slot + h])
            for h in (0, 1)
        ]

    def go(copies):
        for copy in copies:
            copy.start()

    def wait(copies):
        for copy in copies:
            copy.wait()

    def lhs_loads(ref, p, chips, base):
        loads = []
        for half, c in enumerate((1 - core, core)):
            for k, r in enumerate(chips):
                src = d_pre.at[rows((2 * place.chip_at(r) + c) * shard, shard)]
                n = half * len(chips) + k
                view = ref if p is None else ref.at[p]
                loads.append(pltpu.make_async_copy(src, view.at[pl.ds(n * shard, shard)], load_sem.at[base + n]))
        return loads

    place.barrier()
    for i in range(4):
        go(narrow_weights(i))

    def exchange(k, i, count, size, columns, base, part):
        region = (0, 4, 6, 7)[k]
        dst = d2d.at[pl.ds(region * shard, count * shard), columns]
        return remote(part, dst, d2d_send.at[base + i], d2d_recv.at[base + i], place.sibling)

    def onward(k, i, count, p, columns, base, part):
        region = (0, 4, 6)[k]
        dst = ici.at[pl.ds(region * shard, count * shard), columns]
        return remote(part, dst, ici_send.at[base + i], ici_recv.at[base + i], place.across(turn(p, k)))

    def stage_chips(p, k):
        a, b, c = order(p)
        tail = [(0, 0), (0, 1), (1, 0), (1, 1)]
        if k == 0:
            return [tuple(across(a)[d] + s * across(b)[d] + t * across(c)[d] for d in range(3)) for s, t in tail]
        if k == 1:
            return [across(b), across(b, c)]
        return [across(c)] if k == 2 else [(0, 0, 0)]

    def stage(k, items, lhs, out, lag_b, lag_c, prepare=None, filler=None):
        count = (4, 2, 1, 1)[k]
        size = n1 if k == 0 else n2
        base = (0, 16, 24, 32)[k]
        locate = narrow if k == 0 else wide
        slots = lag_c + 1
        n_in = 1 + k
        from_ici = [(), ((2, 4),), ((1, 2), (5, 6)), ((0, 1), (4, 5), (6, 7))][k]

        def body(acc, term, staged):
            def columns(i):
                return lanes(locate(i)[2], size)

            def sources(i):
                region = (0, 4, 6, 7)[k]
                views = [d2d.at[pl.ds(region * shard, count * shard), columns(i)]]
                views += [ici.at[pl.ds(a * shard, (b - a) * shard), columns(i)] for a, b in from_ici]
                slot = lax.rem(i, slots)
                return [
                    pltpu.make_async_copy(view, staged.at[slot, n], stage_sem.at[slot * n_in + n]) for n, view in enumerate(views)
                ]

            def send(i):
                slot = lax.rem(i, slots)
                return exchange(k, i, count, size, columns(i), base, term.at[slot])

            def leave(i):
                if k < 3:
                    return onward(k, i, count, locate(i)[0], columns(i), base, out.at[i])
                return pltpu.make_async_copy(out.at[i], dx.at[:, columns(i)], dx_sem.at[i])

            def fetch(j):
                view = d2d.at[pl.ds(0, count * shard), columns(j)]
                remote(view, view, d2d_send.at[base + j], d2d_recv.at[base + j], place.sibling).wait_recv()
                p, t, start = locate(j)
                if k == 1:
                    for h in (0, 1):
                        n = unpick(p, 2 * t + h, 4)
                        view = ici.at[pl.ds(0, 4 * shard), lanes(start + h * n1, n1)]
                        remote(view, view, ici_send.at[n], ici_recv.at[n], place.sibling).wait_recv()
                elif k > 1:
                    n = (16, 24)[k - 2] + j
                    view = ici.at[pl.ds(0, (2, 1)[k - 2] * shard), columns(j)]
                    remote(view, view, ici_send.at[n], ici_recv.at[n], place.sibling).wait_recv()
                go(sources(j))

            def add(j, slot):
                total = acc[slot]
                for n in range(n_in):
                    total = total + staged[slot, n].astype(F32)
                out[j] = total.astype(BF16)

            @pl.loop(0, items)
            def _(i):
                p, _, start = locate(i)
                slot = lax.rem(i, slots)
                wait(narrow_weights(i) if k == 0 else wide_weights(i))
                if prepare is not None:
                    prepare(i)

                @pl.when(i >= slots)
                def _():
                    send(i - slots).wait_send()

                @pl.when(i >= lag_c)
                def _():
                    wait(sources(i - lag_c))

                add(lax.max(i - lag_c, 0), lax.rem(i + slots - lag_c, slots))
                if k == 0:
                    w = weights[rows(lax.rem(i, 4) * n1, n1), :]
                else:
                    w = weights[rows(lax.rem(i, 2) * n2, n2), :]
                value = dot(lhs[...] if k == 3 else lhs[p], w, NT)
                term[slot] = value[: count * shard].astype(BF16)
                acc[slot] = value[count * shard :]
                send(i).start()

                @pl.when(i >= lag_c)
                def _():
                    leave(i - lag_c).start()

                if k == 0:
                    @pl.when(i + 4 < items)
                    def _():
                        go(narrow_weights(i + 4))

                    @pl.when(i == items - 3)
                    def _():
                        go(wide_weights(0))

                    @pl.when(i == items - 1)
                    def _():
                        go(wide_weights(1))
                elif k < 3:
                    go(wide_weights(lax.rem(i + 2, 8)))
                else:
                    @pl.when(i + 2 < items)
                    def _():
                        go(wide_weights(i + 2))

                if filler is not None:
                    filler(i)

                @pl.when(i >= lag_b)
                def _():
                    fetch(i - lag_b)

            for j in range(items - lag_b, items):
                fetch(j)
            for j in range(items - lag_c, items):
                wait(sources(j))
                add(j, j % slots)
                leave(j).start()

            for i in range(max(items - slots, 0), items):
                send(i).wait_send()

        pl.run_scoped(
            body,
            pltpu.VMEM((slots, count * shard, size), F32),
            pltpu.VMEM((slots, count * shard, size), BF16),
            pltpu.VMEM((slots, n_in, count * shard, size), BF16),
        )

    loads2 = [c for p in range(3) for c in lhs_loads(lhs2, p, stage_chips(p, 1), 24 + 4 * p)]
    loads3 = [c for p in range(3) for c in lhs_loads(lhs3, p, stage_chips(p, 2), 36 + 2 * p)]
    loads4 = lhs_loads(lhs4, None, stage_chips(0, 3), 42)

    def main(right, right_sem):
        right_load = pltpu.make_async_copy(d_pre, right, right_sem.at[0])

        def first(lhs1):
            loads = [lhs_loads(lhs1, p, stage_chips(p, 0), 8 * p) for p in range(3)]
            for some in loads + [loads2, [right_load], loads3, loads4]:
                go(some)

            def prepare(i):
                for p in range(3):
                    @pl.when(i == p)
                    def _():
                        wait(loads[p])

            stage(0, 16, lhs1, out1, 1, 2, prepare=prepare)

        pl.run_scoped(first, pltpu.VMEM((3, 8 * shard, ff), BF16))

        def second(x_buf, dw_buf):
            def x_load(i):
                slot = lax.rem(i, 2)
                return pltpu.make_async_copy(x_all.at[:, lanes(i * n1, n1)], x_buf.at[slot], x_sem.at[slot])

            def dw_store(i):
                slot = lax.rem(i, 2)
                return pltpu.make_async_copy(dw_buf.at[slot], dw_in.at[rows(i * n1, n1)], dw_sem.at[slot])

            x_load(0).start()
            x_load(1).start()
            wait(loads2)
            right_load.wait()

            def tile(i):
                slot = lax.rem(i, 2)
                x_load(i).wait()

                @pl.when(i >= 2)
                def _():
                    dw_store(i - 2).wait()

                @pl.loop(0, 2)
                def _(h):
                    part = lanes(h * (ff // 2), ff // 2)
                    dw_buf[slot, :, part] = dot(x_buf[slot], right[:, part], TN).astype(BF16)

                dw_store(i).start()

                @pl.when(i + 2 < 8)
                def _():
                    x_load(i + 2).start()

            stage(1, 8, lhs2, out2, 0, 1, filler=tile)
            dw_store(6).wait()
            dw_store(7).wait()

        pl.run_scoped(second, pltpu.VMEM((2, tokens, n1), BF16), pltpu.VMEM((2, n1, ff), BF16))

    pl.run_scoped(main, pltpu.VMEM((tokens, ff), BF16), pltpu.SemaphoreType.DMA((1,)))
    def last(out3, out4):
        wait(loads3)
        wait(loads4)
        stage(2, 8, lhs3, out3, 2, 4)
        stage(3, 8, lhs4, out4, 2, 4)
        for i in range(16):
            onward(0, i, 4, narrow(i)[0], lanes(narrow(i)[2], n1), 0, out1.at[i]).wait_send()
        for i in range(8):
            onward(1, i, 2, wide(i)[0], lanes(wide(i)[2], n2), 16, out2.at[i]).wait_send()
            onward(2, i, 1, wide(i)[0], lanes(wide(i)[2], n2), 24, out3.at[i]).wait_send()
            pltpu.make_async_copy(out4.at[i], dx.at[:, lanes(wide(i)[2], n2)], dx_sem.at[i]).wait()

    pl.run_scoped(last, pltpu.VMEM((8, shard, n2), BF16), pltpu.VMEM((8, shard, n2), BF16))


def scatter(x_all, d_pre, w_in, shard):
    tokens, ff = d_pre.shape
    width = x_all.shape[1]
    n1, n2 = width // 16, width // 8
    dma, vmem = pltpu.SemaphoreType.DMA, pltpu.VMEM
    return pl.pallas_call(
        scatter_kernel,
        in_specs=[ANY] * 3,
        out_specs=[ANY] * 4,
        out_shape=[
            jax.ShapeDtypeStruct((shard, width), BF16),
            jax.ShapeDtypeStruct((width // 2, ff), BF16),
            jax.ShapeDtypeStruct((7 * shard, width), BF16),
            jax.ShapeDtypeStruct((8 * shard, width), BF16),
        ],
        scratch_shapes=[
            vmem((16, 4 * shard, n1), BF16),
            vmem((8, 2 * shard, n2), BF16),
            vmem((3, 4 * shard, ff), BF16),
            vmem((3, 2 * shard, ff), BF16),
            vmem((2 * shard, ff), BF16),
            vmem((4 * n1, ff), BF16),
            dma((32,)), dma((32,)), dma((40,)), dma((40,)), dma((4,)), dma((44,)), dma((20,)), dma((8,)), dma((2,)), dma((2,)),
        ],
        compiler_params=pltpu.CompilerParams(collective_id=1, has_side_effects=True, vmem_limit_bytes=VMEM_LIMIT),
        cost_estimate=pl.CostEstimate(flops=3 * tokens * ff * width, bytes_accessed=400_000_000, transcendentals=0),
        name="scatter_dx",
    )(x_all, d_pre, w_in)[:2]


def finish_kernel(x_ref, d_pre_ref, part_ref, down_ref, dw_in, dw_down, buf, copy_sem, buf_sem):
    i = pl.program_id(0)
    n, ff = part_ref.shape
    count = pl.num_programs(0)
    slot = lax.rem(i, 2)
    copies = [
        pltpu.make_async_copy(part_ref, dw_in.at[rows(i * n, n)], copy_sem.at[0]),
        pltpu.make_async_copy(down_ref, dw_down.at[rows(i * down_ref.shape[0], down_ref.shape[0])], copy_sem.at[1]),
    ]

    def store(i):
        slot = lax.rem(i, 2)
        return pltpu.make_async_copy(buf.at[slot], dw_in.at[rows((count + i) * n, n)], buf_sem.at[slot])

    for copy in copies:
        copy.start()

    @pl.when(i >= 2)
    def _():
        store(i - 2).wait()

    @pl.loop(0, 2)
    def _(h):
        half = lanes(h * (ff // 2), ff // 2)
        buf[slot, :, half] = dot(x_ref[...], d_pre_ref[:, half], TN).astype(BF16)

    store(i).start()
    for copy in copies:
        copy.wait()

    @pl.when(i == count - 1)
    def _():
        store(i - 1).wait()
        store(i).wait()


def finish(x_all, d_pre, dw_in_part, dw_down_part):
    tokens, ff = d_pre.shape
    width = x_all.shape[1]
    n = width // 16
    return pl.pallas_call(
        finish_kernel,
        grid=(8,),
        in_specs=[
            pl.BlockSpec((tokens, n), lambda i: (0, 8 + i)),
            pl.BlockSpec((tokens, ff), lambda i: (0, 0)),
            pl.BlockSpec((n, ff), lambda i: (i, 0)),
            pl.BlockSpec((ff // 8, width), lambda i: (i, 0)),
        ],
        out_specs=[ANY] * 2,
        out_shape=[jax.ShapeDtypeStruct((width, ff), BF16), jax.ShapeDtypeStruct((ff, width), BF16)],
        scratch_shapes=[pltpu.VMEM((2, n, ff), BF16), pltpu.SemaphoreType.DMA((2,)), pltpu.SemaphoreType.DMA((2,))],
        compiler_params=pltpu.CompilerParams(dimension_semantics=("arbitrary",), vmem_limit_bytes=VMEM_LIMIT),
        cost_estimate=pl.CostEstimate(flops=tokens * ff * width, bytes_accessed=140_000_000, transcendentals=0),
        name="finish",
    )(x_all, d_pre, dw_in_part, dw_down_part)


def solution(mesh):
    def body(x, dy, pre, w_in, w_down):
        x_all, _, d_pre, _, _, dw_down = forward(x, dy, pre, w_down)
        dx, dw_in = scatter(x_all, d_pre, w_in, x.shape[0])
        dw_in, dw_down = finish(x_all, d_pre, dw_in, dw_down)
        return dx, dw_in, dw_down

    return jax.shard_map(
        body,
        mesh=mesh,
        in_specs=(P(("dp", "tp")), P(("dp", "tp")), P("dp", "tp"), P(None, "tp"), P("tp", None)),
        out_specs=(P(("dp", "tp")), P("dp", "tp"), P(("dp", "tp"))),
        check_vma=False,
    )
```

```python
import functools

import jax
import jax.numpy as jnp
from jax import lax
from jax.experimental import pallas as pl
from jax.experimental.pallas import tpu as pltpu
from jax.sharding import PartitionSpec as P

VMEM_LIMIT = 66_000_000
WEIGHT = (4, 2, 1)
F32, BF16 = jnp.float32, jnp.bfloat16
ANY = pl.BlockSpec(memory_space=pl.ANY)
CHIPS = [(a, b, c) for a in (0, 1) for b in (0, 1) for c in (0, 1)]


def act(pre):
    return jax.nn.gelu(pre)


def dot(a, b, dims):
    return lax.dot_general(a, b, (dims, ((), ())), preferred_element_type=F32)


NT, TN = ((1,), (1,)), ((0,), (0,))


def rows(start, size):
    return pl.ds(pl.multiple_of(start, 16), size)


def lanes(start, size):
    return pl.ds(pl.multiple_of(start, 128), size)


class Place:
    def __init__(self):
        me = lax.axis_index("tp")
        self.chip, self.core = lax.div(me, 2), lax.rem(me, 2)
        self.step = [w * (1 - 2 * lax.rem(lax.div(self.chip, w), 2)) for w in WEIGHT]
        self.sibling = self.device(self.chip, 1 - self.core)

    def chip_at(self, r):
        return self.chip + sum(self.step[d] * r[d] for d in range(3) if isinstance(r[d], jax.Array) or r[d])

    def device(self, chip, core):
        return {"tp": 2 * chip + core}

    def across(self, d):
        if isinstance(d, int):
            return self.device(self.chip + self.step[d], self.core)
        r = (lax.div(2 - d, 2), lax.rem(d, 2), lax.div(d, 2))
        return self.device(self.chip_at(r), self.core)

    def barrier(self):
        sem = pltpu.get_barrier_semaphore()
        for peer in [self.sibling] + [self.across(d) for d in range(3)]:
            pl.semaphore_signal(sem, inc=1, device_id=peer, device_id_type=pl.DeviceIdType.MESH)
        pl.semaphore_wait(sem, 4)


def remote(src, dst, send, recv, device):
    return pltpu.make_async_remote_copy(src, dst, send, recv, device_id=device, device_id_type=pl.DeviceIdType.MESH)


def order(p):
    return p, (p + 1) % 3, (p + 2) % 3


def across(*dims):
    return tuple(int(d in dims) for d in range(3))


class Gather:
    def __init__(self, place, src, dst, sems, base, halves):
        self.place, self.src, self.dst, self.halves = place, src, dst, halves
        self.shard, width = src.shape
        self.size = self.shard // halves
        self.send, self.recv, self.out, self.back = (functools.partial(lambda s, i: s.at[base + i], s) for s in sems)
        tiles = width // 128
        ends = [128 * (tiles * k // 3) for k in range(4)]
        self.columns = [pl.ds(ends[k], ends[k + 1] - ends[k]) for k in range(3)]

    def rows_of(self, r, core, h=None):
        start = (2 * self.place.chip_at(r) + core) * self.shard
        return rows(start, self.shard) if h is None else rows(start + h * self.size, self.size)

    def piece(self, p, r, core, h):
        return self.dst.at[self.rows_of(r, core, h), self.columns[p]]

    @staticmethod
    def index(p, r, h):
        return 24 * h + 8 * p + 4 * r[0] + 2 * r[1] + r[2]

    def hop(self, p, r, h):
        d = [d for d in order(p) if r[d]][-1]
        q = tuple(r[e] * (e != d) for e in range(3))
        dst = self.piece(p, q, self.place.core, h)
        src = dst if any(q) else self.src.at[pl.ds(h * self.size, self.size), self.columns[p]]
        i = self.index(p, r, h)
        return remote(src, dst, self.send(i), self.recv(i), self.place.across(d))

    def arrive(self, p, r, h):
        view, i = self.piece(p, r, self.place.core, h), self.index(p, r, h)
        remote(view, view, self.send(i), self.recv(i), self.place.sibling).wait_recv()

    def share(self, p, r, h):
        view, i = self.piece(p, r, self.place.core, h), self.index(p, r, h)
        return remote(view, view, self.out(i), self.back(i), self.place.sibling)

    def shared(self, p, r, h):
        view, i = self.piece(p, r, 1 - self.place.core, h), self.index(p, r, h)
        remote(view, view, self.out(i), self.back(i), self.place.sibling).wait_recv()

    def share_own(self):
        return remote(self.src, self.dst.at[self.rows_of((0, 0, 0), self.place.core)], self.out(0), self.back(0), self.place.sibling)

    def shared_own(self):
        view = self.dst.at[self.rows_of((0, 0, 0), 1 - self.place.core)]
        remote(view, view, self.out(0), self.back(0), self.place.sibling).wait_recv()

    def shared_all(self, chips, h):
        for p in range(3):
            for r in chips:
                self.shared(p, r, h)

    def begin(self):
        self.share_own().start()
        for h in range(self.halves):
            for k in range(3):
                for d in range(3):
                    self.hop((d - k) % 3, across(d), h).start()

    def act(self, n, h=0):
        for p in range(3):
            a, b, c = order(p)
            seq = [across(a), across(b), across(c), across(a, b), across(a, c), across(b, c), across(a, b, c)]
            follow = {0: [across(a, b), across(a, c)], 1: [across(b, c)], 3: [across(a, b, c)]}
            self.arrive(p, seq[n], h)
            for r in follow.get(n, []):
                self.hop(p, r, h).start()
            self.share(p, seq[n], h).start()

    def drain(self):
        self.share_own().wait_send()
        for h in range(self.halves):
            for p in range(3):
                for r in CHIPS[1:]:
                    self.hop(p, r, h).wait_send()
                    self.share(p, r, h).wait_send()


NEAR = [(1, 0, 0), (0, 1, 0), (0, 0, 1)]
MIDDLE = [(1, 1, 0), (0, 1, 1), (1, 0, 1)]
FAR = [(1, 1, 1)]
HERE = [(0, 0, 0)]


def forward_kernel(x, dy, pre, w_down, x_all, dy_all, d_pre, hidden, slope, dw_down, send, recv, out, back, w_sem, load_sem, store_sem, own_sem):
    place = Place()
    shard, width = dy.shape
    half = shard // 2
    tokens, ff = pre.shape
    block = ff // 4
    place.barrier()
    sems = (send, recv, out, back)
    gather_dy = Gather(place, dy, dy_all, sems, 0, 2)
    gather_x = Gather(place, x, x_all, sems, 48, 1)
    gather_dy.begin()
    mine = gather_dy.rows_of(HERE[0], place.core)

    def gradient(weights):
        def load_weights(j):
            part = pl.ds(j * block, block)
            return pltpu.make_async_copy(w_down.at[part], weights.at[part], w_sem.at[j])

        for j in range(4):
            load_weights(j).start()

        def before(x_buf):
            taken = pltpu.make_async_copy(x, x_buf, own_sem.at[0])
            taken.start()

            def gelu(pre_ref, hidden_ref, slope_ref):
                value, pull = jax.vjp(act, pre_ref[...].astype(F32))
                hidden_ref[...] = value.astype(BF16)
                slope_ref[...] = pull(jnp.ones_like(value))[0]

            spec = pl.BlockSpec((shard, ff), lambda i: (i, 0))
            pltpu.emit_pipeline(gelu, grid=(tokens // shard,), in_specs=[spec], out_specs=[spec, spec])(pre, hidden, slope)
            taken.wait()
            put = pltpu.make_async_copy(x_buf, x_all.at[mine], own_sem.at[1])
            put.start()
            for n in range(3):
                gather_dy.act(n, 0)
            gather_dy.shared_own()
            put.wait()

        pl.run_scoped(before, pltpu.VMEM((shard, width), BF16))

        def chunks(lhs, slopes, result):
            batches = [(HERE, None), (NEAR, 0), (NEAR, 1), (MIDDLE, 0), (MIDDLE, 1), (FAR, None)]

            def parts(n):
                chips, h = batches[n]
                size = shard if h is None else half
                cores = (place.core, 1 - place.core)
                return [(gather_dy.rows_of(r, c, h), pl.ds(k * size, size)) for k, (r, c) in enumerate((r, c) for r in chips for c in cores)]

            def rows_in(n):
                return sum(part.size for _, part in parts(n))

            def loads(n):
                copies = []
                for k, (src, part) in enumerate(parts(n)):
                    at = 12 * (n % 2) + k
                    there = dy if (n == 0 and k == 0) else dy_all.at[src]
                    copies.append(pltpu.make_async_copy(there, lhs.at[n % 2, part], load_sem.at[at]))
                    copies.append(pltpu.make_async_copy(slope.at[src], slopes.at[n % 2, part], load_sem.at[at + 6]))
                return copies

            def stores(n):
                return [
                    pltpu.make_async_copy(result.at[n % 2, part], d_pre.at[dst], store_sem.at[6 * (n % 2) + k])
                    for k, (dst, part) in enumerate(parts(n))
                ]

            own = pltpu.make_async_copy(lhs.at[0, pl.ds(0, shard)], dy_all.at[mine], own_sem.at[0])

            def ready(n):
                chips, h = batches[n]
                if n == 2:
                    for k in range(3):
                        gather_dy.act(k, 1)
                if n in (3, 4):
                    for k in (3, 4, 5):
                        gather_dy.act(k, h)
                if n == 5:
                    gather_dy.act(6, 0)
                    gather_dy.act(6, 1)
                for h in (0, 1) if h is None else (h,):
                    gather_dy.shared_all(chips, h)
                if n == 2:
                    own.wait()
                for copy in loads(n):
                    copy.start()

            when = (2, 3, 4, 4, 3)
            for copy in loads(0):
                copy.start()
            for n in range(6):
                for copy in loads(n):
                    copy.wait()
                if n == 0:
                    own.start()
                    for j in range(4):
                        load_weights(j).wait()
                if n >= 2:
                    for copy in stores(n - 2):
                        copy.wait()
                size, slot = rows_in(n), n % 2

                @pl.loop(0, 4)
                def _(j):
                    if n < 5 and when[n] < 4:
                        @pl.when(j == when[n])
                        def _():
                            ready(n + 1)

                    columns = lanes(j * block, block)
                    d_hidden = dot(lhs[slot, :size], weights[rows(j * block, block), :], NT)
                    result[slot, :size, columns] = (d_hidden * slopes[slot, :size, columns]).astype(BF16)

                for copy in stores(n):
                    copy.start()
                if n < 5 and when[n] == 4:
                    ready(n + 1)
                if n == 3:
                    gather_x.begin()
            for n in (4, 5):
                for copy in stores(n):
                    copy.wait()

        pl.run_scoped(chunks, pltpu.VMEM((2, 6 * half, width), BF16), pltpu.VMEM((2, 6 * half, ff), F32), pltpu.VMEM((2, 6 * half, ff), BF16))

    pl.run_scoped(gradient, pltpu.VMEM((ff, width), BF16))

    tm, tn = ff // 2, width // 8

    def product(h_ref, dy_ref, o_ref):
        at = pl.program_id(0) * 8 + pl.program_id(1)
        for n, when in enumerate((1, 4, 7, 10, 13, 15)):
            @pl.when(at == when)
            def _():
                gather_x.act(n)

        o_ref[...] = dot(h_ref[...], dy_ref[...], TN).astype(BF16)

    pltpu.emit_pipeline(
        product,
        grid=(2, 8),
        in_specs=[pl.BlockSpec((tokens, tm), lambda i, j: (0, i)), pl.BlockSpec((tokens, tn), lambda i, j: (0, j))],
        out_specs=[pl.BlockSpec((tm, tn), lambda i, j: (i, j))],
    )(hidden, dy_all, dw_down)
    gather_x.act(6)
    gather_x.shared_own()
    gather_x.shared_all(CHIPS[1:], 0)
    gather_dy.drain()
    gather_x.drain()


def forward(x, dy, pre, w_down):
    shard, width = dy.shape
    tokens, ff = pre.shape
    dma = pltpu.SemaphoreType.DMA
    whole = jax.ShapeDtypeStruct((tokens, width), BF16)
    return pl.pallas_call(
        forward_kernel,
        in_specs=[ANY] * 4,
        out_specs=[ANY] * 6,
        out_shape=[
            whole,
            whole,
            jax.ShapeDtypeStruct((tokens, ff), BF16),
            jax.ShapeDtypeStruct((tokens, ff), BF16),
            jax.ShapeDtypeStruct((tokens, ff), F32),
            jax.ShapeDtypeStruct((ff, width), BF16),
        ],
        scratch_shapes=[dma((72,)), dma((72,)), dma((72,)), dma((72,)), dma((4,)), dma((24,)), dma((12,)), dma((2,))],
        compiler_params=pltpu.CompilerParams(collective_id=0, has_side_effects=True, vmem_limit_bytes=VMEM_LIMIT),
        cost_estimate=pl.CostEstimate(flops=4 * tokens * ff * width, bytes_accessed=400_000_000, transcendentals=tokens * ff),
        name="gather_gradient",
    )(x, dy, pre, w_down)


def scatter_kernel(x_all, d_pre, w_in, dx, dw_in, ici, d2d, out1, out2, lhs2, lhs3, lhs4, weights,
                   ici_send, ici_recv, d2d_send, d2d_recv, w_sem, load_sem, stage_sem, dx_sem, x_sem, dw_sem):
    place = Place()
    chip, core = place.chip, place.core
    shard, width = dx.shape
    tokens, ff = d_pre.shape
    n1, n2 = width // 16, width // 8

    def pick(i, group):
        k = lax.div(i, 3 * group)
        p = (1 - k) * lax.rem(i, 3) + k * lax.rem(i, 2)
        t = (1 - k) * lax.div(i, 3) + k * (group + lax.div(i - 3 * group, 2))
        return p, t

    def unpick(p, t, group):
        k = lax.div(t, group)
        return (1 - k) * (3 * t + p) + k * (3 * group + 2 * (t - group) + p)

    def turn(p, k):
        return lax.rem(p + k, 3)

    def narrow(i):
        p, t = pick(i, 4)
        return p, t, p * (3 * n2) + t * n1

    def wide(i):
        p, t = pick(i, 2)
        return p, t, p * (3 * n2) + t * n2

    def narrow_weights(i):
        slot = lax.rem(i, 4)
        return [pltpu.make_async_copy(w_in.at[rows(narrow(i)[2], n1)], weights.at[rows(slot * n1, n1)], w_sem.at[slot])]

    def wide_weights(i):
        start, slot = wide(i)[2], lax.rem(i, 2)
        return [
            pltpu.make_async_copy(w_in.at[rows(start + h * n1, n1)], weights.at[rows(slot * n2 + h * n1, n1)], w_sem.at[2 * slot + h])
            for h in (0, 1)
        ]

    def go(copies):
        for copy in copies:
            copy.start()

    def wait(copies):
        for copy in copies:
            copy.wait()

    def lhs_loads(ref, p, chips, base):
        loads = []
        for half, c in enumerate((1 - core, core)):
            for k, r in enumerate(chips):
                src = d_pre.at[rows((2 * place.chip_at(r) + c) * shard, shard)]
                n = half * len(chips) + k
                view = ref if p is None else ref.at[p]
                loads.append(pltpu.make_async_copy(src, view.at[pl.ds(n * shard, shard)], load_sem.at[base + n]))
        return loads

    place.barrier()
    for i in range(4):
        go(narrow_weights(i))

    def exchange(k, i, count, size, columns, base, part):
        region = (0, 4, 6, 7)[k]
        dst = d2d.at[pl.ds(region * shard, count * shard), columns]
        return remote(part, dst, d2d_send.at[base + i], d2d_recv.at[base + i], place.sibling)

    def onward(k, i, count, p, columns, base, part):
        region = (0, 4, 6)[k]
        dst = ici.at[pl.ds(region * shard, count * shard), columns]
        return remote(part, dst, ici_send.at[base + i], ici_recv.at[base + i], place.across(turn(p, k)))

    def stage_chips(p, k):
        a, b, c = order(p)
        tail = [(0, 0), (0, 1), (1, 0), (1, 1)]
        if k == 0:
            return [tuple(across(a)[d] + s * across(b)[d] + t * across(c)[d] for d in range(3)) for s, t in tail]
        if k == 1:
            return [across(b), across(b, c)]
        return [across(c)] if k == 2 else [(0, 0, 0)]

    def stage(k, items, lhs, out, lag_b, lag_c, prepare=None, filler=None):
        count = (4, 2, 1, 1)[k]
        size = n1 if k == 0 else n2
        base = (0, 16, 24, 32)[k]
        locate = narrow if k == 0 else wide
        slots = lag_c + 1
        n_in = 1 + k
        from_ici = [(), ((2, 4),), ((1, 2), (5, 6)), ((0, 1), (4, 5), (6, 7))][k]

        def body(acc, term, staged):
            def columns(i):
                return lanes(locate(i)[2], size)

            def sources(i):
                region = (0, 4, 6, 7)[k]
                views = [d2d.at[pl.ds(region * shard, count * shard), columns(i)]]
                views += [ici.at[pl.ds(a * shard, (b - a) * shard), columns(i)] for a, b in from_ici]
                slot = lax.rem(i, slots)
                return [
                    pltpu.make_async_copy(view, staged.at[slot, n], stage_sem.at[slot * n_in + n]) for n, view in enumerate(views)
                ]

            def send(i):
                slot = lax.rem(i, slots)
                return exchange(k, i, count, size, columns(i), base, term.at[slot])

            def leave(i):
                if k < 3:
                    return onward(k, i, count, locate(i)[0], columns(i), base, out.at[i])
                return pltpu.make_async_copy(out.at[i], dx.at[:, columns(i)], dx_sem.at[i])

            def fetch(j):
                view = d2d.at[pl.ds(0, count * shard), columns(j)]
                remote(view, view, d2d_send.at[base + j], d2d_recv.at[base + j], place.sibling).wait_recv()
                p, t, start = locate(j)
                if k == 1:
                    for h in (0, 1):
                        n = unpick(p, 2 * t + h, 4)
                        view = ici.at[pl.ds(0, 4 * shard), lanes(start + h * n1, n1)]
                        remote(view, view, ici_send.at[n], ici_recv.at[n], place.sibling).wait_recv()
                elif k > 1:
                    n = (16, 24)[k - 2] + j
                    view = ici.at[pl.ds(0, (2, 1)[k - 2] * shard), columns(j)]
                    remote(view, view, ici_send.at[n], ici_recv.at[n], place.sibling).wait_recv()
                go(sources(j))

            def add(j, slot):
                total = acc[slot]
                for n in range(n_in):
                    total = total + staged[slot, n].astype(F32)
                out[j] = total.astype(BF16)

            @pl.loop(0, items)
            def _(i):
                p, _, start = locate(i)
                slot = lax.rem(i, slots)
                wait(narrow_weights(i) if k == 0 else wide_weights(i))
                if prepare is not None:
                    prepare(i)

                @pl.when(i >= slots)
                def _():
                    send(i - slots).wait_send()

                @pl.when(i >= lag_c)
                def _():
                    wait(sources(i - lag_c))

                add(lax.max(i - lag_c, 0), lax.rem(i + slots - lag_c, slots))
                if k == 0:
                    w = weights[rows(lax.rem(i, 4) * n1, n1), :]
                else:
                    w = weights[rows(lax.rem(i, 2) * n2, n2), :]
                value = dot(lhs[...] if k == 3 else lhs[p], w, NT)
                term[slot] = value[: count * shard].astype(BF16)
                acc[slot] = value[count * shard :]
                send(i).start()

                @pl.when(i >= lag_c)
                def _():
                    leave(i - lag_c).start()

                if k == 0:
                    @pl.when(i + 4 < items)
                    def _():
                        go(narrow_weights(i + 4))

                    @pl.when(i == items - 3)
                    def _():
                        go(wide_weights(0))

                    @pl.when(i == items - 1)
                    def _():
                        go(wide_weights(1))
                elif k < 3:
                    go(wide_weights(lax.rem(i + 2, 8)))
                else:
                    @pl.when(i + 2 < items)
                    def _():
                        go(wide_weights(i + 2))

                if filler is not None:
                    filler(i)

                @pl.when(i >= lag_b)
                def _():
                    fetch(i - lag_b)

            for j in range(items - lag_b, items):
                fetch(j)
            for j in range(items - lag_c, items):
                wait(sources(j))
                add(j, j % slots)
                leave(j).start()

            for i in range(max(items - slots, 0), items):
                send(i).wait_send()

        pl.run_scoped(
            body,
            pltpu.VMEM((slots, count * shard, size), F32),
            pltpu.VMEM((slots, count * shard, size), BF16),
            pltpu.VMEM((slots, n_in, count * shard, size), BF16),
        )

    loads2 = [c for p in range(3) for c in lhs_loads(lhs2, p, stage_chips(p, 1), 24 + 4 * p)]
    loads3 = [c for p in range(3) for c in lhs_loads(lhs3, p, stage_chips(p, 2), 36 + 2 * p)]
    loads4 = lhs_loads(lhs4, None, stage_chips(0, 3), 42)

    def main(right, right_sem):
        right_load = pltpu.make_async_copy(d_pre, right, right_sem.at[0])

        def first(lhs1):
            loads = [lhs_loads(lhs1, p, stage_chips(p, 0), 8 * p) for p in range(3)]
            for some in loads + [loads2, [right_load], loads3, loads4]:
                go(some)

            def prepare(i):
                for p in range(3):
                    @pl.when(i == p)
                    def _():
                        wait(loads[p])

            stage(0, 16, lhs1, out1, 1, 3, prepare=prepare)

        pl.run_scoped(first, pltpu.VMEM((3, 8 * shard, ff), BF16))

        def second(x_buf, dw_buf):
            def x_load(i):
                slot = lax.rem(i, 2)
                return pltpu.make_async_copy(x_all.at[:, lanes(i * n1, n1)], x_buf.at[slot], x_sem.at[slot])

            def dw_store(i):
                slot = lax.rem(i, 2)
                return pltpu.make_async_copy(dw_buf.at[slot], dw_in.at[rows(i * n1, n1)], dw_sem.at[slot])

            x_load(0).start()
            x_load(1).start()
            wait(loads2)
            right_load.wait()

            def tile(i):
                slot = lax.rem(i, 2)
                x_load(i).wait()

                @pl.when(i >= 2)
                def _():
                    dw_store(i - 2).wait()

                @pl.loop(0, 2)
                def _(h):
                    part = lanes(h * (ff // 2), ff // 2)
                    dw_buf[slot, :, part] = dot(x_buf[slot], right[:, part], TN).astype(BF16)

                dw_store(i).start()

                @pl.when(i + 2 < 8)
                def _():
                    x_load(i + 2).start()

            stage(1, 8, lhs2, out2, 0, 2, filler=tile)
            dw_store(6).wait()
            dw_store(7).wait()

        pl.run_scoped(second, pltpu.VMEM((2, tokens, n1), BF16), pltpu.VMEM((2, n1, ff), BF16))

    pl.run_scoped(main, pltpu.VMEM((tokens, ff), BF16), pltpu.SemaphoreType.DMA((1,)))
    def last(out3, out4):
        wait(loads3)
        wait(loads4)
        stage(2, 8, lhs3, out3, 2, 5)
        stage(3, 8, lhs4, out4, 2, 5)
        for i in range(16):
            onward(0, i, 4, narrow(i)[0], lanes(narrow(i)[2], n1), 0, out1.at[i]).wait_send()
        for i in range(8):
            onward(1, i, 2, wide(i)[0], lanes(wide(i)[2], n2), 16, out2.at[i]).wait_send()
            onward(2, i, 1, wide(i)[0], lanes(wide(i)[2], n2), 24, out3.at[i]).wait_send()
            pltpu.make_async_copy(out4.at[i], dx.at[:, lanes(wide(i)[2], n2)], dx_sem.at[i]).wait()

    pl.run_scoped(last, pltpu.VMEM((8, shard, n2), BF16), pltpu.VMEM((8, shard, n2), BF16))


def scatter(x_all, d_pre, w_in, shard):
    tokens, ff = d_pre.shape
    width = x_all.shape[1]
    n1, n2 = width // 16, width // 8
    dma, vmem = pltpu.SemaphoreType.DMA, pltpu.VMEM
    return pl.pallas_call(
        scatter_kernel,
        in_specs=[ANY] * 3,
        out_specs=[ANY] * 4,
        out_shape=[
            jax.ShapeDtypeStruct((shard, width), BF16),
            jax.ShapeDtypeStruct((width // 2, ff), BF16),
            jax.ShapeDtypeStruct((7 * shard, width), BF16),
            jax.ShapeDtypeStruct((8 * shard, width), BF16),
        ],
        scratch_shapes=[
            vmem((16, 4 * shard, n1), BF16),
            vmem((8, 2 * shard, n2), BF16),
            vmem((3, 4 * shard, ff), BF16),
            vmem((3, 2 * shard, ff), BF16),
            vmem((2 * shard, ff), BF16),
            vmem((4 * n1, ff), BF16),
            dma((32,)), dma((32,)), dma((40,)), dma((40,)), dma((4,)), dma((44,)), dma((24,)), dma((8,)), dma((2,)), dma((2,)),
        ],
        compiler_params=pltpu.CompilerParams(collective_id=1, has_side_effects=True, vmem_limit_bytes=VMEM_LIMIT),
        cost_estimate=pl.CostEstimate(flops=3 * tokens * ff * width, bytes_accessed=400_000_000, transcendentals=0),
        name="scatter_dx",
    )(x_all, d_pre, w_in)[:2]


def finish_kernel(x_ref, d_pre_ref, part_ref, down_ref, dw_in, dw_down, buf, copy_sem, buf_sem):
    i = pl.program_id(0)
    n, ff = part_ref.shape
    count = pl.num_programs(0)
    slot = lax.rem(i, 2)
    copies = [
        pltpu.make_async_copy(part_ref, dw_in.at[rows(i * n, n)], copy_sem.at[0]),
        pltpu.make_async_copy(down_ref, dw_down.at[rows(i * down_ref.shape[0], down_ref.shape[0])], copy_sem.at[1]),
    ]

    def store(i):
        slot = lax.rem(i, 2)
        return pltpu.make_async_copy(buf.at[slot], dw_in.at[rows((count + i) * n, n)], buf_sem.at[slot])

    for copy in copies:
        copy.start()

    @pl.when(i >= 2)
    def _():
        store(i - 2).wait()

    @pl.loop(0, 2)
    def _(h):
        half = lanes(h * (ff // 2), ff // 2)
        buf[slot, :, half] = dot(x_ref[...], d_pre_ref[:, half], TN).astype(BF16)

    store(i).start()
    for copy in copies:
        copy.wait()

    @pl.when(i == count - 1)
    def _():
        store(i - 1).wait()
        store(i).wait()


def finish(x_all, d_pre, dw_in_part, dw_down_part):
    tokens, ff = d_pre.shape
    width = x_all.shape[1]
    n = width // 16
    return pl.pallas_call(
        finish_kernel,
        grid=(8,),
        in_specs=[
            pl.BlockSpec((tokens, n), lambda i: (0, 8 + i)),
            pl.BlockSpec((tokens, ff), lambda i: (0, 0)),
            pl.BlockSpec((n, ff), lambda i: (i, 0)),
            pl.BlockSpec((ff // 8, width), lambda i: (i, 0)),
        ],
        out_specs=[ANY] * 2,
        out_shape=[jax.ShapeDtypeStruct((width, ff), BF16), jax.ShapeDtypeStruct((ff, width), BF16)],
        scratch_shapes=[pltpu.VMEM((2, n, ff), BF16), pltpu.SemaphoreType.DMA((2,)), pltpu.SemaphoreType.DMA((2,))],
        compiler_params=pltpu.CompilerParams(dimension_semantics=("arbitrary",), vmem_limit_bytes=VMEM_LIMIT),
        cost_estimate=pl.CostEstimate(flops=tokens * ff * width, bytes_accessed=140_000_000, transcendentals=0),
        name="finish",
    )(x_all, d_pre, dw_in_part, dw_down_part)


def solution(mesh):
    def body(x, dy, pre, w_in, w_down):
        x_all, _, d_pre, _, _, dw_down = forward(x, dy, pre, w_down)
        dx, dw_in = scatter(x_all, d_pre, w_in, x.shape[0])
        dw_in, dw_down = finish(x_all, d_pre, dw_in, dw_down)
        return dx, dw_in, dw_down

    return jax.shard_map(
        body,
        mesh=mesh,
        in_specs=(P(("dp", "tp")), P(("dp", "tp")), P("dp", "tp"), P(None, "tp"), P("tp", None)),
        out_specs=(P(("dp", "tp")), P("dp", "tp"), P(("dp", "tp"))),
        check_vma=False,
    )
```

```python
import functools

import jax
import jax.numpy as jnp
from jax import lax
from jax.experimental import pallas as pl
from jax.experimental.pallas import tpu as pltpu
from jax.sharding import PartitionSpec as P

VMEM_LIMIT = 67_000_000
WEIGHT = (4, 2, 1)
F32, BF16 = jnp.float32, jnp.bfloat16
ANY = pl.BlockSpec(memory_space=pl.ANY)
CHIPS = [(a, b, c) for a in (0, 1) for b in (0, 1) for c in (0, 1)]


def act(pre):
    return jax.nn.gelu(pre)


def dot(a, b, dims):
    return lax.dot_general(a, b, (dims, ((), ())), preferred_element_type=F32)


NT, TN = ((1,), (1,)), ((0,), (0,))


def rows(start, size):
    return pl.ds(pl.multiple_of(start, 16), size)


def lanes(start, size):
    return pl.ds(pl.multiple_of(start, 128), size)


class Place:
    def __init__(self):
        me = lax.axis_index("tp")
        self.chip, self.core = lax.div(me, 2), lax.rem(me, 2)
        self.step = [w * (1 - 2 * lax.rem(lax.div(self.chip, w), 2)) for w in WEIGHT]
        self.sibling = self.device(self.chip, 1 - self.core)

    def chip_at(self, r):
        return self.chip + sum(self.step[d] * r[d] for d in range(3) if isinstance(r[d], jax.Array) or r[d])

    def device(self, chip, core):
        return {"tp": 2 * chip + core}

    def across(self, d):
        if isinstance(d, int):
            return self.device(self.chip + self.step[d], self.core)
        r = (lax.div(2 - d, 2), lax.rem(d, 2), lax.div(d, 2))
        return self.device(self.chip_at(r), self.core)

    def barrier(self):
        sem = pltpu.get_barrier_semaphore()
        for peer in [self.sibling] + [self.across(d) for d in range(3)]:
            pl.semaphore_signal(sem, inc=1, device_id=peer, device_id_type=pl.DeviceIdType.MESH)
        pl.semaphore_wait(sem, 4)


def remote(src, dst, send, recv, device):
    return pltpu.make_async_remote_copy(src, dst, send, recv, device_id=device, device_id_type=pl.DeviceIdType.MESH)


def order(p):
    return p, (p + 1) % 3, (p + 2) % 3


def across(*dims):
    return tuple(int(d in dims) for d in range(3))


class Gather:
    def __init__(self, place, src, dst, sems, base, halves):
        self.place, self.src, self.dst, self.halves = place, src, dst, halves
        self.shard, width = src.shape
        self.size = self.shard // halves
        self.send, self.recv, self.out, self.back = (functools.partial(lambda s, i: s.at[base + i], s) for s in sems)
        tiles = width // 128
        ends = [128 * (tiles * k // 3) for k in range(4)]
        self.columns = [pl.ds(ends[k], ends[k + 1] - ends[k]) for k in range(3)]

    def rows_of(self, r, core, h=None):
        start = (2 * self.place.chip_at(r) + core) * self.shard
        return rows(start, self.shard) if h is None else rows(start + h * self.size, self.size)

    def piece(self, p, r, core, h):
        return self.dst.at[self.rows_of(r, core, h), self.columns[p]]

    @staticmethod
    def index(p, r, h):
        return 24 * h + 8 * p + 4 * r[0] + 2 * r[1] + r[2]

    def hop(self, p, r, h):
        d = [d for d in order(p) if r[d]][-1]
        q = tuple(r[e] * (e != d) for e in range(3))
        dst = self.piece(p, q, self.place.core, h)
        src = dst if any(q) else self.src.at[pl.ds(h * self.size, self.size), self.columns[p]]
        i = self.index(p, r, h)
        return remote(src, dst, self.send(i), self.recv(i), self.place.across(d))

    def arrive(self, p, r, h):
        view, i = self.piece(p, r, self.place.core, h), self.index(p, r, h)
        remote(view, view, self.send(i), self.recv(i), self.place.sibling).wait_recv()

    def share(self, p, r, h):
        view, i = self.piece(p, r, self.place.core, h), self.index(p, r, h)
        return remote(view, view, self.out(i), self.back(i), self.place.sibling)

    def shared(self, p, r, h):
        view, i = self.piece(p, r, 1 - self.place.core, h), self.index(p, r, h)
        remote(view, view, self.out(i), self.back(i), self.place.sibling).wait_recv()

    def share_own(self):
        return remote(self.src, self.dst.at[self.rows_of((0, 0, 0), self.place.core)], self.out(0), self.back(0), self.place.sibling)

    def shared_own(self):
        view = self.dst.at[self.rows_of((0, 0, 0), 1 - self.place.core)]
        remote(view, view, self.out(0), self.back(0), self.place.sibling).wait_recv()

    def shared_all(self, chips, h):
        for p in range(3):
            for r in chips:
                self.shared(p, r, h)

    def begin(self):
        self.share_own().start()
        for h in range(self.halves):
            for k in range(3):
                for d in range(3):
                    self.hop((d - k) % 3, across(d), h).start()

    def act(self, n, h=0):
        for p in range(3):
            a, b, c = order(p)
            seq = [across(a), across(b), across(c), across(a, b), across(a, c), across(b, c), across(a, b, c)]
            follow = {0: [across(a, b), across(a, c)], 1: [across(b, c)], 3: [across(a, b, c)]}
            self.arrive(p, seq[n], h)
            for r in follow.get(n, []):
                self.hop(p, r, h).start()
            self.share(p, seq[n], h).start()

    def drain(self):
        self.share_own().wait_send()
        for h in range(self.halves):
            for p in range(3):
                for r in CHIPS[1:]:
                    self.hop(p, r, h).wait_send()
                    self.share(p, r, h).wait_send()


NEAR = [(1, 0, 0), (0, 1, 0), (0, 0, 1)]
MIDDLE = [(1, 1, 0), (0, 1, 1), (1, 0, 1)]
FAR = [(1, 1, 1)]
HERE = [(0, 0, 0)]


def backward_kernel(x, dy, pre, w_down, w_in, x_all, dy_all, d_pre, hidden, slope, dw_down, dx, dw_in, ici, d2d,
                    send, recv, out, back, w_sem, load_sem, store_sem, own_sem, *scatter_sems):
    place = Place()
    shard, width = dy.shape
    half = shard // 2
    tokens, ff = pre.shape
    block = ff // 4
    place.barrier()
    sems = (send, recv, out, back)
    gather_dy = Gather(place, dy, dy_all, sems, 0, 2)
    gather_x = Gather(place, x, x_all, sems, 48, 1)
    gather_dy.begin()
    mine = gather_dy.rows_of(HERE[0], place.core)

    def gradient(weights):
        def load_weights(j):
            part = pl.ds(j * block, block)
            return pltpu.make_async_copy(w_down.at[part], weights.at[part], w_sem.at[j])

        for j in range(4):
            load_weights(j).start()

        def before(x_buf):
            taken = pltpu.make_async_copy(x, x_buf, own_sem.at[0])
            taken.start()

            def gelu(pre_ref, hidden_ref, slope_ref):
                value, pull = jax.vjp(act, pre_ref[...].astype(F32))
                hidden_ref[...] = value.astype(BF16)
                slope_ref[...] = pull(jnp.ones_like(value))[0]

            spec = pl.BlockSpec((shard, ff), lambda i: (i, 0))
            pltpu.emit_pipeline(gelu, grid=(tokens // shard,), in_specs=[spec], out_specs=[spec, spec])(pre, hidden, slope)
            taken.wait()
            put = pltpu.make_async_copy(x_buf, x_all.at[mine], own_sem.at[1])
            put.start()
            for n in range(3):
                gather_dy.act(n, 0)
            gather_dy.shared_own()
            put.wait()

        pl.run_scoped(before, pltpu.VMEM((shard, width), BF16))

        def chunks(lhs, slopes, result):
            batches = [(HERE, None), (NEAR, 0), (NEAR, 1), (MIDDLE, 0), (MIDDLE, 1), (FAR, None)]

            def parts(n):
                chips, h = batches[n]
                size = shard if h is None else half
                cores = (place.core, 1 - place.core)
                return [(gather_dy.rows_of(r, c, h), pl.ds(k * size, size)) for k, (r, c) in enumerate((r, c) for r in chips for c in cores)]

            def rows_in(n):
                return sum(part.size for _, part in parts(n))

            def loads(n):
                copies = []
                for k, (src, part) in enumerate(parts(n)):
                    at = 12 * (n % 2) + k
                    there = dy if (n == 0 and k == 0) else dy_all.at[src]
                    copies.append(pltpu.make_async_copy(there, lhs.at[n % 2, part], load_sem.at[at]))
                    copies.append(pltpu.make_async_copy(slope.at[src], slopes.at[n % 2, part], load_sem.at[at + 6]))
                return copies

            def stores(n):
                return [
                    pltpu.make_async_copy(result.at[n % 2, part], d_pre.at[dst], store_sem.at[6 * (n % 2) + k])
                    for k, (dst, part) in enumerate(parts(n))
                ]

            own = pltpu.make_async_copy(lhs.at[0, pl.ds(0, shard)], dy_all.at[mine], own_sem.at[0])

            def ready(n):
                chips, h = batches[n]
                if n == 2:
                    for k in range(3):
                        gather_dy.act(k, 1)
                if n in (3, 4):
                    for k in (3, 4, 5):
                        gather_dy.act(k, h)
                if n == 5:
                    gather_dy.act(6, 0)
                    gather_dy.act(6, 1)
                for h in (0, 1) if h is None else (h,):
                    gather_dy.shared_all(chips, h)
                if n == 2:
                    own.wait()
                for copy in loads(n):
                    copy.start()

            when = (2, 3, 4, 4, 3)
            for copy in loads(0):
                copy.start()
            for n in range(6):
                for copy in loads(n):
                    copy.wait()
                if n == 0:
                    own.start()
                    for j in range(4):
                        load_weights(j).wait()
                if n >= 2:
                    for copy in stores(n - 2):
                        copy.wait()
                size, slot = rows_in(n), n % 2

                @pl.loop(0, 4)
                def _(j):
                    if n < 5 and when[n] < 4:
                        @pl.when(j == when[n])
                        def _():
                            ready(n + 1)

                    columns = lanes(j * block, block)
                    d_hidden = dot(lhs[slot, :size], weights[rows(j * block, block), :], NT)
                    result[slot, :size, columns] = (d_hidden * slopes[slot, :size, columns]).astype(BF16)

                for copy in stores(n):
                    copy.start()
                if n < 5 and when[n] == 4:
                    ready(n + 1)
                if n == 3:
                    gather_x.begin()
            for n in (4, 5):
                for copy in stores(n):
                    copy.wait()

        pl.run_scoped(chunks, pltpu.VMEM((2, 6 * half, width), BF16), pltpu.VMEM((2, 6 * half, ff), F32), pltpu.VMEM((2, 6 * half, ff), BF16))

    pl.run_scoped(gradient, pltpu.VMEM((ff, width), BF16))

    tm, tn = ff // 2, width // 8

    def product(h_ref, dy_ref, o_ref):
        at = pl.program_id(0) * 8 + pl.program_id(1)
        for n, when in enumerate((1, 4, 7, 10, 13, 15)):
            @pl.when(at == when)
            def _():
                gather_x.act(n)

        o_ref[...] = dot(h_ref[...], dy_ref[...], TN).astype(BF16)

    def down():
        pltpu.emit_pipeline(
            product,
            grid=(2, 8),
            in_specs=[pl.BlockSpec((tokens, tm), lambda i, j: (0, i)), pl.BlockSpec((tokens, tn), lambda i, j: (0, j))],
            out_specs=[pl.BlockSpec((tm, tn), lambda i, j: (i, j))],
        )(hidden, dy_all, dw_down)

    def rest(lhs, weights, right):
        scatter(place, gather_x, down, x_all, d_pre, w_in, dx, dw_in, ici, d2d, lhs, weights, right, *scatter_sems)

    pl.run_scoped(
        rest, pltpu.VMEM((3, 8 * shard, ff), BF16), pltpu.VMEM((width // 4, ff), BF16), pltpu.VMEM((tokens, ff), BF16)
    )
    gather_dy.drain()
    gather_x.drain()


def scatter(place, gather_x, down, x_all, d_pre, w_in, dx, dw_in, ici, d2d, lhs_buf, weights, right,
            ici_send, ici_recv, d2d_send, d2d_recv, w_sem, load_sem, stage_sem, dx_sem, x_sem, dw_sem, right_sem):
    core = place.core
    shard, width = dx.shape
    tokens, ff = d_pre.shape
    n1, n2 = width // 16, width // 8

    def pick(i, group):
        k = lax.div(i, 3 * group)
        p = (1 - k) * lax.rem(i, 3) + k * lax.rem(i, 2)
        t = (1 - k) * lax.div(i, 3) + k * (group + lax.div(i - 3 * group, 2))
        return p, t

    def unpick(p, t, group):
        k = lax.div(t, group)
        return (1 - k) * (3 * t + p) + k * (3 * group + 2 * (t - group) + p)

    def turn(p, k):
        return lax.rem(p + k, 3)

    def narrow(i):
        p, t = pick(i, 4)
        return p, t, p * (3 * n2) + t * n1

    def wide(i):
        p, t = pick(i, 2)
        return p, t, p * (3 * n2) + t * n2

    def narrow_weights(i):
        slot = lax.rem(i, 4)
        return [pltpu.make_async_copy(w_in.at[rows(narrow(i)[2], n1)], weights.at[rows(slot * n1, n1)], w_sem.at[slot])]

    def wide_weights(i):
        start, slot = wide(i)[2], lax.rem(i, 2)
        return [
            pltpu.make_async_copy(w_in.at[rows(start + h * n1, n1)], weights.at[rows(slot * n2 + h * n1, n1)], w_sem.at[2 * slot + h])
            for h in (0, 1)
        ]

    def go(copies):
        for copy in copies:
            copy.start()

    def wait(copies):
        for copy in copies:
            copy.wait()

    def lhs_loads(p, first, chips, base):
        loads = []
        for half, c in enumerate((1 - core, core)):
            for k, r in enumerate(chips):
                src = d_pre.at[rows((2 * place.chip_at(r) + c) * shard, shard)]
                n = half * len(chips) + k
                loads.append(pltpu.make_async_copy(src, lhs_buf.at[p, pl.ds(first + n * shard, shard)], load_sem.at[base + n]))
        return loads

    def exchange(k, i, count, size, columns, base, part):
        region = (0, 4, 6, 7)[k]
        dst = d2d.at[pl.ds(region * shard, count * shard), columns]
        return remote(part, dst, d2d_send.at[base + i], d2d_recv.at[base + i], place.sibling)

    def onward(k, i, count, p, columns, base, part):
        region = (0, 4, 6)[k]
        dst = ici.at[pl.ds(region * shard, count * shard), columns]
        return remote(part, dst, ici_send.at[base + i], ici_recv.at[base + i], place.across(turn(p, k)))

    def stage_chips(p, k):
        a, b, c = order(p)
        tail = [(0, 0), (0, 1), (1, 0), (1, 1)]
        if k == 0:
            return [tuple(across(a)[d] + s * across(b)[d] + t * across(c)[d] for d in range(3)) for s, t in tail]
        if k == 1:
            return [across(b), across(b, c)]
        return [across(c)] if k == 2 else [(0, 0, 0)]

    def stage(k, items, out, lag_b, lag_c, prepare=None, filler=None):
        count = (4, 2, 1, 1)[k]
        size = n1 if k == 0 else n2
        base = (0, 16, 24, 32)[k]
        locate = narrow if k == 0 else wide
        slots, n_term, n_staged = lag_c, 2, lag_c - lag_b + 1
        n_in = 1 + k
        from_ici = [(), ((2, 4),), ((1, 2), (5, 6)), ((0, 1), (4, 5), (6, 7))][k]

        def body(acc, term, staged):
            def columns(i):
                return lanes(locate(i)[2], size)

            def sources(i):
                region = (0, 4, 6, 7)[k]
                views = [d2d.at[pl.ds(region * shard, count * shard), columns(i)]]
                views += [ici.at[pl.ds(a * shard, (b - a) * shard), columns(i)] for a, b in from_ici]
                slot = lax.rem(i, n_staged)
                return [
                    pltpu.make_async_copy(view, staged.at[slot, n], stage_sem.at[slot * n_in + n]) for n, view in enumerate(views)
                ]

            def send(i):
                return exchange(k, i, count, size, columns(i), base, term.at[lax.rem(i, n_term)])

            def leave(i):
                if k < 3:
                    return onward(k, i, count, locate(i)[0], columns(i), base, out.at[i])
                return pltpu.make_async_copy(out.at[i], dx.at[:, columns(i)], dx_sem.at[i])

            def fetch(j):
                view = d2d.at[pl.ds(0, count * shard), columns(j)]
                remote(view, view, d2d_send.at[base + j], d2d_recv.at[base + j], place.sibling).wait_recv()
                p, t, start = locate(j)
                if k == 1:
                    for h in (0, 1):
                        n = unpick(p, 2 * t + h, 4)
                        view = ici.at[pl.ds(0, 4 * shard), lanes(start + h * n1, n1)]
                        remote(view, view, ici_send.at[n], ici_recv.at[n], place.sibling).wait_recv()
                elif k > 1:
                    n = (16, 24)[k - 2] + j
                    view = ici.at[pl.ds(0, (2, 1)[k - 2] * shard), columns(j)]
                    remote(view, view, ici_send.at[n], ici_recv.at[n], place.sibling).wait_recv()
                go(sources(j))

            def add(j, slot, there):
                total = acc[slot]
                for n in range(n_in):
                    total = total + staged[there, n].astype(F32)
                out[j] = total.astype(BF16)

            @pl.loop(0, items)
            def _(i):
                p, _, start = locate(i)
                slot = lax.rem(i, slots)
                wait(narrow_weights(i) if k == 0 else wide_weights(i))
                if prepare is not None:
                    prepare(i)

                @pl.when(i >= n_term)
                def _():
                    send(i - n_term).wait_send()

                @pl.when(i >= lag_c)
                def _():
                    wait(sources(i - lag_c))

                add(lax.max(i - lag_c, 0), slot, lax.rem(i + n_staged * lag_c - lag_c, n_staged))
                if k == 0:
                    w = weights[rows(lax.rem(i, 4) * n1, n1), :]
                else:
                    w = weights[rows(lax.rem(i, 2) * n2, n2), :]
                where = ((0, 8), (0, 4), (4, 2), (6, 2))[k]
                value = dot(lhs_buf[0 if k == 3 else p, pl.ds(where[0] * shard, where[1] * shard)], w, NT)
                term[lax.rem(i, n_term)] = value[: count * shard].astype(BF16)
                acc[slot] = value[count * shard :]
                send(i).start()

                @pl.when(i >= lag_c)
                def _():
                    leave(i - lag_c).start()

                if k == 0:
                    @pl.when(i + 4 < items)
                    def _():
                        go(narrow_weights(i + 4))

                    @pl.when(i == items - 3)
                    def _():
                        go(wide_weights(0))

                    @pl.when(i == items - 1)
                    def _():
                        go(wide_weights(1))
                elif k < 3:
                    go(wide_weights(lax.rem(i + 2, 8)))
                else:
                    @pl.when(i + 2 < items)
                    def _():
                        go(wide_weights(i + 2))

                if filler is not None:
                    filler(i)

                @pl.when(i >= lag_b)
                def _():
                    fetch(i - lag_b)

            for i in range(items, items + lag_c):
                j = i - lag_c
                wait(sources(j))
                add(j, j % slots, j % n_staged)
                leave(j).start()
                if i - lag_b < items:
                    fetch(i - lag_b)
            for i in range(items - n_term, items):
                send(i).wait_send()

        pl.run_scoped(
            body,
            pltpu.VMEM((slots, count * shard, size), F32),
            pltpu.VMEM((n_term, count * shard, size), BF16),
            pltpu.VMEM((n_staged, n_in, count * shard, size), BF16),
        )

    loads1 = [lhs_loads(p, 0, stage_chips(p, 0), 8 * p) for p in range(3)]
    loads2 = [c for p in range(3) for c in lhs_loads(p, 0, stage_chips(p, 1), 24 + 4 * p)]
    loads3 = [c for p in range(3) for c in lhs_loads(p, 4 * shard, stage_chips(p, 2), 36 + 2 * p)]
    loads4 = lhs_loads(0, 6 * shard, stage_chips(0, 3), 42)
    right_load = pltpu.make_async_copy(d_pre, right, right_sem.at[0])
    for i in range(4):
        go(narrow_weights(i))
    for some in loads1:
        go(some)
    right_load.start()
    down()
    for some in loads1:
        wait(some)

    def main(out2, x_buf, dw_buf):
        def x_load(i):
            slot = lax.rem(i, 2)
            return pltpu.make_async_copy(x_all.at[:, lanes(i * n1, n1)], x_buf.at[slot], x_sem.at[slot])

        def dw_store(i):
            slot = lax.rem(i, 2)
            return pltpu.make_async_copy(dw_buf.at[slot], dw_in.at[rows(i * n1, n1)], dw_sem.at[slot])

        def tiles(a, b):
            @pl.loop(a, b)
            def _(i):
                slot = lax.rem(i, 2)
                x_load(i).wait()

                @pl.when(i >= 2)
                def _():
                    dw_store(i - 2).wait()

                @pl.loop(0, 2)
                def _(h):
                    part = lanes(h * (ff // 2), ff // 2)
                    dw_buf[slot, :, part] = dot(x_buf[slot], right[:, part], TN).astype(BF16)

                dw_store(i).start()

                @pl.when(i + 2 < 8)
                def _():
                    x_load(i + 2).start()

        def fill2(i):
            turn, on = lax.div(i + 1, 3), lax.div(lax.rem(i, 3), 2)
            tiles(turn - on, turn - on + on * (2 * turn - 1))

        def fill3(i):
            turn, on = lax.div(i + 1, 3), lax.div(lax.rem(i, 3), 2)
            tiles(4 + turn, 4 + turn + on)

        def fill4(i):
            on = lax.div(lax.rem(i, 3), 2) * lax.div(i, 3)
            tiles(7, 7 + on)

        def early(out1):
            def prepare(i):
                @pl.when(i == 5)
                def _():
                    gather_x.act(6)

            stage(0, 16, out1, 1, 3, prepare=prepare)
            for some in (loads2, loads3, loads4):
                go(some)
            gather_x.shared_own()
            gather_x.shared_all(CHIPS[1:], 0)
            x_load(0).start()
            x_load(1).start()
            right_load.wait()
            for some in (loads2, loads3, loads4):
                wait(some)
            stage(1, 8, out2, 0, 2, filler=fill2)
            for i in range(16):
                onward(0, i, 4, narrow(i)[0], lanes(narrow(i)[2], n1), 0, out1.at[i]).wait_send()

        pl.run_scoped(early, pltpu.VMEM((16, 4 * shard, n1), BF16))
        tiles(4, 5)

        def late(out3, out4):
            stage(2, 8, out3, 2, 5, filler=fill3)
            stage(3, 8, out4, 2, 5, filler=fill4)
            dw_store(6).wait()
            dw_store(7).wait()
            for i in range(8):
                onward(1, i, 2, wide(i)[0], lanes(wide(i)[2], n2), 16, out2.at[i]).wait_send()
                onward(2, i, 1, wide(i)[0], lanes(wide(i)[2], n2), 24, out3.at[i]).wait_send()
                pltpu.make_async_copy(out4.at[i], dx.at[:, lanes(wide(i)[2], n2)], dx_sem.at[i]).wait()

        pl.run_scoped(late, pltpu.VMEM((8, shard, n2), BF16), pltpu.VMEM((8, shard, n2), BF16))

    pl.run_scoped(
        main,
        pltpu.VMEM((8, 2 * shard, n2), BF16),
        pltpu.VMEM((2, tokens, n1), BF16),
        pltpu.VMEM((2, n1, ff), BF16),
    )


def backward(x, dy, pre, w_in, w_down):
    shard, width = dy.shape
    tokens, ff = pre.shape
    dma = pltpu.SemaphoreType.DMA

    def shape(*size, dtype=BF16):
        return jax.ShapeDtypeStruct(size, dtype)

    x_all, _, d_pre, _, _, dw_down, dx, dw_in, _, _ = pl.pallas_call(
        backward_kernel,
        in_specs=[ANY] * 5,
        out_specs=[ANY] * 10,
        out_shape=[
            shape(tokens, width),
            shape(tokens, width),
            shape(tokens, ff),
            shape(tokens, ff),
            shape(tokens, ff, dtype=F32),
            shape(ff, width),
            shape(shard, width),
            shape(width // 2, ff),
            shape(7 * shard, width),
            shape(8 * shard, width),
        ],
        scratch_shapes=[dma((n,)) for n in (72, 72, 72, 72, 4, 24, 12, 2, 32, 32, 40, 40, 4, 44, 24, 8, 2, 2, 1)],
        compiler_params=pltpu.CompilerParams(collective_id=0, has_side_effects=True, vmem_limit_bytes=VMEM_LIMIT),
        cost_estimate=pl.CostEstimate(flops=7 * tokens * ff * width, bytes_accessed=800_000_000, transcendentals=tokens * ff),
        name="backward",
    )(x, dy, pre, w_down, w_in)
    return x_all, d_pre, dw_down, dx, dw_in


def finish_kernel(x_ref, d_pre_ref, part_ref, down_ref, dw_in, dw_down, buf, copy_sem, buf_sem):
    i = pl.program_id(0)
    n, ff = part_ref.shape
    count = pl.num_programs(0)
    slot = lax.rem(i, 2)
    copies = [
        pltpu.make_async_copy(part_ref, dw_in.at[rows(i * n, n)], copy_sem.at[0]),
        pltpu.make_async_copy(down_ref, dw_down.at[rows(i * down_ref.shape[0], down_ref.shape[0])], copy_sem.at[1]),
    ]

    def store(i):
        slot = lax.rem(i, 2)
        return pltpu.make_async_copy(buf.at[slot], dw_in.at[rows((count + i) * n, n)], buf_sem.at[slot])

    for copy in copies:
        copy.start()

    @pl.when(i >= 2)
    def _():
        store(i - 2).wait()

    @pl.loop(0, 2)
    def _(h):
        half = lanes(h * (ff // 2), ff // 2)
        buf[slot, :, half] = dot(x_ref[...], d_pre_ref[:, half], TN).astype(BF16)

    store(i).start()
    for copy in copies:
        copy.wait()

    @pl.when(i == count - 1)
    def _():
        store(i - 1).wait()
        store(i).wait()


def finish(x_all, d_pre, dw_in_part, dw_down_part):
    tokens, ff = d_pre.shape
    width = x_all.shape[1]
    n = width // 16
    return pl.pallas_call(
        finish_kernel,
        grid=(8,),
        in_specs=[
            pl.BlockSpec((tokens, n), lambda i: (0, 8 + i)),
            pl.BlockSpec((tokens, ff), lambda i: (0, 0)),
            pl.BlockSpec((n, ff), lambda i: (i, 0)),
            pl.BlockSpec((ff // 8, width), lambda i: (i, 0)),
        ],
        out_specs=[ANY] * 2,
        out_shape=[jax.ShapeDtypeStruct((width, ff), BF16), jax.ShapeDtypeStruct((ff, width), BF16)],
        scratch_shapes=[pltpu.VMEM((2, n, ff), BF16), pltpu.SemaphoreType.DMA((2,)), pltpu.SemaphoreType.DMA((2,))],
        compiler_params=pltpu.CompilerParams(dimension_semantics=("arbitrary",), vmem_limit_bytes=VMEM_LIMIT),
        cost_estimate=pl.CostEstimate(flops=tokens * ff * width, bytes_accessed=140_000_000, transcendentals=0),
        name="finish",
    )(x_all, d_pre, dw_in_part, dw_down_part)


def solution(mesh):
    def body(x, dy, pre, w_in, w_down):
        x_all, d_pre, dw_down, dx, dw_in = backward(x, dy, pre, w_in, w_down)
        dw_in, dw_down = finish(x_all, d_pre, dw_in, dw_down)
        return dx, dw_in, dw_down

    return jax.shard_map(
        body,
        mesh=mesh,
        in_specs=(P(("dp", "tp")), P(("dp", "tp")), P("dp", "tp"), P(None, "tp"), P("tp", None)),
        out_specs=(P(("dp", "tp")), P("dp", "tp"), P(("dp", "tp"))),
        check_vma=False,
    )
```

```python
import functools

import jax
import jax.numpy as jnp
from jax import lax
from jax.experimental import pallas as pl
from jax.experimental.pallas import tpu as pltpu
from jax.sharding import PartitionSpec as P

VMEM_LIMIT = 67_000_000
WEIGHT = (4, 2, 1)
F32, BF16 = jnp.float32, jnp.bfloat16
ANY = pl.BlockSpec(memory_space=pl.ANY)
CHIPS = [(a, b, c) for a in (0, 1) for b in (0, 1) for c in (0, 1)]


def act(pre):
    return jax.nn.gelu(pre)


def dot(a, b, dims):
    return lax.dot_general(a, b, (dims, ((), ())), preferred_element_type=F32)


NT, TN = ((1,), (1,)), ((0,), (0,))


def rows(start, size):
    return pl.ds(pl.multiple_of(start, 16), size)


def lanes(start, size):
    return pl.ds(pl.multiple_of(start, 128), size)


class Place:
    def __init__(self):
        me = lax.axis_index("tp")
        self.chip, self.core = lax.div(me, 2), lax.rem(me, 2)
        self.step = [w * (1 - 2 * lax.rem(lax.div(self.chip, w), 2)) for w in WEIGHT]
        self.sibling = self.device(self.chip, 1 - self.core)

    def chip_at(self, r):
        return self.chip + sum(self.step[d] * r[d] for d in range(3) if isinstance(r[d], jax.Array) or r[d])

    def device(self, chip, core):
        return {"tp": 2 * chip + core}

    def across(self, d):
        if isinstance(d, int):
            return self.device(self.chip + self.step[d], self.core)
        r = (lax.div(2 - d, 2), lax.rem(d, 2), lax.div(d, 2))
        return self.device(self.chip_at(r), self.core)

    def barrier(self):
        sem = pltpu.get_barrier_semaphore()
        for peer in [self.sibling] + [self.across(d) for d in range(3)]:
            pl.semaphore_signal(sem, inc=1, device_id=peer, device_id_type=pl.DeviceIdType.MESH)
        pl.semaphore_wait(sem, 4)


def remote(src, dst, send, recv, device):
    return pltpu.make_async_remote_copy(src, dst, send, recv, device_id=device, device_id_type=pl.DeviceIdType.MESH)


def order(p):
    return p, (p + 1) % 3, (p + 2) % 3


def across(*dims):
    return tuple(int(d in dims) for d in range(3))


class Gather:
    def __init__(self, place, src, dst, sems, base, halves):
        self.place, self.src, self.dst, self.halves = place, src, dst, halves
        self.shard, width = src.shape
        self.size = self.shard // halves
        self.send, self.recv, self.out, self.back = (functools.partial(lambda s, i: s.at[base + i], s) for s in sems)
        tiles = width // 128
        ends = [128 * (tiles * k // 3) for k in range(4)]
        self.columns = [pl.ds(ends[k], ends[k + 1] - ends[k]) for k in range(3)]

    def rows_of(self, r, core, h=None):
        start = (2 * self.place.chip_at(r) + core) * self.shard
        return rows(start, self.shard) if h is None else rows(start + h * self.size, self.size)

    def piece(self, p, r, core, h):
        return self.dst.at[self.rows_of(r, core, h), self.columns[p]]

    @staticmethod
    def index(p, r, h):
        return 24 * h + 8 * p + 4 * r[0] + 2 * r[1] + r[2]

    def hop(self, p, r, h):
        d = [d for d in order(p) if r[d]][-1]
        q = tuple(r[e] * (e != d) for e in range(3))
        dst = self.piece(p, q, self.place.core, h)
        src = dst if any(q) else self.src.at[pl.ds(h * self.size, self.size), self.columns[p]]
        i = self.index(p, r, h)
        return remote(src, dst, self.send(i), self.recv(i), self.place.across(d))

    def arrive(self, p, r, h):
        view, i = self.piece(p, r, self.place.core, h), self.index(p, r, h)
        remote(view, view, self.send(i), self.recv(i), self.place.sibling).wait_recv()

    def share(self, p, r, h):
        view, i = self.piece(p, r, self.place.core, h), self.index(p, r, h)
        return remote(view, view, self.out(i), self.back(i), self.place.sibling)

    def shared(self, p, r, h):
        view, i = self.piece(p, r, 1 - self.place.core, h), self.index(p, r, h)
        remote(view, view, self.out(i), self.back(i), self.place.sibling).wait_recv()

    def share_own(self):
        return remote(self.src, self.dst.at[self.rows_of((0, 0, 0), self.place.core)], self.out(0), self.back(0), self.place.sibling)

    def shared_own(self):
        view = self.dst.at[self.rows_of((0, 0, 0), 1 - self.place.core)]
        remote(view, view, self.out(0), self.back(0), self.place.sibling).wait_recv()

    def shared_all(self, chips, h):
        for p in range(3):
            for r in chips:
                self.shared(p, r, h)

    def begin(self):
        self.share_own().start()
        for h in range(self.halves):
            for k in range(3):
                for d in range(3):
                    self.hop((d - k) % 3, across(d), h).start()

    def act(self, n, h=0):
        for p in range(3):
            a, b, c = order(p)
            seq = [across(a), across(b), across(c), across(a, b), across(a, c), across(b, c), across(a, b, c)]
            follow = {0: [across(a, b), across(a, c)], 1: [across(b, c)], 3: [across(a, b, c)]}
            self.arrive(p, seq[n], h)
            for r in follow.get(n, []):
                self.hop(p, r, h).start()
            self.share(p, seq[n], h).start()

    def drain(self):
        self.share_own().wait_send()
        for h in range(self.halves):
            for p in range(3):
                for r in CHIPS[1:]:
                    self.hop(p, r, h).wait_send()
                    self.share(p, r, h).wait_send()


NEAR = [(1, 0, 0), (0, 1, 0), (0, 0, 1)]
MIDDLE = [(1, 1, 0), (0, 1, 1), (1, 0, 1)]
FAR = [(1, 1, 1)]
HERE = [(0, 0, 0)]


def backward_kernel(x, dy, pre, w_down, w_in, x_all, dy_all, d_pre, hidden, dw_down, dx, dw_in, ici, d2d,
                    send, recv, out, back, w_sem, load_sem, pre_sem, hidden_sem, store_sem, own_sem, *scatter_sems):
    place = Place()
    shard, width = dy.shape
    half = shard // 2
    tokens, ff = pre.shape
    block = ff // 4
    place.barrier()
    sems = (send, recv, out, back)
    gather_dy = Gather(place, dy, dy_all, sems, 0, 2)
    gather_x = Gather(place, x, x_all, sems, 48, 1)
    gather_dy.begin()
    mine = gather_dy.rows_of(HERE[0], place.core)
    batches = [(HERE, None), (NEAR, 0), (NEAR, 1), (MIDDLE, 0), (MIDDLE, 1), (FAR, None)]

    def parts(n):
        chips, h = batches[n]
        size = shard if h is None else half
        cores = (place.core, 1 - place.core)
        return [(gather_dy.rows_of(r, c, h), pl.ds(k * size, size)) for k, (r, c) in enumerate((r, c) for r in chips for c in cores)]

    def rows_in(n):
        return sum(part.size for _, part in parts(n))

    def gradient(weights, lhs, slopes, result, values):
        def load_weights(j):
            part = rows(j * block, block)
            return pltpu.make_async_copy(w_down.at[part], weights.at[part], w_sem.at[j])

        def pre_loads(n):
            return [
                pltpu.make_async_copy(pre.at[src], values.at[n % 2, part], pre_sem.at[6 * (n % 2) + k])
                for k, (src, part) in enumerate(parts(n))
            ]

        def hidden_stores(n):
            return [
                pltpu.make_async_copy(values.at[n % 2, part], hidden.at[dst], hidden_sem.at[6 * (n % 2) + k])
                for k, (dst, part) in enumerate(parts(n))
            ]

        def row_load(n, k):
            src, part = parts(n)[k]
            there = dy if (n == 0 and k == 0) else dy_all.at[src]
            return pltpu.make_async_copy(there, lhs.at[n % 2, part], load_sem.at[6 * (n % 2) + k])

        def stores(n):
            return [
                pltpu.make_async_copy(result.at[n % 2, part], d_pre.at[dst], store_sem.at[6 * (n % 2) + k])
                for k, (dst, part) in enumerate(parts(n))
            ]

        def gelu(n):
            for copy in pre_loads(n):
                copy.wait()
            slot, some = n % 2, 32 if shard >= 64 else 16

            @pl.loop(0, rows_in(n) // some)
            def _(i):
                part = rows(i * some, some)
                value, pull = jax.vjp(act, values[slot, part, :].astype(F32))
                slopes[slot, part, :] = pull(jnp.ones_like(value))[0]
                values[slot, part, :] = value.astype(BF16)

            for copy in hidden_stores(n):
                copy.start()

        own_row = pltpu.make_async_copy(lhs.at[0, pl.ds(0, shard)], dy_all.at[mine], own_sem.at[0])

        for copy in pre_loads(0):
            copy.start()
        row_load(0, 0).start()
        for copy in pre_loads(1):
            copy.start()
        for j in range(4):
            load_weights(j).start()
        gelu(0)
        gather_dy.shared_own()
        row_load(0, 1).start()
        gelu(1)
        row_load(0, 0).wait()
        own_row.start()
        row_load(0, 1).wait()

        passes = [
            ([(0, 0)], [(1, 0)], [(2, 0)]),
            ([(0, 1)], [(1, 1)], [(2, 1)]),
            ([(3, 0)], [(4, 0)], [(5, 0)]),
            ([(3, 1)], [(4, 1)], [(5, 1)]),
            ([(6, 0)], [(6, 1)], []),
            ([], [], []),
        ]
        for n in range(6):
            if n:
                for k in range(len(parts(n))):
                    row_load(n, k).wait()
            if n < 4:
                for copy in hidden_stores(n):
                    copy.wait()
                for copy in pre_loads(n + 2):
                    copy.start()
            if n >= 2:
                for copy in stores(n - 2):
                    copy.wait()
            size, slot = rows_in(n), n % 2

            @pl.loop(0, 4)
            def _(j):
                if n == 0:
                    load_weights(j).wait()
                for at in (2, 3):
                    if passes[n][at - 2]:
                        @pl.when(j == at)
                        def _():
                            for k, h in passes[n][at - 2]:
                                gather_dy.act(k, h)

                columns = lanes(j * block, block)
                d_hidden = dot(lhs[slot, :size], weights[rows(j * block, block), :], NT)
                result[slot, :size, columns] = (d_hidden * slopes[slot, :size, columns]).astype(BF16)

            for copy in stores(n):
                copy.start()
            if n == 3:
                gather_x.begin()
            if n < 4:
                gelu(n + 2)
            for k, h in passes[n][2]:
                gather_dy.act(k, h)
            if n < 5:
                chips, h = batches[n + 1]
                for h in (0, 1) if h is None else (h,):
                    gather_dy.shared_all(chips, h)
                if n == 1:
                    own_row.wait()
                for k in range(len(parts(n + 1))):
                    row_load(n + 1, k).start()
        taken = pltpu.make_async_copy(x, lhs.at[0, pl.ds(0, shard)], own_sem.at[0])
        taken.start()
        for n in (4, 5):
            for copy in hidden_stores(n):
                copy.wait()
            for copy in stores(n):
                copy.wait()
        taken.wait()
        put = pltpu.make_async_copy(lhs.at[0, pl.ds(0, shard)], x_all.at[mine], own_sem.at[1])
        put.start()
        put.wait()

    pl.run_scoped(
        gradient,
        pltpu.VMEM((ff, width), BF16),
        pltpu.VMEM((2, 6 * half, width), BF16),
        pltpu.VMEM((2, 6 * half, ff), F32),
        pltpu.VMEM((2, 6 * half, ff), BF16),
        pltpu.VMEM((2, 6 * half, ff), BF16),
    )

    tm, tn = ff // 2, width // 8

    def down(loads):
        def product(h_ref, dy_ref, o_ref):
            at = pl.program_id(0) * 8 + pl.program_id(1)
            for n, when in enumerate((1, 4, 7, 10, 13, 15)):
                @pl.when(at == when)
                def _():
                    gather_x.act(n)

            for n, some in enumerate(loads):
                @pl.when(at == 2 + 2 * n)
                def _():
                    for copy in some:
                        copy.start()

            o_ref[...] = dot(h_ref[...], dy_ref[...], TN).astype(BF16)

        pltpu.emit_pipeline(
            product,
            grid=(2, 8),
            in_specs=[pl.BlockSpec((tokens, tm), lambda i, j: (0, i)), pl.BlockSpec((tokens, tn), lambda i, j: (0, j))],
            out_specs=[pl.BlockSpec((tm, tn), lambda i, j: (i, j))],
        )(hidden, dy_all, dw_down)

    def rest(lhs, weights, right):
        scatter(place, gather_x, down, x_all, d_pre, w_in, dx, dw_in, ici, d2d, lhs, weights, right, *scatter_sems)

    pl.run_scoped(
        rest, pltpu.VMEM((3, 8 * shard, ff), BF16), pltpu.VMEM((width // 4, ff), BF16), pltpu.VMEM((tokens, ff), BF16)
    )
    gather_dy.drain()
    gather_x.drain()


def scatter(place, gather_x, down, x_all, d_pre, w_in, dx, dw_in, ici, d2d, lhs_buf, weights, right,
            ici_send, ici_recv, d2d_send, d2d_recv, w_sem, load_sem, stage_sem, dx_sem, x_sem, dw_sem, right_sem):
    core = place.core
    shard, width = dx.shape
    tokens, ff = d_pre.shape
    n1, n2 = width // 16, width // 8

    def pick(i, group):
        k = lax.div(i, 3 * group)
        p = (1 - k) * lax.rem(i, 3) + k * lax.rem(i, 2)
        t = (1 - k) * lax.div(i, 3) + k * (group + lax.div(i - 3 * group, 2))
        return p, t

    def unpick(p, t, group):
        k = lax.div(t, group)
        return (1 - k) * (3 * t + p) + k * (3 * group + 2 * (t - group) + p)

    def turn(p, k):
        return lax.rem(p + k, 3)

    def narrow(i):
        p, t = pick(i, 4)
        return p, t, p * (3 * n2) + t * n1

    def wide(i):
        p, t = pick(i, 2)
        return p, t, p * (3 * n2) + t * n2

    def narrow_weights(i):
        slot = lax.rem(i, 4)
        return [pltpu.make_async_copy(w_in.at[rows(narrow(i)[2], n1)], weights.at[rows(slot * n1, n1)], w_sem.at[slot])]

    def wide_weights(i):
        start, slot = wide(i)[2], lax.rem(i, 2)
        return [
            pltpu.make_async_copy(w_in.at[rows(start + h * n1, n1)], weights.at[rows(slot * n2 + h * n1, n1)], w_sem.at[2 * slot + h])
            for h in (0, 1)
        ]

    def go(copies):
        for copy in copies:
            copy.start()

    def wait(copies):
        for copy in copies:
            copy.wait()

    def lhs_loads(p, first, chips, base):
        loads = []
        for half, c in enumerate((1 - core, core)):
            for k, r in enumerate(chips):
                src = d_pre.at[rows((2 * place.chip_at(r) + c) * shard, shard)]
                n = half * len(chips) + k
                loads.append(pltpu.make_async_copy(src, lhs_buf.at[p, pl.ds(first + n * shard, shard)], load_sem.at[base + n]))
        return loads

    def exchange(k, i, count, size, columns, base, part):
        region = (0, 4, 6, 7)[k]
        dst = d2d.at[pl.ds(region * shard, count * shard), columns]
        return remote(part, dst, d2d_send.at[base + i], d2d_recv.at[base + i], place.sibling)

    def onward(k, i, count, p, columns, base, part):
        region = (0, 4, 6)[k]
        dst = ici.at[pl.ds(region * shard, count * shard), columns]
        return remote(part, dst, ici_send.at[base + i], ici_recv.at[base + i], place.across(turn(p, k)))

    def stage_chips(p, k):
        a, b, c = order(p)
        tail = [(0, 0), (0, 1), (1, 0), (1, 1)]
        if k == 0:
            return [tuple(across(a)[d] + s * across(b)[d] + t * across(c)[d] for d in range(3)) for s, t in tail]
        if k == 1:
            return [across(b), across(b, c)]
        return [across(c)] if k == 2 else [(0, 0, 0)]

    def stage(k, items, out, lag_b, lag_c, prepare=None, filler=None, between=None):
        count = (4, 2, 1, 1)[k]
        size = n1 if k == 0 else n2
        base = (0, 16, 24, 32)[k]
        locate = narrow if k == 0 else wide
        slots, n_term, n_staged = lag_c, 2, lag_c - lag_b + 1
        n_in = 1 + k
        from_ici = [(), ((2, 4),), ((1, 2), (5, 6)), ((0, 1), (4, 5), (6, 7))][k]

        def body(acc, term, staged):
            def columns(i):
                return lanes(locate(i)[2], size)

            def sources(i):
                region = (0, 4, 6, 7)[k]
                views = [d2d.at[pl.ds(region * shard, count * shard), columns(i)]]
                views += [ici.at[pl.ds(a * shard, (b - a) * shard), columns(i)] for a, b in from_ici]
                slot = lax.rem(i, n_staged)
                return [
                    pltpu.make_async_copy(view, staged.at[slot, n], stage_sem.at[slot * n_in + n]) for n, view in enumerate(views)
                ]

            def send(i):
                return exchange(k, i, count, size, columns(i), base, term.at[lax.rem(i, n_term)])

            def leave(i):
                if k < 3:
                    return onward(k, i, count, locate(i)[0], columns(i), base, out.at[i])
                return pltpu.make_async_copy(out.at[i], dx.at[:, columns(i)], dx_sem.at[i])

            def fetch(j):
                view = d2d.at[pl.ds(0, count * shard), columns(j)]
                remote(view, view, d2d_send.at[base + j], d2d_recv.at[base + j], place.sibling).wait_recv()
                p, t, start = locate(j)
                if k == 1:
                    for h in (0, 1):
                        n = unpick(p, 2 * t + h, 4)
                        view = ici.at[pl.ds(0, 4 * shard), lanes(start + h * n1, n1)]
                        remote(view, view, ici_send.at[n], ici_recv.at[n], place.sibling).wait_recv()
                elif k > 1:
                    n = (16, 24)[k - 2] + j
                    view = ici.at[pl.ds(0, (2, 1)[k - 2] * shard), columns(j)]
                    remote(view, view, ici_send.at[n], ici_recv.at[n], place.sibling).wait_recv()
                go(sources(j))

            def add(j, slot, there):
                total = acc[slot]
                for n in range(n_in):
                    total = total + staged[there, n].astype(F32)
                out[j] = total.astype(BF16)

            @pl.loop(0, items)
            def _(i):
                p, _, start = locate(i)
                slot = lax.rem(i, slots)
                wait(narrow_weights(i) if k == 0 else wide_weights(i))
                if prepare is not None:
                    prepare(i)

                @pl.when(i >= n_term)
                def _():
                    send(i - n_term).wait_send()

                @pl.when(i >= lag_c)
                def _():
                    wait(sources(i - lag_c))

                add(lax.max(i - lag_c, 0), slot, lax.rem(i + n_staged * lag_c - lag_c, n_staged))
                if k == 0:
                    w = weights[rows(lax.rem(i, 4) * n1, n1), :]
                else:
                    w = weights[rows(lax.rem(i, 2) * n2, n2), :]
                where = ((0, 8), (0, 4), (4, 2), (6, 2))[k]
                value = dot(lhs_buf[0 if k == 3 else p, pl.ds(where[0] * shard, where[1] * shard)], w, NT)
                term[lax.rem(i, n_term)] = value[: count * shard].astype(BF16)
                acc[slot] = value[count * shard :]
                send(i).start()

                @pl.when(i >= lag_c)
                def _():
                    leave(i - lag_c).start()

                if k == 0:
                    @pl.when(i + 4 < items)
                    def _():
                        go(narrow_weights(i + 4))

                    @pl.when(i == items - 3)
                    def _():
                        go(wide_weights(0))

                    @pl.when(i == items - 1)
                    def _():
                        go(wide_weights(1))
                elif k < 3:
                    go(wide_weights(lax.rem(i + 2, 8)))
                else:
                    @pl.when(i + 2 < items)
                    def _():
                        go(wide_weights(i + 2))

                if filler is not None:
                    filler(i)

                @pl.when(i >= lag_b)
                def _():
                    fetch(i - lag_b)

            if between is not None:
                between()
            for i in range(items, items + lag_c):
                j = i - lag_c
                wait(sources(j))
                add(j, j % slots, j % n_staged)
                leave(j).start()
                if i - lag_b < items:
                    fetch(i - lag_b)
            for i in range(items - n_term, items):
                send(i).wait_send()

        pl.run_scoped(
            body,
            pltpu.VMEM((slots, count * shard, size), F32),
            pltpu.VMEM((n_term, count * shard, size), BF16),
            pltpu.VMEM((n_staged, n_in, count * shard, size), BF16),
        )

    loads1 = [lhs_loads(p, 0, stage_chips(p, 0), 8 * p) for p in range(3)]
    loads2 = [lhs_loads(p, 0, stage_chips(p, 1), 24 + 4 * p) for p in range(3)]
    loads3 = [lhs_loads(p, 4 * shard, stage_chips(p, 2), 36 + 2 * p) for p in range(3)]
    loads4 = lhs_loads(0, 6 * shard, stage_chips(0, 3), 42)
    right_load = pltpu.make_async_copy(d_pre, right, right_sem.at[0])
    down([[copy for i in range(4) for copy in narrow_weights(i)], loads1[0], loads1[1], loads1[2], [right_load]])
    for some in loads1:
        wait(some)

    def main(out2, x_buf, dw_buf):
        def x_load(i):
            slot = lax.rem(i, 2)
            return pltpu.make_async_copy(x_all.at[:, lanes(i * n1, n1)], x_buf.at[slot], x_sem.at[slot])

        def dw_store(i):
            slot = lax.rem(i, 2)
            return pltpu.make_async_copy(dw_buf.at[slot], dw_in.at[rows(i * n1, n1)], dw_sem.at[slot])

        def tiles(a, b):
            @pl.loop(a, b)
            def _(i):
                slot = lax.rem(i, 2)
                x_load(i).wait()

                @pl.when(i >= 2)
                def _():
                    dw_store(i - 2).wait()

                @pl.loop(0, 2)
                def _(h):
                    part = lanes(h * (ff // 2), ff // 2)
                    dw_buf[slot, :, part] = dot(x_buf[slot], right[:, part], TN).astype(BF16)

                dw_store(i).start()

                @pl.when(i + 2 < 8)
                def _():
                    x_load(i + 2).start()

        def fill2(i):
            turn, on = lax.div(i + 1, 3), lax.div(lax.rem(i, 3), 2)
            tiles(turn, turn + on * turn)

        def fill3(i):
            turn, on = lax.div(i + 1, 3), lax.div(lax.rem(i, 3), 2)
            tiles(4 + turn, 4 + turn + on)

        def fill4(i):
            on = lax.div(lax.rem(i, 3), 2) * lax.div(i, 3)
            tiles(7, 7 + on)

        def early(out1):
            def prepare(i):
                @pl.when(i == 3)
                def _():
                    gather_x.act(6)

                @pl.when(i == 12)
                def _():
                    gather_x.shared_own()
                    gather_x.shared_all(CHIPS[1:], 0)
                    x_load(0).start()
                    x_load(1).start()
                    go(loads2[2])
                    go(loads3[2])

                @pl.when(i == 15)
                def _():
                    go(loads2[0])
                    go(loads3[0])
                    go(loads4)

            def between():
                go(loads2[1])
                go(loads3[1])
                right_load.wait()
                tiles(0, 1)

            def prepare2(i):
                for p in range(3):
                    @pl.when(i == p)
                    def _():
                        wait(loads2[p])

            stage(0, 16, out1, 1, 3, prepare=prepare, between=between)
            stage(1, 8, out2, 1, 3, prepare=prepare2, filler=fill2, between=lambda: tiles(4, 5))
            for i in range(16):
                onward(0, i, 4, narrow(i)[0], lanes(narrow(i)[2], n1), 0, out1.at[i]).wait_send()

        pl.run_scoped(early, pltpu.VMEM((16, 4 * shard, n1), BF16))

        def late(out3, out4):
            for some in loads3 + [loads4]:
                wait(some)
            stage(2, 8, out3, 2, 5, filler=fill3)
            stage(3, 8, out4, 2, 5, filler=fill4)
            dw_store(6).wait()
            dw_store(7).wait()
            for i in range(8):
                onward(1, i, 2, wide(i)[0], lanes(wide(i)[2], n2), 16, out2.at[i]).wait_send()
                onward(2, i, 1, wide(i)[0], lanes(wide(i)[2], n2), 24, out3.at[i]).wait_send()
                pltpu.make_async_copy(out4.at[i], dx.at[:, lanes(wide(i)[2], n2)], dx_sem.at[i]).wait()

        pl.run_scoped(late, pltpu.VMEM((8, shard, n2), BF16), pltpu.VMEM((8, shard, n2), BF16))

    pl.run_scoped(
        main,
        pltpu.VMEM((8, 2 * shard, n2), BF16),
        pltpu.VMEM((2, tokens, n1), BF16),
        pltpu.VMEM((2, n1, ff), BF16),
    )


def backward(x, dy, pre, w_in, w_down):
    shard, width = dy.shape
    tokens, ff = pre.shape
    dma = pltpu.SemaphoreType.DMA

    def shape(*size):
        return jax.ShapeDtypeStruct(size, BF16)

    x_all, _, d_pre, _, dw_down, dx, dw_in, _, _ = pl.pallas_call(
        backward_kernel,
        in_specs=[ANY] * 5,
        out_specs=[ANY] * 9,
        out_shape=[
            shape(tokens, width),
            shape(tokens, width),
            shape(tokens, ff),
            shape(tokens, ff),
            shape(ff, width),
            shape(shard, width),
            shape(width // 2, ff),
            shape(7 * shard, width),
            shape(8 * shard, width),
        ],
        scratch_shapes=[dma((n,)) for n in (72, 72, 72, 72, 4, 12, 12, 12, 12, 2, 32, 32, 40, 40, 4, 44, 24, 8, 2, 2, 1)],
        compiler_params=pltpu.CompilerParams(collective_id=0, has_side_effects=True, vmem_limit_bytes=VMEM_LIMIT),
        cost_estimate=pl.CostEstimate(flops=7 * tokens * ff * width, bytes_accessed=800_000_000, transcendentals=tokens * ff),
        name="backward",
    )(x, dy, pre, w_down, w_in)
    return x_all, d_pre, dw_down, dx, dw_in


def finish_kernel(x_ref, d_pre_ref, part_ref, down_ref, dw_in, dw_down, buf, copy_sem, buf_sem):
    i = pl.program_id(0)
    n, ff = part_ref.shape
    count = pl.num_programs(0)
    slot = lax.rem(i, 2)
    copies = [
        pltpu.make_async_copy(part_ref, dw_in.at[rows(i * n, n)], copy_sem.at[0]),
        pltpu.make_async_copy(down_ref, dw_down.at[rows(i * down_ref.shape[0], down_ref.shape[0])], copy_sem.at[1]),
    ]

    def store(i):
        slot = lax.rem(i, 2)
        return pltpu.make_async_copy(buf.at[slot], dw_in.at[rows((count + i) * n, n)], buf_sem.at[slot])

    for copy in copies:
        copy.start()

    @pl.when(i >= 2)
    def _():
        store(i - 2).wait()

    @pl.loop(0, 2)
    def _(h):
        half = lanes(h * (ff // 2), ff // 2)
        buf[slot, :, half] = dot(x_ref[...], d_pre_ref[:, half], TN).astype(BF16)

    store(i).start()
    for copy in copies:
        copy.wait()

    @pl.when(i == count - 1)
    def _():
        store(i - 1).wait()
        store(i).wait()


def finish(x_all, d_pre, dw_in_part, dw_down_part):
    tokens, ff = d_pre.shape
    width = x_all.shape[1]
    n = width // 16
    return pl.pallas_call(
        finish_kernel,
        grid=(8,),
        in_specs=[
            pl.BlockSpec((tokens, n), lambda i: (0, 8 + i)),
            pl.BlockSpec((tokens, ff), lambda i: (0, 0)),
            pl.BlockSpec((n, ff), lambda i: (i, 0)),
            pl.BlockSpec((ff // 8, width), lambda i: (i, 0)),
        ],
        out_specs=[ANY] * 2,
        out_shape=[jax.ShapeDtypeStruct((width, ff), BF16), jax.ShapeDtypeStruct((ff, width), BF16)],
        scratch_shapes=[pltpu.VMEM((2, n, ff), BF16), pltpu.SemaphoreType.DMA((2,)), pltpu.SemaphoreType.DMA((2,))],
        compiler_params=pltpu.CompilerParams(dimension_semantics=("arbitrary",), vmem_limit_bytes=VMEM_LIMIT),
        cost_estimate=pl.CostEstimate(flops=tokens * ff * width, bytes_accessed=140_000_000, transcendentals=0),
        name="finish",
    )(x_all, d_pre, dw_in_part, dw_down_part)


def solution(mesh):
    def body(x, dy, pre, w_in, w_down):
        x_all, d_pre, dw_down, dx, dw_in = backward(x, dy, pre, w_in, w_down)
        dw_in, dw_down = finish(x_all, d_pre, dw_in, dw_down)
        return dx, dw_in, dw_down

    return jax.shard_map(
        body,
        mesh=mesh,
        in_specs=(P(("dp", "tp")), P(("dp", "tp")), P("dp", "tp"), P(None, "tp"), P("tp", None)),
        out_specs=(P(("dp", "tp")), P("dp", "tp"), P(("dp", "tp"))),
        check_vma=False,
    )
```

```python
import functools

import jax
import jax.numpy as jnp
from jax import lax
from jax.experimental import pallas as pl
from jax.experimental.pallas import tpu as pltpu
from jax.sharding import PartitionSpec as P

VMEM_LIMIT = 67_000_000
WEIGHT = (4, 2, 1)
HELD = 6
F32, BF16 = jnp.float32, jnp.bfloat16
ANY = pl.BlockSpec(memory_space=pl.ANY)


def act(pre):
    return jax.nn.gelu(pre)


def dot(a, b, dims):
    return lax.dot_general(a, b, (dims, ((), ())), preferred_element_type=F32)


NT, TN = ((1,), (1,)), ((0,), (0,))


def odd(i):
    return lax.rem(i, 2)


def rows(start, size):
    return pl.ds(pl.multiple_of(start, 16), size)


def lanes(start, size):
    return pl.ds(pl.multiple_of(start, 128), size)


class Place:
    def __init__(self):
        me = lax.axis_index("tp")
        self.chip, self.core = lax.div(me, 2), lax.rem(me, 2)
        self.step = [w * (1 - 2 * lax.rem(lax.div(self.chip, w), 2)) for w in WEIGHT]
        self.sibling = self.device(self.chip, 1 - self.core)

    def chip_at(self, r):
        return self.chip + sum(self.step[d] * r[d] for d in range(3) if isinstance(r[d], jax.Array) or r[d])

    def device(self, chip, core):
        return {"tp": 2 * chip + core}

    def across(self, d):
        if isinstance(d, int):
            return self.device(self.chip + self.step[d], self.core)
        r = (lax.div(2 - d, 2), lax.rem(d, 2), lax.div(d, 2))
        return self.device(self.chip_at(r), self.core)

    def barrier(self):
        sem = pltpu.get_barrier_semaphore()
        for peer in [self.sibling] + [self.across(d) for d in range(3)]:
            pl.semaphore_signal(sem, inc=1, device_id=peer, device_id_type=pl.DeviceIdType.MESH)
        pl.semaphore_wait(sem, 4)


def remote(src, dst, send, recv, device):
    return pltpu.make_async_remote_copy(src, dst, send, recv, device_id=device, device_id_type=pl.DeviceIdType.MESH)


def order(p):
    return p, (p + 1) % 3, (p + 2) % 3


def across(*dims):
    return tuple(int(d in dims) for d in range(3))


HERE, NEAR, FAR = [across()], [across(d) for d in range(3)], [across(*range(3))]
MIDDLE = [across(*order(d)[:2]) for d in range(3)]
OTHERS = NEAR + MIDDLE + FAR


class Gather:
    def __init__(self, place, src, dst, sems, base, halves):
        self.place, self.src, self.dst, self.halves = place, src, dst, halves
        self.shard, width = src.shape
        self.size = self.shard // halves
        self.send, self.recv, self.out, self.back = (functools.partial(lambda s, i: s.at[base + i], s) for s in sems)
        tiles = width // 128
        ends = [128 * (tiles * k // 3) for k in range(4)]
        self.columns = [pl.ds(ends[k], ends[k + 1] - ends[k]) for k in range(3)]

    def rows_of(self, r, core, h=None):
        start = (2 * self.place.chip_at(r) + core) * self.shard
        return rows(start, self.shard) if h is None else rows(start + h * self.size, self.size)

    def piece(self, p, r, core, h):
        return self.dst.at[self.rows_of(r, core, h), self.columns[p]]

    @staticmethod
    def index(p, r, h):
        return 24 * h + 8 * p + 4 * r[0] + 2 * r[1] + r[2]

    def hop(self, p, r, h):
        d = [d for d in order(p) if r[d]][-1]
        q = tuple(r[e] * (e != d) for e in range(3))
        dst = self.piece(p, q, self.place.core, h)
        src = dst if any(q) else self.src.at[pl.ds(h * self.size, self.size), self.columns[p]]
        i = self.index(p, r, h)
        return remote(src, dst, self.send(i), self.recv(i), self.place.across(d))

    def arrive(self, p, r, h):
        view, i = self.piece(p, r, self.place.core, h), self.index(p, r, h)
        remote(view, view, self.send(i), self.recv(i), self.place.sibling).wait_recv()

    def share(self, p, r, h):
        view, i = self.piece(p, r, self.place.core, h), self.index(p, r, h)
        return remote(view, view, self.out(i), self.back(i), self.place.sibling)

    def shared(self, p, r, h):
        view, i = self.piece(p, r, 1 - self.place.core, h), self.index(p, r, h)
        remote(view, view, self.out(i), self.back(i), self.place.sibling).wait_recv()

    def share_own(self):
        return remote(self.src, self.dst.at[self.rows_of((0, 0, 0), self.place.core)], self.out(0), self.back(0), self.place.sibling)

    def shared_own(self):
        view = self.dst.at[self.rows_of((0, 0, 0), 1 - self.place.core)]
        remote(view, view, self.out(0), self.back(0), self.place.sibling).wait_recv()

    def shared_all(self, chips, h):
        for p in range(3):
            for r in chips:
                self.shared(p, r, h)

    def begin(self):
        self.share_own().start()
        for h in range(self.halves):
            for k in range(3):
                for d in range(3):
                    self.hop((d - k) % 3, across(d), h).start()

    def act(self, n, h=0):
        for p in range(3):
            a, b, c = order(p)
            seq = [across(a), across(b), across(c), across(a, b), across(a, c), across(b, c), across(a, b, c)]
            follow = {0: [across(a, b), across(a, c)], 1: [across(b, c)], 3: [across(a, b, c)]}
            self.arrive(p, seq[n], h)
            for r in follow.get(n, []):
                self.hop(p, r, h).start()
            self.share(p, seq[n], h).start()

    def drain(self):
        self.share_own().wait_send()
        for h in range(self.halves):
            for p in range(3):
                for r in OTHERS:
                    self.hop(p, r, h).wait_send()
                    self.share(p, r, h).wait_send()


def backward_kernel(x, dy, pre, w_down, w_in, x_all, dy_all, d_pre, hidden, dw_down, dx, dw_in, ici, d2d,
                    send, recv, out, back, w_sem, load_sem, pre_sem, hidden_sem, store_sem, own_sem, *scatter_sems):
    place = Place()
    shard, width = dy.shape
    half = shard // 2
    tokens, ff = pre.shape
    block = ff // 4
    place.barrier()
    sems = (send, recv, out, back)
    gather_dy = Gather(place, dy, dy_all, sems, 0, 2)
    gather_x = Gather(place, x, x_all, sems, 48, 1)
    gather_dy.begin()
    mine = gather_dy.rows_of(HERE[0], place.core)
    batches = [(HERE, None), (NEAR, 0), (NEAR, 1), (MIDDLE, 0), (MIDDLE, 1), (FAR, None)]

    def parts(n):
        chips, h = batches[n]
        size = shard if h is None else half
        cores = (place.core, 1 - place.core)
        return [(gather_dy.rows_of(r, c, h), pl.ds(k * size, size)) for k, (r, c) in enumerate((r, c) for r in chips for c in cores)]

    def rows_in(n):
        return sum(part.size for _, part in parts(n))

    def gradient(weights, lhs, slopes, result, values):
        def load_weights(j):
            part = rows(j * block, block)
            return pltpu.make_async_copy(w_down.at[part], weights.at[part], w_sem.at[j])

        def pre_loads(n):
            return [
                pltpu.make_async_copy(pre.at[src], values.at[n % 2, part], pre_sem.at[6 * (n % 2) + k])
                for k, (src, part) in enumerate(parts(n))
            ]

        def hidden_stores(n):
            return [
                pltpu.make_async_copy(values.at[n % 2, part], hidden.at[dst], hidden_sem.at[6 * (n % 2) + k])
                for k, (dst, part) in enumerate(parts(n))
            ]

        def row_load(n, k):
            src, part = parts(n)[k]
            there = dy if (n == 0 and k == 0) else dy_all.at[src]
            return pltpu.make_async_copy(there, lhs.at[n % 2, part], load_sem.at[6 * (n % 2) + k])

        def stores(n):
            return [
                pltpu.make_async_copy(result.at[n % 2, part], d_pre.at[dst], store_sem.at[6 * (n % 2) + k])
                for k, (dst, part) in enumerate(parts(n))
            ]

        def gelu(n):
            for copy in pre_loads(n):
                copy.wait()
            slot, some = n % 2, 32 if shard >= 64 else 16

            @pl.loop(0, rows_in(n) // some)
            def _(i):
                part = rows(i * some, some)
                value, pull = jax.vjp(act, values[slot, part, :].astype(F32))
                slopes[slot, part, :] = pull(jnp.ones_like(value))[0]
                values[slot, part, :] = value.astype(BF16)

            for copy in hidden_stores(n):
                copy.start()

        first = pl.ds(0, shard)
        own_row = pltpu.make_async_copy(lhs.at[0, first], dy_all.at[mine], own_sem.at[0])
        own_x = [
            pltpu.make_async_copy(x, lhs.at[1, first], own_sem.at[1]),
            pltpu.make_async_copy(lhs.at[1, first], x_all.at[mine], own_sem.at[1]),
        ]

        def arrivals(n):
            chips, h = batches[n]
            if chips is FAR:
                return [(6, 0), (6, 1)]
            return [(k + 3 * (chips is MIDDLE), h) for k in range(3)]

        def row_loads(n, mine):
            return [row_load(n, k) for k in range(1 - mine, len(parts(n)), 2)]

        for copy in pre_loads(0):
            copy.start()
        row_load(0, 0).start()
        load_weights(0).start()
        for copy in pre_loads(1):
            copy.start()
        gelu(0)
        gather_dy.shared_own()
        row_load(0, 1).start()
        for j in range(1, 4):
            load_weights(j).start()
        own_x[0].start()
        row_load(0, 0).wait()
        own_row.start()
        row_load(0, 1).wait()

        for n in range(6):
            if n:
                for copy in row_loads(n, True) + row_loads(n, False):
                    copy.wait()
            if n < 4 and n != 1:
                for copy in hidden_stores(n):
                    copy.wait()
                for copy in pre_loads(n + 2):
                    copy.start()
            if n >= 2:
                for copy in stores(n - 2):
                    copy.wait()
            size, slot = rows_in(n), n % 2
            pieces = arrivals(n + 1) if n < 5 else []

            @pl.loop(0, 4)
            def _(j):
                if n == 0:
                    load_weights(j).wait()
                for at, (k, h) in enumerate(pieces[:2]):
                    @pl.when(j == at + 2)
                    def _():
                        gather_dy.act(k, h)

                columns = lanes(j * block, block)
                d_hidden = dot(lhs[slot, :size], weights[rows(j * block, block), :], NT)
                result[slot, :size, columns] = (d_hidden * slopes[slot, :size, columns]).astype(BF16)

            for copy in stores(n):
                copy.start()
            if n == 0:
                own_x[0].wait()
                own_x[1].start()
                gelu(1)
                own_x[1].wait()
                for copy in hidden_stores(1):
                    copy.wait()
                for copy in pre_loads(3):
                    copy.start()
            if n == 3:
                gather_x.begin()
            if n < 4:
                gelu(n + 2)
            for k, h in pieces[2:]:
                gather_dy.act(k, h)
            if n < 5:
                if n == 1:
                    own_row.wait()
                for copy in row_loads(n + 1, True):
                    copy.start()
                chips, h = batches[n + 1]
                for h in (0, 1) if h is None else (h,):
                    gather_dy.shared_all(chips, h)
                for copy in row_loads(n + 1, False):
                    copy.start()
        for n in (4, 5):
            for copy in hidden_stores(n) + stores(n):
                copy.wait()

    pl.run_scoped(
        gradient,
        pltpu.VMEM((ff, width), BF16),
        pltpu.VMEM((2, 6 * half, width), BF16),
        pltpu.VMEM((2, 6 * half, ff), F32),
        pltpu.VMEM((2, 6 * half, ff), BF16),
        pltpu.VMEM((2, 6 * half, ff), BF16),
    )

    tm, tn = ff // 2, width // 8

    def down(loads):
        def product(h_ref, dy_ref, o_ref):
            at = pl.program_id(0) * pl.num_programs(1) + pl.program_id(1)
            group, place_in = lax.div(at, 3), lax.rem(at, 3)

            @pl.when(place_in == 1)
            def _():
                for n in range(5):
                    @pl.when(group == n)
                    def _():
                        gather_x.act(n)

            @pl.when(place_in == 2)
            def _():
                for n, some in enumerate(loads):
                    @pl.when(group == n)
                    def _():
                        for copy in some:
                            copy.start()

            @pl.when(at == 15)
            def _():
                gather_x.act(5)

            o_ref[...] = dot(h_ref[...], dy_ref[...], TN).astype(BF16)

        pltpu.emit_pipeline(
            product,
            grid=(2, 8),
            in_specs=[pl.BlockSpec((tokens, tm), lambda i, j: (0, i)), pl.BlockSpec((tokens, tn), lambda i, j: (0, j))],
            out_specs=[pl.BlockSpec((tm, tn), lambda i, j: (i, j))],
        )(hidden, dy_all, dw_down)

    def rest(lhs, weights, right):
        scatter(place, gather_x, down, x_all, d_pre, w_in, dx, dw_in, ici, d2d, lhs, weights, right, *scatter_sems)

    pl.run_scoped(
        rest, pltpu.VMEM((3, 8 * shard, ff), BF16), pltpu.VMEM((width // 4, ff), BF16), pltpu.VMEM((tokens, ff), BF16)
    )
    gather_dy.drain()
    gather_x.drain()


def scatter(place, gather_x, down, x_all, d_pre, w_in, dx, dw_in, ici, d2d, lhs_buf, weights, right,
            ici_send, ici_recv, d2d_send, d2d_recv, w_sem, load_sem, stage_sem, dx_sem, x_sem, dw_sem, right_sem):
    core = place.core
    shard, width = dx.shape
    tokens, ff = d_pre.shape
    n1, n2 = width // 16, width // 8

    def pick(i, group):
        k = lax.div(i, 3 * group)
        p = (1 - k) * lax.rem(i, 3) + k * odd(i)
        t = (1 - k) * lax.div(i, 3) + k * (group + lax.div(i - 3 * group, 2))
        return p, t

    def unpick(p, t, group):
        k = lax.div(t, group)
        return (1 - k) * (3 * t + p) + k * (3 * group + 2 * (t - group) + p)

    def turn(p, k):
        return lax.rem(p + k, 3)

    def narrow(i):
        p, t = pick(i, 4)
        return p, t, p * (3 * n2) + t * n1

    def wide(i):
        p, t = pick(i, 2)
        return p, t, p * (3 * n2) + t * n2

    def narrow_weights(i):
        slot = lax.rem(i, 4)
        return [pltpu.make_async_copy(w_in.at[rows(narrow(i)[2], n1)], weights.at[rows(slot * n1, n1)], w_sem.at[slot])]

    def wide_weights(i):
        start, slot = wide(i)[2], odd(i)
        return [
            pltpu.make_async_copy(w_in.at[rows(start + h * n1, n1)], weights.at[rows(slot * n2 + h * n1, n1)], w_sem.at[2 * slot + h])
            for h in (0, 1)
        ]

    def go(copies):
        for copy in copies:
            copy.start()

    def wait(copies):
        for copy in copies:
            copy.wait()

    def lhs_loads(p, first, chips, base):
        loads = []
        for half, c in enumerate((1 - core, core)):
            for k, r in enumerate(chips):
                src = d_pre.at[rows((2 * place.chip_at(r) + c) * shard, shard)]
                n = half * len(chips) + k
                loads.append(pltpu.make_async_copy(src, lhs_buf.at[p, pl.ds(first + n * shard, shard)], load_sem.at[base + n]))
        return loads

    def exchange(k, i, count, columns, base, part):
        region = (0, 4, 6)[k]
        dst = d2d.at[pl.ds(region * shard, count * shard), columns]
        return remote(part, dst, d2d_send.at[base + i], d2d_recv.at[base + i], place.sibling)

    def onward(k, i, count, p, columns, base, part):
        region = (0, 4, 6)[k]
        dst = ici.at[pl.ds(region * shard, count * shard), columns]
        return remote(part, dst, ici_send.at[base + i], ici_recv.at[base + i], place.across(turn(p, k)))

    def stage_chips(p, k):
        a, b, c = order(p)
        tail = [(0, 0), (0, 1), (1, 0), (1, 1)]
        if k == 0:
            return [tuple(across(a)[d] + s * across(b)[d] + t * across(c)[d] for d in range(3)) for s, t in tail]
        if k == 1:
            return [across(b), across(b, c)]
        return [across(c)] + HERE

    def stage(k, items, out, between, prepare=None, filler=None, keep=None, lag_b=1, lag_c=3):
        count, moved = (4, 2, 1)[k], (4, 2, 2)[k]
        size = n1 if k == 0 else n2
        base = (0, 16, 24)[k]
        locate = narrow if k == 0 else wide
        slots, n_term, n_staged = lag_c, 2, lag_c
        n_in = 1 + k
        from_ici = [(), ((2, 4),), ((1, 2), (5, 6))][k]

        def body(acc, term, staged):
            def columns(i):
                return lanes(locate(i)[2], size)

            def sources(i):
                region = (0, 4, 6)[k]
                views = [d2d.at[pl.ds(region * shard, count * shard), columns(i)]]
                views += [ici.at[pl.ds(a * shard, (b - a) * shard), columns(i)] for a, b in from_ici]
                slot = lax.rem(i, n_staged)
                return [
                    pltpu.make_async_copy(view, staged.at[slot, n], stage_sem.at[slot * n_in + n]) for n, view in enumerate(views)
                ]

            def send(i):
                return exchange(k, i, moved, columns(i), base, term.at[lax.rem(i, n_term)])

            def leave(i):
                return onward(k, i, count, locate(i)[0], columns(i), base, out.at[i])

            def fetch(j):
                view = d2d.at[pl.ds(0, moved * shard), columns(j)]
                remote(view, view, d2d_send.at[base + j], d2d_recv.at[base + j], place.sibling).wait_recv()
                p, t, start = locate(j)
                if k == 1:
                    for h in range(2):
                        n = unpick(p, 2 * t + h, 4)
                        view = ici.at[pl.ds(0, 4 * shard), lanes(start + h * n1, n1)]
                        remote(view, view, ici_send.at[n], ici_recv.at[n], place.sibling).wait_recv()
                elif k == 2:
                    n = 16 + j
                    view = ici.at[pl.ds(0, 2 * shard), columns(j)]
                    remote(view, view, ici_send.at[n], ici_recv.at[n], place.sibling).wait_recv()
                go(sources(j))

            def add(j, slot, there):
                total = acc[slot]
                for n in range(n_in):
                    total = total + staged[there, n].astype(F32)
                out[j] = total.astype(BF16)

            @pl.loop(0, items)
            def _(i):
                p, _, start = locate(i)
                slot = lax.rem(i, slots)
                wait(narrow_weights(i) if k == 0 else wide_weights(i))
                if prepare is not None:
                    prepare(i)

                @pl.when(i >= n_term)
                def _():
                    send(i - n_term).wait_send()

                @pl.when(i >= lag_c)
                def _():
                    wait(sources(i - lag_c))

                add(lax.max(i - lag_c, 0), slot, lax.rem(i, n_staged))
                if k == 0:
                    w = weights[rows(lax.rem(i, 4) * n1, n1), :]
                else:
                    w = weights[rows(odd(i) * n2, n2), :]
                value = dot(lhs_buf[p, pl.ds((k // 2) * 4 * shard, 2 * moved * shard)], w, NT)
                term[lax.rem(i, n_term)] = value[: moved * shard].astype(BF16)
                acc[slot] = value[moved * shard : (moved + count) * shard]
                if k == 2:
                    keep[i] = value[(moved + count) * shard :]
                send(i).start()

                @pl.when(i >= lag_c)
                def _():
                    leave(i - lag_c).start()

                if k == 0:
                    @pl.when(i + 4 < items)
                    def _():
                        go(narrow_weights(i + 4))

                    @pl.when(i == items - 3)
                    def _():
                        go(wide_weights(0))

                    @pl.when(i == items - 1)
                    def _():
                        go(wide_weights(1))
                elif k == 1:
                    go(wide_weights(lax.rem(i + 2, items)))
                else:
                    @pl.when(i + 2 < items)
                    def _():
                        go(wide_weights(i + 2))

                if filler is not None:
                    filler(i)

                @pl.when(i >= lag_b)
                def _():
                    fetch(i - lag_b)

            between()
            for j in range(items - lag_b, items):
                fetch(j)
            for j in range(items - lag_c, items):
                wait(sources(j))
                add(j, j % slots, j % n_staged)
                leave(j).start()
            for i in range(items - n_term, items):
                send(i).wait_send()

        pl.run_scoped(
            body,
            pltpu.VMEM((slots, count * shard, size), F32),
            pltpu.VMEM((n_term, moved * shard, size), BF16),
            pltpu.VMEM((n_staged, n_in, count * shard, size), BF16),
        )

    loads1 = [lhs_loads(p, 0, stage_chips(p, 0), 8 * p) for p in range(3)]
    loads2 = [lhs_loads(p, 0, stage_chips(p, 1), 24 + 4 * p) for p in range(3)]
    loads3 = [lhs_loads(p, 4 * shard, stage_chips(p, 2), 36 + 4 * p) for p in range(3)]
    right_load = pltpu.make_async_copy(d_pre, right, right_sem.at[0])
    down([[copy for i in range(4) for copy in narrow_weights(i)], *loads1, [right_load]])
    for some in loads1:
        wait(some)

    def main(out2, x_buf, dw_buf):
        def x_load(i):
            slot = odd(i)
            return pltpu.make_async_copy(x_all.at[:, lanes(i * n1, n1)], x_buf.at[slot], x_sem.at[slot])

        def dw_store(i):
            slot = odd(i)
            return pltpu.make_async_copy(dw_buf.at[slot], dw_in.at[rows(i * n1, n1)], dw_sem.at[slot])

        def tiles(a, b):
            @pl.loop(a, b)
            def _(i):
                slot = odd(i)
                x_load(i).wait()

                @pl.when(i >= 2)
                def _():
                    dw_store(i - 2).wait()

                @pl.loop(0, 2)
                def _(h):
                    part = lanes(h * (ff // 2), ff // 2)
                    dw_buf[slot, :, part] = dot(x_buf[slot], right[:, part], TN).astype(BF16)

                dw_store(i).start()

                @pl.when(i + 2 < HELD)
                def _():
                    x_load(i + 2).start()

        def fill2(i):
            turn, on = lax.div(i + 1, 3), lax.div(lax.rem(i, 3), 2)
            tiles(turn, turn + on)

        def fill3(i):
            on = lax.div(lax.rem(i, 3), 2) * lax.div(i, 3)
            tiles(4, 4 + on)

        def early(out1):
            def prepare(i):
                @pl.when(i == 3)
                def _():
                    gather_x.act(6)

                @pl.when(i == 12)
                def _():
                    gather_x.shared_own()
                    gather_x.shared_all(OTHERS, 0)
                    x_load(0).start()
                    x_load(1).start()
                    go(loads2[2] + loads3[2])

                @pl.when(i == 15)
                def _():
                    go(loads2[0] + loads3[0])

            def between():
                go(loads2[1] + loads3[1])
                right_load.wait()
                tiles(0, 1)

            def prepare2(i):
                for p in range(3):
                    @pl.when(i == p)
                    def _():
                        wait(loads2[p] + loads3[p])

            stage(0, 16, out1, between, prepare=prepare)
            stage(1, 8, out2, lambda: tiles(3, 4), prepare=prepare2, filler=fill2)
            for i in range(16):
                onward(0, i, 4, narrow(i)[0], lanes(narrow(i)[2], n1), 0, out1.at[i]).wait_send()

        pl.run_scoped(early, pltpu.VMEM((16, 4 * shard, n1), BF16))

        def late(out3, keep):
            stage(2, 8, out3, lambda: tiles(5, 6), filler=fill3, keep=keep)
            pl.run_scoped(functools.partial(final, keep), pltpu.VMEM((8, shard, n2), BF16), pltpu.VMEM((4, 4, shard, n2), BF16))
            for i in range(8):
                onward(1, i, 2, wide(i)[0], lanes(wide(i)[2], n2), 16, out2.at[i]).wait_send()
                onward(2, i, 1, wide(i)[0], lanes(wide(i)[2], n2), 24, out3.at[i]).wait_send()

        def final(keep, out4, staged):
            def columns(i):
                return lanes(wide(i)[2], n2)

            def sources(i):
                views = [d2d.at[pl.ds(7 * shard, shard), columns(i)]]
                views += [ici.at[pl.ds(n * shard, shard), columns(i)] for n in (0, 4, 6)]
                slot = lax.rem(i, 4)
                return [pltpu.make_async_copy(view, staged.at[slot, n], stage_sem.at[4 * slot + n]) for n, view in enumerate(views)]

            def store(i):
                return pltpu.make_async_copy(out4.at[i], dx.at[:, columns(i)], dx_sem.at[i])

            @pl.loop(0, 8 + 3)
            def _(i):
                @pl.when(i >= 3)
                def _():
                    j = i - 3
                    wait(sources(j))
                    total = keep[j]
                    for n in range(4):
                        total = total + staged[lax.rem(j, 4), n].astype(F32)
                    out4[j] = total.astype(BF16)
                    store(j).start()

                @pl.when(i < 8)
                def _():
                    view = ici.at[pl.ds(0, shard), columns(i)]
                    remote(view, view, ici_send.at[24 + i], ici_recv.at[24 + i], place.sibling).wait_recv()
                    go(sources(i))

            dw_store(HELD - 2).wait()
            dw_store(HELD - 1).wait()
            for i in range(8):
                store(i).wait()

        pl.run_scoped(late, pltpu.VMEM((8, shard, n2), BF16), pltpu.VMEM((8, shard, n2), F32))

    pl.run_scoped(
        main,
        pltpu.VMEM((8, 2 * shard, n2), BF16),
        pltpu.VMEM((2, tokens, n1), BF16),
        pltpu.VMEM((2, n1, ff), BF16),
    )


def backward(x, dy, pre, w_in, w_down):
    shard, width = dy.shape
    tokens, ff = pre.shape
    dma = pltpu.SemaphoreType.DMA

    def shape(*size):
        return jax.ShapeDtypeStruct(size, BF16)

    x_all, _, d_pre, _, dw_down, dx, dw_in, _, _ = pl.pallas_call(
        backward_kernel,
        in_specs=[ANY] * 5,
        out_specs=[ANY] * 9,
        out_shape=[
            shape(tokens, width),
            shape(tokens, width),
            shape(tokens, ff),
            shape(tokens, ff),
            shape(ff, width),
            shape(shard, width),
            shape(HELD * width // 16, ff),
            shape(7 * shard, width),
            shape(8 * shard, width),
        ],
        scratch_shapes=[dma((n,)) for n in [72] * 4 + [4] + [12] * 4 + [2] + [32] * 4 + [4, 48, 16, 8, 2, 2, 1]],
        compiler_params=pltpu.CompilerParams(collective_id=0, has_side_effects=True, vmem_limit_bytes=VMEM_LIMIT),
        cost_estimate=pl.CostEstimate(flops=7 * tokens * ff * width, bytes_accessed=800_000_000, transcendentals=tokens * ff),
        name="backward",
    )(x, dy, pre, w_down, w_in)
    return x_all, d_pre, dw_down, dx, dw_in


def finish_kernel(x_ref, d_pre, part, down, dw_in, dw_down, right, buf, copies, tiles, right_sem, buf_sem, in_sem, out_sem):
    i, steps = pl.program_id(0), 16 - HELD
    n, ff = buf.shape[1:]
    slot = odd(i)
    piece = down.shape[0] // 16

    def right_load(h):
        half = pl.ds(h * (ff // 2), ff // 2)
        return pltpu.make_async_copy(d_pre.at[:, half], right.at[h], right_sem.at[h])

    def store(i):
        slot = odd(i)
        return pltpu.make_async_copy(buf.at[slot], dw_in.at[rows((HELD + i) * n, n)], buf_sem.at[slot])

    after = steps - HELD

    def moves(i, n_):
        at = 3 * odd(i) + n_
        held = copies.at[2 * odd(i) + n_] if n_ < 2 else tiles.at[odd(i)]
        where, k, size = (down, 2 * i + n_, piece) if n_ < 2 else (part, i - after, n)
        to = dw_down if n_ < 2 else dw_in
        span = rows(k * size, size)
        return (
            pltpu.make_async_copy(where.at[span], held, in_sem.at[at]),
            pltpu.make_async_copy(held, to.at[span], out_sem.at[at]),
        )

    def each(i, f):
        for n_ in range(3):
            @pl.when((i < 8) if n_ < 2 else ((i >= after) & (i < steps)))
            def _():
                f(*moves(i, n_))

    @pl.when(i == 0)
    def _():
        right_load(0).start()
        right_load(1).start()
        each(i, lambda into, out_of: into.start())

    @pl.when(i >= 2)
    def _():
        store(i - 2).wait()

    @pl.when(i > 0)
    def _():
        each(i - 1, lambda into, out_of: out_of.wait())

    @pl.when(i + 1 < steps)
    def _():
        each(i + 1, lambda into, out_of: into.start())

    @pl.when(i > 0)
    def _():
        each(i, lambda into, out_of: (into.wait(), out_of.start()))

    for h in range(2):
        @pl.when(i == 0)
        def _():
            right_load(h).wait()

        buf[slot, :, pl.ds(h * (ff // 2), ff // 2)] = dot(x_ref[...], right[h], TN).astype(BF16)

    store(i).start()

    @pl.when(i == 0)
    def _():
        each(i, lambda into, out_of: (into.wait(), out_of.start()))

    @pl.when(i == steps - 1)
    def _():
        each(i, lambda into, out_of: out_of.wait())
        store(i - 1).wait()
        store(i).wait()


def finish(x_all, d_pre, dw_in_part, dw_down_part):
    tokens, ff = d_pre.shape
    width = x_all.shape[1]
    n = width // 16
    dma = pltpu.SemaphoreType.DMA
    return pl.pallas_call(
        finish_kernel,
        grid=(16 - HELD,),
        in_specs=[pl.BlockSpec((tokens, n), lambda i: (0, HELD + i)), ANY, ANY, ANY],
        out_specs=[ANY] * 2,
        out_shape=[jax.ShapeDtypeStruct((width, ff), BF16), jax.ShapeDtypeStruct((ff, width), BF16)],
        scratch_shapes=[
            pltpu.VMEM((2, tokens, ff // 2), BF16),
            pltpu.VMEM((2, n, ff), BF16),
            pltpu.VMEM((4, ff // 16, width), BF16),
            pltpu.VMEM((2, n, ff), BF16),
            dma((2,)),
            dma((2,)),
            dma((6,)),
            dma((6,)),
        ],
        compiler_params=pltpu.CompilerParams(dimension_semantics=("arbitrary",), vmem_limit_bytes=VMEM_LIMIT),
        cost_estimate=pl.CostEstimate(flops=tokens * ff * width, bytes_accessed=140_000_000, transcendentals=0),
        name="finish",
    )(x_all, d_pre, dw_in_part, dw_down_part)


def solution(mesh):
    def body(x, dy, pre, w_in, w_down):
        x_all, d_pre, dw_down, dx, dw_in = backward(x, dy, pre, w_in, w_down)
        dw_in, dw_down = finish(x_all, d_pre, dw_in, dw_down)
        return dx, dw_in, dw_down

    return jax.shard_map(
        body,
        mesh=mesh,
        in_specs=(P(("dp", "tp")), P(("dp", "tp")), P("dp", "tp"), P(None, "tp"), P("tp", None)),
        out_specs=(P(("dp", "tp")), P("dp", "tp"), P(("dp", "tp"))),
        check_vma=False,
    )
```

```python
import functools

import jax
import jax.numpy as jnp
from jax import lax
from jax.experimental import pallas as pl
from jax.experimental.pallas import tpu as pltpu
from jax.sharding import PartitionSpec as P

VMEM_LIMIT = 67_000_000
WEIGHT = (4, 2, 1)
HELD = 8
F32, BF16 = jnp.float32, jnp.bfloat16
ANY = pl.BlockSpec(memory_space=pl.ANY)


def act(pre):
    return jax.nn.gelu(pre)


def dot(a, b, dims):
    return lax.dot_general(a, b, (dims, ((), ())), preferred_element_type=F32)


NT, TN = ((1,), (1,)), ((0,), (0,))


def odd(i):
    return lax.rem(i, 2)


def rows(start, size):
    return pl.ds(pl.multiple_of(start, 16), size)


def lanes(start, size):
    return pl.ds(pl.multiple_of(start, 128), size)


class Place:
    def __init__(self):
        me = lax.axis_index("tp")
        self.chip, self.core = lax.div(me, 2), lax.rem(me, 2)
        self.step = [w * (1 - 2 * lax.rem(lax.div(self.chip, w), 2)) for w in WEIGHT]
        self.sibling = self.device(self.chip, 1 - self.core)

    def chip_at(self, r):
        return self.chip + sum(self.step[d] * r[d] for d in range(3) if isinstance(r[d], jax.Array) or r[d])

    def device(self, chip, core):
        return {"tp": 2 * chip + core}

    def across(self, d):
        if isinstance(d, int):
            return self.device(self.chip + self.step[d], self.core)
        r = (lax.div(2 - d, 2), lax.rem(d, 2), lax.div(d, 2))
        return self.device(self.chip_at(r), self.core)

    def barrier(self):
        sem = pltpu.get_barrier_semaphore()
        for peer in [self.sibling] + [self.across(d) for d in range(3)]:
            pl.semaphore_signal(sem, inc=1, device_id=peer, device_id_type=pl.DeviceIdType.MESH)
        pl.semaphore_wait(sem, 4)


def remote(src, dst, send, recv, device):
    return pltpu.make_async_remote_copy(src, dst, send, recv, device_id=device, device_id_type=pl.DeviceIdType.MESH)


def order(p):
    return p, (p + 1) % 3, (p + 2) % 3


def across(*dims):
    return tuple(int(d in dims) for d in range(3))


HERE, NEAR, FAR = [across()], [across(d) for d in range(3)], [across(*range(3))]
MIDDLE = [across(*order(d)[:2]) for d in range(3)]
OTHERS = NEAR + MIDDLE + FAR


class Gather:
    def __init__(self, place, src, dst, sems, base, halves, shares):
        self.place, self.src, self.dst, self.halves = place, src, dst, halves
        self.shard, width = src.shape
        self.size = self.shard // halves
        self.send, self.recv, self.out, self.back = (functools.partial(lambda s, i: s.at[base + i], s) for s in sems)
        tiles = width // 128
        ends = [128 * (tiles * sum(shares[:k]) // sum(shares)) for k in range(4)]
        self.columns = [pl.ds(ends[k], ends[k + 1] - ends[k]) for k in range(3)]

    def rows_of(self, r, core, h=None):
        start = (2 * self.place.chip_at(r) + core) * self.shard
        return rows(start, self.shard) if h is None else rows(start + h * self.size, self.size)

    def piece(self, p, r, core, h):
        return self.dst.at[self.rows_of(r, core, h), self.columns[p]]

    @staticmethod
    def index(p, r, h):
        return 24 * h + 8 * p + 4 * r[0] + 2 * r[1] + r[2]

    def hop(self, p, r, h):
        d = [d for d in order(p) if r[d]][-1]
        q = tuple(r[e] * (e != d) for e in range(3))
        dst = self.piece(p, q, self.place.core, h)
        src = dst if any(q) else self.src.at[pl.ds(h * self.size, self.size), self.columns[p]]
        i = self.index(p, r, h)
        return remote(src, dst, self.send(i), self.recv(i), self.place.across(d))

    def arrive(self, p, r, h):
        view, i = self.piece(p, r, self.place.core, h), self.index(p, r, h)
        remote(view, view, self.send(i), self.recv(i), self.place.sibling).wait_recv()

    def share(self, p, r, h):
        view, i = self.piece(p, r, self.place.core, h), self.index(p, r, h)
        return remote(view, view, self.out(i), self.back(i), self.place.sibling)

    def shared(self, p, r, h):
        view, i = self.piece(p, r, 1 - self.place.core, h), self.index(p, r, h)
        remote(view, view, self.out(i), self.back(i), self.place.sibling).wait_recv()

    def share_own(self):
        return remote(self.src, self.dst.at[self.rows_of((0, 0, 0), self.place.core)], self.out(0), self.back(0), self.place.sibling)

    def shared_own(self):
        view = self.dst.at[self.rows_of((0, 0, 0), 1 - self.place.core)]
        remote(view, view, self.out(0), self.back(0), self.place.sibling).wait_recv()

    def shared_all(self, chips, h):
        for p in range(3):
            for r in chips:
                self.shared(p, r, h)

    def begin(self):
        self.share_own().start()
        for h in range(self.halves):
            for k in range(3):
                for d in range(3):
                    self.hop((d - k) % 3, across(d), h).start()

    def act(self, n, h=0):
        for p in range(3):
            a, b, c = order(p)
            seq = [across(a), across(b), across(c), across(a, b), across(a, c), across(b, c), across(a, b, c)]
            follow = {0: [across(a, b), across(a, c)], 1: [across(b, c)], 3: [across(a, b, c)]}
            self.arrive(p, seq[n], h)
            for r in follow.get(n, []):
                self.hop(p, r, h).start()
            self.share(p, seq[n], h).start()

    def drain(self):
        self.share_own().wait_send()
        for h in range(self.halves):
            for p in range(3):
                for r in OTHERS:
                    self.hop(p, r, h).wait_send()
                    self.share(p, r, h).wait_send()


def backward_kernel(x, dy, pre, w_down, w_in, x_all, dy_all, d_pre, hidden, dw_down, dx, dw_in, ici, d2d,
                    send, recv, out, back, w_sem, load_sem, pre_sem, hidden_sem, store_sem, own_sem, *scatter_sems):
    place = Place()
    shard, width = dy.shape
    half = shard // 2
    tokens, ff = pre.shape
    block = ff // 4
    place.barrier()
    sems = (send, recv, out, back)
    gather_dy = Gather(place, dy, dy_all, sems, 0, 2, (22, 21, 21))
    gather_x = Gather(place, x, x_all, sems, 48, 1, (25, 22, 17))
    gather_dy.begin()
    mine = gather_dy.rows_of(HERE[0], place.core)
    batches = [(HERE, None), (NEAR, 0), (NEAR, 1), (MIDDLE, 0), (MIDDLE, 1), (FAR, None)]

    def parts(n):
        chips, h = batches[n]
        size = shard if h is None else half
        cores = (place.core, 1 - place.core)
        return [(gather_dy.rows_of(r, c, h), pl.ds(k * size, size)) for k, (r, c) in enumerate((r, c) for r in chips for c in cores)]

    def rows_in(n):
        return sum(part.size for _, part in parts(n))

    def gradient(weights, lhs, slopes, result, values):
        def load_weights(j):
            part = rows(j * block, block)
            return pltpu.make_async_copy(w_down.at[part], weights.at[part], w_sem.at[j])

        def pre_loads(n):
            return [
                pltpu.make_async_copy(pre.at[src], values.at[n % 2, part], pre_sem.at[6 * (n % 2) + k])
                for k, (src, part) in enumerate(parts(n))
            ]

        def hidden_stores(n):
            return [
                pltpu.make_async_copy(values.at[n % 2, part], hidden.at[dst], hidden_sem.at[6 * (n % 2) + k])
                for k, (dst, part) in enumerate(parts(n))
            ]

        def row_load(n, k):
            src, part = parts(n)[k]
            there = dy if (n == 0 and k == 0) else dy_all.at[src]
            return pltpu.make_async_copy(there, lhs.at[n % 2, part], load_sem.at[6 * (n % 2) + k])

        def stores(n):
            return [
                pltpu.make_async_copy(result.at[n % 2, part], d_pre.at[dst], store_sem.at[6 * (n % 2) + k])
                for k, (dst, part) in enumerate(parts(n))
            ]

        def gelu(n):
            for copy in pre_loads(n):
                copy.wait()
            slot, some = n % 2, 32 if shard >= 64 else 16

            @pl.loop(0, rows_in(n) // some)
            def _(i):
                part = rows(i * some, some)
                value, pull = jax.vjp(act, values[slot, part, :].astype(F32))
                slopes[slot, part, :] = pull(jnp.ones_like(value))[0]
                values[slot, part, :] = value.astype(BF16)

            for copy in hidden_stores(n):
                copy.start()

        first = pl.ds(0, shard)
        own_row = pltpu.make_async_copy(lhs.at[0, first], dy_all.at[mine], own_sem.at[0])
        own_x = [
            pltpu.make_async_copy(x, lhs.at[1, first], own_sem.at[1]),
            pltpu.make_async_copy(lhs.at[1, first], x_all.at[mine], own_sem.at[1]),
        ]

        def arrivals(n):
            chips, h = batches[n]
            if chips is FAR:
                return [(6, 0), (6, 1)]
            return [(k + 3 * (chips is MIDDLE), h) for k in range(3)]

        def row_loads(n, mine):
            return [row_load(n, k) for k in range(1 - mine, len(parts(n)), 2)]

        for copy in pre_loads(0):
            copy.start()
        row_load(0, 0).start()
        load_weights(0).start()
        for copy in pre_loads(1):
            copy.start()
        gelu(0)
        gather_dy.shared_own()
        row_load(0, 1).start()
        for j in range(1, 4):
            load_weights(j).start()
        own_x[0].start()
        row_load(0, 0).wait()
        own_row.start()
        row_load(0, 1).wait()

        for n in range(6):
            if n:
                for copy in row_loads(n, True) + row_loads(n, False):
                    copy.wait()
            if n < 4 and n != 1:
                for copy in hidden_stores(n):
                    copy.wait()
                for copy in pre_loads(n + 2):
                    copy.start()
            if n >= 2:
                for copy in stores(n - 2):
                    copy.wait()
            size, slot = rows_in(n), n % 2
            pieces = arrivals(n + 1) if n < 5 else []

            @pl.loop(0, 4)
            def _(j):
                if n == 0:
                    load_weights(j).wait()
                for at, (k, h) in enumerate(pieces[:2]):
                    @pl.when(j == at + 2)
                    def _():
                        gather_dy.act(k, h)

                columns = lanes(j * block, block)
                d_hidden = dot(lhs[slot, :size], weights[rows(j * block, block), :], NT)
                result[slot, :size, columns] = (d_hidden * slopes[slot, :size, columns]).astype(BF16)

            for copy in stores(n):
                copy.start()
            if n == 0:
                own_x[0].wait()
                own_x[1].start()
                gelu(1)
                own_x[1].wait()
                for copy in hidden_stores(1):
                    copy.wait()
                for copy in pre_loads(3):
                    copy.start()
            if n == 3:
                gather_x.begin()
            if n < 4:
                gelu(n + 2)
            for k, h in pieces[2:]:
                gather_dy.act(k, h)
            if n < 5:
                if n == 1:
                    own_row.wait()
                for copy in row_loads(n + 1, True):
                    copy.start()
                chips, h = batches[n + 1]
                for h in (0, 1) if h is None else (h,):
                    gather_dy.shared_all(chips, h)
                for copy in row_loads(n + 1, False):
                    copy.start()
        for n in (4, 5):
            for copy in hidden_stores(n) + stores(n):
                copy.wait()

    pl.run_scoped(
        gradient,
        pltpu.VMEM((ff, width), BF16),
        pltpu.VMEM((2, 6 * half, width), BF16),
        pltpu.VMEM((2, 6 * half, ff), F32),
        pltpu.VMEM((2, 6 * half, ff), BF16),
        pltpu.VMEM((2, 6 * half, ff), BF16),
    )

    tm, tn = ff // 2, width // 8

    def down(loads):
        def product(h_ref, dy_ref, o_ref):
            at = pl.program_id(0) * pl.num_programs(1) + pl.program_id(1)
            group, place_in = lax.div(at, 3), lax.rem(at, 3)

            @pl.when(place_in == 1)
            def _():
                for n in range(5):
                    @pl.when(group == n)
                    def _():
                        gather_x.act(n)

            @pl.when(place_in == 2)
            def _():
                for n, some in enumerate(loads):
                    @pl.when(group == n)
                    def _():
                        for copy in some:
                            copy.start()

            @pl.when(at == 15)
            def _():
                gather_x.act(5)

            o_ref[...] = dot(h_ref[...], dy_ref[...], TN).astype(BF16)

        pltpu.emit_pipeline(
            product,
            grid=(2, 8),
            in_specs=[pl.BlockSpec((tokens, tm), lambda i, j: (0, i)), pl.BlockSpec((tokens, tn), lambda i, j: (0, j))],
            out_specs=[pl.BlockSpec((tm, tn), lambda i, j: (i, j))],
        )(hidden, dy_all, dw_down)

    def rest(lhs, weights, right):
        scatter(place, gather_x, down, x_all, d_pre, w_in, dx, dw_in, ici, d2d, lhs, weights, right, *scatter_sems)

    pl.run_scoped(
        rest, pltpu.VMEM((3, 8 * shard, ff), BF16), pltpu.VMEM((width // 4, ff), BF16), pltpu.VMEM((tokens, ff), BF16)
    )
    gather_dy.drain()
    gather_x.drain()


def scatter(place, gather_x, down, x_all, d_pre, w_in, dx, dw_in, ici, d2d, lhs_buf, weights, right,
            ici_send, ici_recv, d2d_send, d2d_recv, w_sem, load_sem, stage_sem, dx_sem, x_sem, dw_sem, right_sem):
    core = place.core
    shard, width = dx.shape
    tokens, ff = d_pre.shape
    n1, n2 = width // 16, width // 8

    def pick(i, group):
        k = lax.div(i, 3 * group)
        p = (1 - k) * lax.rem(i, 3) + k * odd(i)
        t = (1 - k) * lax.div(i, 3) + k * (group + lax.div(i - 3 * group, 2))
        return p, t

    def unpick(p, t, group):
        k = lax.div(t, group)
        return (1 - k) * (3 * t + p) + k * (3 * group + 2 * (t - group) + p)

    def turn(p, k):
        return lax.rem(p + k, 3)

    def narrow(i):
        p, t = pick(i, 4)
        return p, t, p * (3 * n2) + t * n1

    def wide(i):
        p, t = pick(i, 2)
        return p, t, p * (3 * n2) + t * n2

    def narrow_weights(i):
        slot = lax.rem(i, 4)
        return [pltpu.make_async_copy(w_in.at[rows(narrow(i)[2], n1)], weights.at[rows(slot * n1, n1)], w_sem.at[slot])]

    def wide_weights(i):
        start, slot = wide(i)[2], odd(i)
        return [
            pltpu.make_async_copy(w_in.at[rows(start + h * n1, n1)], weights.at[rows(slot * n2 + h * n1, n1)], w_sem.at[2 * slot + h])
            for h in (0, 1)
        ]

    def go(copies):
        for copy in copies:
            copy.start()

    def wait(copies):
        for copy in copies:
            copy.wait()

    def lhs_loads(p, first, chips, base):
        loads = []
        for half, c in enumerate((1 - core, core)):
            for k, r in enumerate(chips):
                src = d_pre.at[rows((2 * place.chip_at(r) + c) * shard, shard)]
                n = half * len(chips) + k
                loads.append(pltpu.make_async_copy(src, lhs_buf.at[p, pl.ds(first + n * shard, shard)], load_sem.at[base + n]))
        return loads

    def exchange(k, i, count, columns, base, part):
        region = (0, 4, 6)[k]
        dst = d2d.at[pl.ds(region * shard, count * shard), columns]
        return remote(part, dst, d2d_send.at[base + i], d2d_recv.at[base + i], place.sibling)

    def onward(k, i, count, p, columns, base, part):
        region = (0, 4, 6)[k]
        dst = ici.at[pl.ds(region * shard, count * shard), columns]
        return remote(part, dst, ici_send.at[base + i], ici_recv.at[base + i], place.across(turn(p, k)))

    def stage_chips(p, k):
        a, b, c = order(p)
        tail = [(0, 0), (0, 1), (1, 0), (1, 1)]
        if k == 0:
            return [tuple(across(a)[d] + s * across(b)[d] + t * across(c)[d] for d in range(3)) for s, t in tail]
        if k == 1:
            return [across(b), across(b, c)]
        return [across(c)] + HERE

    def stage(k, items, out, between, prepare=None, filler=None, keep=None, lag_b=1, lag_c=3):
        count, moved = (4, 2, 1)[k], (4, 2, 2)[k]
        size = n1 if k == 0 else n2
        base = (0, 16, 24)[k]
        locate = narrow if k == 0 else wide
        slots, n_term, n_staged = lag_c, 2, lag_c
        n_in = 1 + k
        from_ici = [(), ((2, 4),), ((1, 2), (5, 6))][k]

        def body(acc, term, staged):
            def columns(i):
                return lanes(locate(i)[2], size)

            def sources(i):
                region = (0, 4, 6)[k]
                views = [d2d.at[pl.ds(region * shard, count * shard), columns(i)]]
                views += [ici.at[pl.ds(a * shard, (b - a) * shard), columns(i)] for a, b in from_ici]
                slot = lax.rem(i, n_staged)
                return [
                    pltpu.make_async_copy(view, staged.at[slot, n], stage_sem.at[slot * n_in + n]) for n, view in enumerate(views)
                ]

            def send(i):
                return exchange(k, i, moved, columns(i), base, term.at[lax.rem(i, n_term)])

            def leave(i):
                return onward(k, i, count, locate(i)[0], columns(i), base, out.at[i])

            def fetch(j):
                view = d2d.at[pl.ds(0, moved * shard), columns(j)]
                remote(view, view, d2d_send.at[base + j], d2d_recv.at[base + j], place.sibling).wait_recv()
                p, t, start = locate(j)
                if k == 1:
                    for h in range(2):
                        n = unpick(p, 2 * t + h, 4)
                        view = ici.at[pl.ds(0, 4 * shard), lanes(start + h * n1, n1)]
                        remote(view, view, ici_send.at[n], ici_recv.at[n], place.sibling).wait_recv()
                elif k == 2:
                    n = 16 + j
                    view = ici.at[pl.ds(0, 2 * shard), columns(j)]
                    remote(view, view, ici_send.at[n], ici_recv.at[n], place.sibling).wait_recv()
                go(sources(j))

            def add(j, slot, there):
                total = acc[slot]
                for n in range(n_in):
                    total = total + staged[there, n].astype(F32)
                out[j] = total.astype(BF16)

            @pl.loop(0, items)
            def _(i):
                p, _, start = locate(i)
                slot = lax.rem(i, slots)
                wait(narrow_weights(i) if k == 0 else wide_weights(i))
                if prepare is not None:
                    prepare(i)

                @pl.when(i >= n_term)
                def _():
                    send(i - n_term).wait_send()

                @pl.when(i >= lag_c)
                def _():
                    wait(sources(i - lag_c))

                add(lax.max(i - lag_c, 0), slot, lax.rem(i, n_staged))
                if k == 0:
                    w = weights[rows(lax.rem(i, 4) * n1, n1), :]
                else:
                    w = weights[rows(odd(i) * n2, n2), :]
                value = dot(lhs_buf[p, pl.ds((k // 2) * 4 * shard, 2 * moved * shard)], w, NT)
                term[lax.rem(i, n_term)] = value[: moved * shard].astype(BF16)
                acc[slot] = value[moved * shard : (moved + count) * shard]
                if k == 2:
                    keep[i] = value[(moved + count) * shard :]
                send(i).start()

                @pl.when(i >= lag_c)
                def _():
                    leave(i - lag_c).start()

                if k == 0:
                    @pl.when(i + 4 < items)
                    def _():
                        go(narrow_weights(i + 4))

                    @pl.when(i == items - 3)
                    def _():
                        go(wide_weights(0))

                    @pl.when(i == items - 1)
                    def _():
                        go(wide_weights(1))
                elif k == 1:
                    go(wide_weights(lax.rem(i + 2, items)))
                else:
                    @pl.when(i + 2 < items)
                    def _():
                        go(wide_weights(i + 2))

                if filler is not None:
                    filler(i)

                @pl.when(i >= lag_b)
                def _():
                    fetch(i - lag_b)

            between()
            for j in range(items - lag_b, items):
                fetch(j)
            for j in range(items - lag_c, items):
                wait(sources(j))
                add(j, j % slots, j % n_staged)
                leave(j).start()
            for i in range(items - n_term, items):
                send(i).wait_send()

        pl.run_scoped(
            body,
            pltpu.VMEM((slots, count * shard, size), F32),
            pltpu.VMEM((n_term, moved * shard, size), BF16),
            pltpu.VMEM((n_staged, n_in, count * shard, size), BF16),
        )

    loads1 = [lhs_loads(p, 0, stage_chips(p, 0), 8 * p) for p in range(3)]
    loads2 = [lhs_loads(p, 0, stage_chips(p, 1), 24 + 4 * p) for p in range(3)]
    loads3 = [lhs_loads(p, 4 * shard, stage_chips(p, 2), 36 + 4 * p) for p in range(3)]
    right_load = pltpu.make_async_copy(d_pre, right, right_sem.at[0])
    down([[copy for i in range(4) for copy in narrow_weights(i)], *loads1, [right_load]])
    for some in loads1:
        wait(some)

    def main(out2, x_buf, dw_buf):
        def x_load(i):
            slot = odd(i)
            return pltpu.make_async_copy(x_all.at[:, lanes(i * n1, n1)], x_buf.at[slot], x_sem.at[slot])

        def dw_store(i):
            slot = odd(i)
            return pltpu.make_async_copy(dw_buf.at[slot], dw_in.at[rows(i * n1, n1)], dw_sem.at[slot])

        def tiles(a, b):
            @pl.loop(a, b)
            def _(i):
                slot = odd(i)
                x_load(i).wait()

                @pl.when(i >= 2)
                def _():
                    dw_store(i - 2).wait()

                @pl.loop(0, 2)
                def _(h):
                    part = lanes(h * (ff // 2), ff // 2)
                    dw_buf[slot, :, part] = dot(x_buf[slot], right[:, part], TN).astype(BF16)

                dw_store(i).start()

                @pl.when(i + 2 < HELD)
                def _():
                    x_load(i + 2).start()

        def fill2(i):
            turn, on = lax.div(i + 1, 3), lax.div(lax.rem(i, 3), 2)
            tiles(turn, turn + on * turn)

        def fill3(i):
            turn, on = lax.div(i + 1, 3), lax.div(lax.rem(i, 3), 2)
            tiles(4 + turn, 4 + turn + on)

        def early(out1):
            def prepare(i):
                @pl.when(i == 3)
                def _():
                    gather_x.act(6)

                @pl.when(i == 12)
                def _():
                    gather_x.shared_own()
                    gather_x.shared_all(OTHERS, 0)
                    x_load(0).start()
                    x_load(1).start()
                    go(loads2[2] + loads3[2])

                @pl.when(i == 15)
                def _():
                    go(loads2[0] + loads3[0])

            def between():
                go(loads2[1] + loads3[1])
                right_load.wait()
                tiles(0, 1)

            def prepare2(i):
                for p in range(3):
                    @pl.when(i == p)
                    def _():
                        wait(loads2[p] + loads3[p])

            stage(0, 16, out1, between, prepare=prepare)
            stage(1, 8, out2, lambda: tiles(4, 5), prepare=prepare2, filler=fill2)
            for i in range(16):
                onward(0, i, 4, narrow(i)[0], lanes(narrow(i)[2], n1), 0, out1.at[i]).wait_send()

        pl.run_scoped(early, pltpu.VMEM((16, 4 * shard, n1), BF16))

        def late(out3, keep):
            stage(2, 8, out3, lambda: tiles(7, 8), filler=fill3, keep=keep)
            pl.run_scoped(functools.partial(final, keep), pltpu.VMEM((8, shard, n2), BF16), pltpu.VMEM((4, 4, shard, n2), BF16))
            for i in range(8):
                onward(1, i, 2, wide(i)[0], lanes(wide(i)[2], n2), 16, out2.at[i]).wait_send()
                onward(2, i, 1, wide(i)[0], lanes(wide(i)[2], n2), 24, out3.at[i]).wait_send()

        def final(keep, out4, staged):
            def columns(i):
                return lanes(wide(i)[2], n2)

            def sources(i):
                views = [d2d.at[pl.ds(7 * shard, shard), columns(i)]]
                views += [ici.at[pl.ds(n * shard, shard), columns(i)] for n in (0, 4, 6)]
                slot = lax.rem(i, 4)
                return [pltpu.make_async_copy(view, staged.at[slot, n], stage_sem.at[4 * slot + n]) for n, view in enumerate(views)]

            def store(i):
                return pltpu.make_async_copy(out4.at[i], dx.at[:, columns(i)], dx_sem.at[i])

            @pl.loop(0, 8 + 3)
            def _(i):
                @pl.when(i >= 3)
                def _():
                    j = i - 3
                    wait(sources(j))
                    total = keep[j]
                    for n in range(4):
                        total = total + staged[lax.rem(j, 4), n].astype(F32)
                    out4[j] = total.astype(BF16)
                    store(j).start()

                @pl.when(i < 8)
                def _():
                    view = ici.at[pl.ds(0, shard), columns(i)]
                    remote(view, view, ici_send.at[24 + i], ici_recv.at[24 + i], place.sibling).wait_recv()
                    go(sources(i))

            dw_store(HELD - 2).wait()
            dw_store(HELD - 1).wait()
            for i in range(8):
                store(i).wait()

        pl.run_scoped(late, pltpu.VMEM((8, shard, n2), BF16), pltpu.VMEM((8, shard, n2), F32))

    pl.run_scoped(
        main,
        pltpu.VMEM((8, 2 * shard, n2), BF16),
        pltpu.VMEM((2, tokens, n1), BF16),
        pltpu.VMEM((2, n1, ff), BF16),
    )


def backward(x, dy, pre, w_in, w_down):
    shard, width = dy.shape
    tokens, ff = pre.shape
    dma = pltpu.SemaphoreType.DMA

    def shape(*size):
        return jax.ShapeDtypeStruct(size, BF16)

    x_all, _, d_pre, _, dw_down, dx, dw_in, _, _ = pl.pallas_call(
        backward_kernel,
        in_specs=[ANY] * 5,
        out_specs=[ANY] * 9,
        out_shape=[
            shape(tokens, width),
            shape(tokens, width),
            shape(tokens, ff),
            shape(tokens, ff),
            shape(ff, width),
            shape(shard, width),
            shape(HELD * width // 16, ff),
            shape(7 * shard, width),
            shape(8 * shard, width),
        ],
        scratch_shapes=[dma((n,)) for n in [72] * 4 + [4] + [12] * 4 + [2] + [32] * 4 + [4, 48, 16, 8, 2, 2, 1]],
        compiler_params=pltpu.CompilerParams(collective_id=0, has_side_effects=True, vmem_limit_bytes=VMEM_LIMIT),
        cost_estimate=pl.CostEstimate(flops=7 * tokens * ff * width, bytes_accessed=800_000_000, transcendentals=tokens * ff),
        name="backward",
    )(x, dy, pre, w_down, w_in)
    return x_all, d_pre, dw_down, dx, dw_in


def finish_kernel(x_ref, d_pre_ref, part_ref, down_ref, dx_part, dw_in, dw_down, dx, buf, dx_buf, copy_sem, buf_sem, dx_sem):
    i = pl.program_id(0)
    n, ff = part_ref.shape
    count = pl.num_programs(0)
    slot = lax.rem(i, 2)
    copies = [
        pltpu.make_async_copy(part_ref, dw_in.at[rows(i * n, n)], copy_sem.at[0]),
        pltpu.make_async_copy(down_ref, dw_down.at[rows(i * down_ref.shape[0], down_ref.shape[0])], copy_sem.at[1]),
    ]

    def store(i):
        slot = lax.rem(i, 2)
        return pltpu.make_async_copy(buf.at[slot], dw_in.at[rows((count + i) * n, n)], buf_sem.at[slot])

    for copy in copies:
        copy.start()

    through = [pltpu.make_async_copy(dx_part, dx_buf, dx_sem.at[0]), pltpu.make_async_copy(dx_buf, dx, dx_sem.at[1])]

    @pl.when(i == 0)
    def _():
        through[0].start()

    @pl.when(i == 1)
    def _():
        through[0].wait()
        through[1].start()

    @pl.when(i >= 2)
    def _():
        store(i - 2).wait()

    @pl.loop(0, 2)
    def _(h):
        half = lanes(h * (ff // 2), ff // 2)
        buf[slot, :, half] = dot(x_ref[...], d_pre_ref[:, half], TN).astype(BF16)

    store(i).start()
    for copy in copies:
        copy.wait()

    @pl.when(i == count - 1)
    def _():
        through[1].wait()
        store(i - 1).wait()
        store(i).wait()


def finish(x_all, d_pre, dw_in_part, dw_down_part, dx_part):
    tokens, ff = d_pre.shape
    width = x_all.shape[1]
    n = width // 16
    return pl.pallas_call(
        finish_kernel,
        grid=(8,),
        in_specs=[
            pl.BlockSpec((tokens, n), lambda i: (0, 8 + i)),
            pl.BlockSpec((tokens, ff), lambda i: (0, 0)),
            pl.BlockSpec((n, ff), lambda i: (i, 0)),
            pl.BlockSpec((ff // 8, width), lambda i: (i, 0)),
            ANY,
        ],
        out_specs=[ANY] * 3,
        out_shape=[jax.ShapeDtypeStruct(size, BF16) for size in ((width, ff), (ff, width), dx_part.shape)],
        scratch_shapes=[pltpu.VMEM((2, n, ff), BF16), pltpu.VMEM(dx_part.shape, BF16)] + [pltpu.SemaphoreType.DMA((2,))] * 3,
        compiler_params=pltpu.CompilerParams(dimension_semantics=("arbitrary",), vmem_limit_bytes=VMEM_LIMIT),
        cost_estimate=pl.CostEstimate(flops=tokens * ff * width, bytes_accessed=140_000_000, transcendentals=0),
        name="finish",
    )(x_all, d_pre, dw_in_part, dw_down_part, dx_part)


def solution(mesh):
    def body(x, dy, pre, w_in, w_down):
        x_all, d_pre, dw_down, dx, dw_in = backward(x, dy, pre, w_in, w_down)
        dw_in, dw_down, dx = finish(x_all, d_pre, dw_in, dw_down, dx)
        return dx, dw_in, dw_down

    return jax.shard_map(
        body,
        mesh=mesh,
        in_specs=(P(("dp", "tp")), P(("dp", "tp")), P("dp", "tp"), P(None, "tp"), P("tp", None)),
        out_specs=(P(("dp", "tp")), P("dp", "tp"), P(("dp", "tp"))),
        check_vma=False,
    )
```

```python
import functools

import jax
import jax.numpy as jnp
from jax import lax
from jax.experimental import pallas as pl
from jax.experimental.pallas import tpu as pltpu
from jax.sharding import PartitionSpec as P

VMEM_LIMIT = 67_000_000
WEIGHT = (4, 2, 1)
HELD = 8
F32, BF16 = jnp.float32, jnp.bfloat16
ANY = pl.BlockSpec(memory_space=pl.ANY)


def act(pre):
    return jax.nn.gelu(pre)


def dot(a, b, dims):
    return lax.dot_general(a, b, (dims, ((), ())), preferred_element_type=F32)


NT, TN = ((1,), (1,)), ((0,), (0,))


def odd(i):
    return lax.rem(i, 2)


def rows(start, size):
    return pl.ds(pl.multiple_of(start, 16), size)


def lanes(start, size):
    return pl.ds(pl.multiple_of(start, 128), size)


class Place:
    def __init__(self):
        me = lax.axis_index("tp")
        self.chip, self.core = lax.div(me, 2), lax.rem(me, 2)
        self.step = [w * (1 - 2 * lax.rem(lax.div(self.chip, w), 2)) for w in WEIGHT]
        self.sibling = self.device(self.chip, 1 - self.core)

    def chip_at(self, r):
        return self.chip + sum(self.step[d] * r[d] for d in range(3) if isinstance(r[d], jax.Array) or r[d])

    def device(self, chip, core):
        return {"tp": 2 * chip + core}

    def across(self, d):
        if isinstance(d, int):
            return self.device(self.chip + self.step[d], self.core)
        r = (lax.div(2 - d, 2), lax.rem(d, 2), lax.div(d, 2))
        return self.device(self.chip_at(r), self.core)

    def barrier(self):
        sem = pltpu.get_barrier_semaphore()
        for peer in [self.sibling] + [self.across(d) for d in range(3)]:
            pl.semaphore_signal(sem, inc=1, device_id=peer, device_id_type=pl.DeviceIdType.MESH)
        pl.semaphore_wait(sem, 4)


def remote(src, dst, send, recv, device):
    return pltpu.make_async_remote_copy(src, dst, send, recv, device_id=device, device_id_type=pl.DeviceIdType.MESH)


def order(p):
    return p, (p + 1) % 3, (p + 2) % 3


def across(*dims):
    return tuple(int(d in dims) for d in range(3))


HERE, NEAR, FAR = [across()], [across(d) for d in range(3)], [across(*range(3))]
MIDDLE = [across(*order(d)[:2]) for d in range(3)]
OTHERS = NEAR + MIDDLE + FAR


class Gather:
    def __init__(self, place, src, dst, sems, base, halves, shares):
        self.place, self.src, self.dst, self.halves = place, src, dst, halves
        self.shard, width = src.shape
        self.size = self.shard // halves
        self.send, self.recv, self.out, self.back = (functools.partial(lambda s, i: s.at[base + i], s) for s in sems)
        tiles = width // 128
        ends = [128 * (tiles * sum(shares[:k]) // sum(shares)) for k in range(4)]
        self.columns = [pl.ds(ends[k], ends[k + 1] - ends[k]) for k in range(3)]

    def rows_of(self, r, core, h=None):
        start = (2 * self.place.chip_at(r) + core) * self.shard
        return rows(start, self.shard) if h is None else rows(start + h * self.size, self.size)

    def piece(self, p, r, core, h):
        return self.dst.at[self.rows_of(r, core, h), self.columns[p]]

    @staticmethod
    def index(p, r, h):
        return 24 * h + 8 * p + 4 * r[0] + 2 * r[1] + r[2]

    def hop(self, p, r, h):
        d = [d for d in order(p) if r[d]][-1]
        q = tuple(r[e] * (e != d) for e in range(3))
        dst = self.piece(p, q, self.place.core, h)
        src = dst if any(q) else self.src.at[pl.ds(h * self.size, self.size), self.columns[p]]
        i = self.index(p, r, h)
        return remote(src, dst, self.send(i), self.recv(i), self.place.across(d))

    def arrive(self, p, r, h):
        view, i = self.piece(p, r, self.place.core, h), self.index(p, r, h)
        remote(view, view, self.send(i), self.recv(i), self.place.sibling).wait_recv()

    def share(self, p, r, h):
        view, i = self.piece(p, r, self.place.core, h), self.index(p, r, h)
        return remote(view, view, self.out(i), self.back(i), self.place.sibling)

    def shared(self, p, r, h):
        view, i = self.piece(p, r, 1 - self.place.core, h), self.index(p, r, h)
        remote(view, view, self.out(i), self.back(i), self.place.sibling).wait_recv()

    def share_own(self):
        return remote(self.src, self.dst.at[self.rows_of((0, 0, 0), self.place.core)], self.out(0), self.back(0), self.place.sibling)

    def shared_own(self):
        view = self.dst.at[self.rows_of((0, 0, 0), 1 - self.place.core)]
        remote(view, view, self.out(0), self.back(0), self.place.sibling).wait_recv()

    def shared_all(self, chips, h):
        for p in range(3):
            for r in chips:
                self.shared(p, r, h)

    def begin(self):
        self.share_own().start()
        for h in range(self.halves):
            for k in range(3):
                for d in range(3):
                    self.hop((d - k) % 3, across(d), h).start()

    def act(self, n, h=0):
        for p in range(3):
            a, b, c = order(p)
            seq = [across(a), across(b), across(c), across(a, b), across(a, c), across(b, c), across(a, b, c)]
            follow = {0: [across(a, b), across(a, c)], 1: [across(b, c)], 3: [across(a, b, c)]}
            self.arrive(p, seq[n], h)
            for r in follow.get(n, []):
                self.hop(p, r, h).start()
            self.share(p, seq[n], h).start()

    def drain(self):
        self.share_own().wait_send()
        for h in range(self.halves):
            for p in range(3):
                for r in OTHERS:
                    self.hop(p, r, h).wait_send()
                    self.share(p, r, h).wait_send()


def backward_kernel(x, dy, pre, w_down, w_in, x_all, dy_all, d_pre, hidden, dw_down, dx, dw_in, ici, d2d,
                    send, recv, out, back, w_sem, load_sem, pre_sem, hidden_sem, store_sem, own_sem, *scatter_sems):
    place = Place()
    shard, width = dy.shape
    half = shard // 2
    tokens, ff = pre.shape
    block = ff // 4
    place.barrier()
    sems = (send, recv, out, back)
    gather_dy = Gather(place, dy, dy_all, sems, 0, 2, (22, 21, 21))
    gather_x = Gather(place, x, x_all, sems, 48, 1, (25, 22, 17))
    gather_dy.begin()
    mine = gather_dy.rows_of(HERE[0], place.core)
    batches = [(HERE, None), (NEAR, 0), (NEAR, 1), (MIDDLE, 0), (MIDDLE, 1), (FAR, None)]

    def parts(n):
        chips, h = batches[n]
        size = shard if h is None else half
        cores = (place.core, 1 - place.core)
        return [(gather_dy.rows_of(r, c, h), pl.ds(k * size, size)) for k, (r, c) in enumerate((r, c) for r in chips for c in cores)]

    def rows_in(n):
        return sum(part.size for _, part in parts(n))

    def gradient(weights, lhs, slopes, result, values):
        def load_weights(j):
            part = rows(j * block, block)
            return pltpu.make_async_copy(w_down.at[part], weights.at[part], w_sem.at[j])

        def pre_loads(n):
            return [
                pltpu.make_async_copy(pre.at[src], values.at[n % 2, part], pre_sem.at[6 * (n % 2) + k])
                for k, (src, part) in enumerate(parts(n))
            ]

        def hidden_stores(n):
            return [
                pltpu.make_async_copy(values.at[n % 2, part], hidden.at[dst], hidden_sem.at[6 * (n % 2) + k])
                for k, (dst, part) in enumerate(parts(n))
            ]

        def row_load(n, k):
            src, part = parts(n)[k]
            there = dy if (n == 0 and k == 0) else dy_all.at[src]
            return pltpu.make_async_copy(there, lhs.at[n % 2, part], load_sem.at[6 * (n % 2) + k])

        def stores(n):
            return [
                pltpu.make_async_copy(result.at[n % 2, part], d_pre.at[dst], store_sem.at[6 * (n % 2) + k])
                for k, (dst, part) in enumerate(parts(n))
            ]

        def gelu(n):
            for copy in pre_loads(n):
                copy.wait()
            slot, some = n % 2, 32 if shard >= 64 else 16

            @pl.loop(0, rows_in(n) // some)
            def _(i):
                part = rows(i * some, some)
                value, pull = jax.vjp(act, values[slot, part, :].astype(F32))
                slopes[slot, part, :] = pull(jnp.ones_like(value))[0]
                values[slot, part, :] = value.astype(BF16)

            for copy in hidden_stores(n):
                copy.start()

        first = pl.ds(0, shard)
        own_row = pltpu.make_async_copy(lhs.at[0, first], dy_all.at[mine], own_sem.at[0])
        own_x = [
            pltpu.make_async_copy(x, lhs.at[1, first], own_sem.at[1]),
            pltpu.make_async_copy(lhs.at[1, first], x_all.at[mine], own_sem.at[1]),
        ]

        def arrivals(n):
            chips, h = batches[n]
            if chips is FAR:
                return [(6, 0), (6, 1)]
            return [(k + 3 * (chips is MIDDLE), h) for k in range(3)]

        def row_loads(n, mine):
            return [row_load(n, k) for k in range(1 - mine, len(parts(n)), 2)]

        for copy in pre_loads(0):
            copy.start()
        row_load(0, 0).start()
        load_weights(0).start()
        for copy in pre_loads(1):
            copy.start()
        gelu(0)
        gather_dy.shared_own()
        row_load(0, 1).start()
        for j in range(1, 4):
            load_weights(j).start()
        own_x[0].start()
        row_load(0, 0).wait()
        own_row.start()
        row_load(0, 1).wait()

        for n in range(6):
            if n:
                for copy in row_loads(n, True) + row_loads(n, False):
                    copy.wait()
            if n < 4 and n != 1:
                for copy in hidden_stores(n):
                    copy.wait()
                for copy in pre_loads(n + 2):
                    copy.start()
            if n >= 2:
                for copy in stores(n - 2):
                    copy.wait()
            size, slot = rows_in(n), n % 2
            pieces = arrivals(n + 1) if n < 5 else []

            @pl.loop(0, 4)
            def _(j):
                if n == 0:
                    load_weights(j).wait()
                for at, (k, h) in enumerate(pieces[:2]):
                    @pl.when(j == at + 2)
                    def _():
                        gather_dy.act(k, h)

                columns = lanes(j * block, block)
                d_hidden = dot(lhs[slot, :size], weights[rows(j * block, block), :], NT)
                result[slot, :size, columns] = (d_hidden * slopes[slot, :size, columns]).astype(BF16)

            for copy in stores(n):
                copy.start()
            if n == 0:
                own_x[0].wait()
                own_x[1].start()
                gelu(1)
                own_x[1].wait()
                for copy in hidden_stores(1):
                    copy.wait()
                for copy in pre_loads(3):
                    copy.start()
            if n == 3:
                gather_x.begin()
            if n < 4:
                gelu(n + 2)
            for k, h in pieces[2:]:
                gather_dy.act(k, h)
            if n < 5:
                if n == 1:
                    own_row.wait()
                for copy in row_loads(n + 1, True):
                    copy.start()
                chips, h = batches[n + 1]
                for h in (0, 1) if h is None else (h,):
                    gather_dy.shared_all(chips, h)
                for copy in row_loads(n + 1, False):
                    copy.start()
        for n in (4, 5):
            for copy in hidden_stores(n) + stores(n):
                copy.wait()

    pl.run_scoped(
        gradient,
        pltpu.VMEM((ff, width), BF16),
        pltpu.VMEM((2, 6 * half, width), BF16),
        pltpu.VMEM((2, 6 * half, ff), F32),
        pltpu.VMEM((2, 6 * half, ff), BF16),
        pltpu.VMEM((2, 6 * half, ff), BF16),
    )

    tm, tn = ff // 2, width // 8

    def down(loads):
        def product(h_ref, dy_ref, o_ref):
            at = pl.program_id(0) * pl.num_programs(1) + pl.program_id(1)
            group, place_in = lax.div(at, 3), lax.rem(at, 3)

            @pl.when(place_in == 0)
            def _():
                for n in range(5):
                    @pl.when(group == n + 1)
                    def _():
                        gather_x.act(n)

            @pl.when(place_in == 2)
            def _():
                for n, some in enumerate(loads):
                    @pl.when(group == n)
                    def _():
                        for copy in some:
                            copy.start()

            o_ref[...] = dot(h_ref[...], dy_ref[...], TN).astype(BF16)

        pltpu.emit_pipeline(
            product,
            grid=(2, 8),
            in_specs=[pl.BlockSpec((tokens, tm), lambda i, j: (0, i)), pl.BlockSpec((tokens, tn), lambda i, j: (0, j))],
            out_specs=[pl.BlockSpec((tm, tn), lambda i, j: (i, j))],
        )(hidden, dy_all, dw_down)

    def rest(lhs, weights, right):
        scatter(place, gather_x, down, x_all, d_pre, w_in, dx, dw_in, ici, d2d, lhs, weights, right, *scatter_sems)

    pl.run_scoped(
        rest, pltpu.VMEM((3, 8 * shard, ff), BF16), pltpu.VMEM((width // 4, ff), BF16), pltpu.VMEM((tokens, ff), BF16)
    )
    gather_dy.drain()
    gather_x.drain()


def scatter(place, gather_x, down, x_all, d_pre, w_in, dx, dw_in, ici, d2d, lhs_buf, weights, right,
            ici_send, ici_recv, d2d_send, d2d_recv, w_sem, load_sem, stage_sem, dx_sem, x_sem, dw_sem, right_sem):
    core = place.core
    shard, width = dx.shape
    tokens, ff = d_pre.shape
    n1, n2 = width // 16, width // 8

    def pick(i, group):
        k = lax.div(i, 3 * group)
        p = (1 - k) * lax.rem(i, 3) + k * odd(i)
        t = (1 - k) * lax.div(i, 3) + k * (group + lax.div(i - 3 * group, 2))
        return p, t

    def unpick(p, t, group):
        k = lax.div(t, group)
        return (1 - k) * (3 * t + p) + k * (3 * group + 2 * (t - group) + p)

    def turn(p, k):
        return lax.rem(p + k, 3)

    def narrow(i):
        p, t = pick(i, 4)
        return p, t, p * (3 * n2) + t * n1

    def wide(i):
        p, t = pick(i, 2)
        return p, t, p * (3 * n2) + t * n2

    def narrow_weights(i):
        slot = lax.rem(i, 4)
        return [pltpu.make_async_copy(w_in.at[rows(narrow(i)[2], n1)], weights.at[rows(slot * n1, n1)], w_sem.at[slot])]

    def wide_weights(i):
        start, slot = wide(i)[2], odd(i)
        return [
            pltpu.make_async_copy(w_in.at[rows(start + h * n1, n1)], weights.at[rows(slot * n2 + h * n1, n1)], w_sem.at[2 * slot + h])
            for h in (0, 1)
        ]

    def go(copies):
        for copy in copies:
            copy.start()

    def wait(copies):
        for copy in copies:
            copy.wait()

    def lhs_loads(p, first, chips, base):
        loads = []
        for half, c in enumerate((1 - core, core)):
            for k, r in enumerate(chips):
                src = d_pre.at[rows((2 * place.chip_at(r) + c) * shard, shard)]
                n = half * len(chips) + k
                loads.append(pltpu.make_async_copy(src, lhs_buf.at[p, pl.ds(first + n * shard, shard)], load_sem.at[base + n]))
        return loads

    def exchange(k, i, count, columns, base, part):
        region = (0, 4, 6)[k]
        dst = d2d.at[pl.ds(region * shard, count * shard), columns]
        return remote(part, dst, d2d_send.at[base + i], d2d_recv.at[base + i], place.sibling)

    def onward(k, i, count, p, columns, base, part):
        region = (0, 4, 6)[k]
        dst = ici.at[pl.ds(region * shard, count * shard), columns]
        return remote(part, dst, ici_send.at[base + i], ici_recv.at[base + i], place.across(turn(p, k)))

    def stage_chips(p, k):
        a, b, c = order(p)
        tail = [(0, 0), (0, 1), (1, 0), (1, 1)]
        if k == 0:
            return [tuple(across(a)[d] + s * across(b)[d] + t * across(c)[d] for d in range(3)) for s, t in tail]
        if k == 1:
            return [across(b), across(b, c)]
        return [across(c)] + HERE

    def stage(k, items, out, between, prepare=None, filler=None, keep=None, lag_b=1, lag_c=3):
        count, moved = (4, 2, 1)[k], (4, 2, 2)[k]
        size = n1 if k == 0 else n2
        base = (0, 16, 24)[k]
        locate = narrow if k == 0 else wide
        slots, n_term, n_staged = lag_c, 2, lag_c
        n_in = 1 + k
        from_ici = [(), ((2, 4),), ((1, 2), (5, 6))][k]

        def body(acc, term, staged):
            def columns(i):
                return lanes(locate(i)[2], size)

            def sources(i):
                region = (0, 4, 6)[k]
                views = [d2d.at[pl.ds(region * shard, count * shard), columns(i)]]
                views += [ici.at[pl.ds(a * shard, (b - a) * shard), columns(i)] for a, b in from_ici]
                slot = lax.rem(i, n_staged)
                return [
                    pltpu.make_async_copy(view, staged.at[slot, n], stage_sem.at[slot * n_in + n]) for n, view in enumerate(views)
                ]

            def send(i):
                return exchange(k, i, moved, columns(i), base, term.at[lax.rem(i, n_term)])

            def leave(i):
                return onward(k, i, count, locate(i)[0], columns(i), base, out.at[i])

            def fetch(j):
                view = d2d.at[pl.ds(0, moved * shard), columns(j)]
                remote(view, view, d2d_send.at[base + j], d2d_recv.at[base + j], place.sibling).wait_recv()
                p, t, start = locate(j)
                if k == 1:
                    for h in range(2):
                        n = unpick(p, 2 * t + h, 4)
                        view = ici.at[pl.ds(0, 4 * shard), lanes(start + h * n1, n1)]
                        remote(view, view, ici_send.at[n], ici_recv.at[n], place.sibling).wait_recv()
                elif k == 2:
                    n = 16 + j
                    view = ici.at[pl.ds(0, 2 * shard), columns(j)]
                    remote(view, view, ici_send.at[n], ici_recv.at[n], place.sibling).wait_recv()
                go(sources(j))

            def add(j, slot, there):
                total = acc[slot]
                for n in range(n_in):
                    total = total + staged[there, n].astype(F32)
                out[j] = total.astype(BF16)

            @pl.loop(0, items)
            def _(i):
                p, _, start = locate(i)
                slot = lax.rem(i, slots)
                wait(narrow_weights(i) if k == 0 else wide_weights(i))
                if prepare is not None:
                    prepare(i)

                @pl.when(i >= n_term)
                def _():
                    send(i - n_term).wait_send()

                @pl.when(i >= lag_c)
                def _():
                    wait(sources(i - lag_c))

                add(lax.max(i - lag_c, 0), slot, lax.rem(i, n_staged))
                if k == 0:
                    w = weights[rows(lax.rem(i, 4) * n1, n1), :]
                else:
                    w = weights[rows(odd(i) * n2, n2), :]
                value = dot(lhs_buf[p, pl.ds((k // 2) * 4 * shard, 2 * moved * shard)], w, NT)
                term[lax.rem(i, n_term)] = value[: moved * shard].astype(BF16)
                acc[slot] = value[moved * shard : (moved + count) * shard]
                if k == 2:
                    keep[i] = value[(moved + count) * shard :]
                send(i).start()

                @pl.when(i >= lag_c)
                def _():
                    leave(i - lag_c).start()

                if k == 0:
                    @pl.when(i + 4 < items)
                    def _():
                        go(narrow_weights(i + 4))

                    @pl.when(i == items - 3)
                    def _():
                        go(wide_weights(0))

                    @pl.when(i == items - 1)
                    def _():
                        go(wide_weights(1))
                elif k == 1:
                    go(wide_weights(lax.rem(i + 2, items)))
                else:
                    @pl.when(i + 2 < items)
                    def _():
                        go(wide_weights(i + 2))

                if filler is not None:
                    filler(i)

                @pl.when(i >= lag_b)
                def _():
                    fetch(i - lag_b)

            def close(j):
                wait(sources(j))
                add(j, j % slots, j % n_staged)
                leave(j).start()

            def midway():
                fetch(items - 1)
                close(items - 2)

            close(items - 3)
            between(midway)
            close(items - 1)

            for i in range(items - n_term, items):
                send(i).wait_send()

        pl.run_scoped(
            body,
            pltpu.VMEM((slots, count * shard, size), F32),
            pltpu.VMEM((n_term, moved * shard, size), BF16),
            pltpu.VMEM((n_staged, n_in, count * shard, size), BF16),
        )

    loads1 = [lhs_loads(p, 0, stage_chips(p, 0), 8 * p) for p in range(3)]
    loads2 = [lhs_loads(p, 0, stage_chips(p, 1), 24 + 4 * p) for p in range(3)]
    loads3 = [lhs_loads(p, 4 * shard, stage_chips(p, 2), 36 + 4 * p) for p in range(3)]
    right_load = pltpu.make_async_copy(d_pre, right, right_sem.at[0])
    down([[copy for i in range(4) for copy in narrow_weights(i)], *loads1, [right_load]])
    for some in loads1:
        wait(some)

    def main(out2, x_buf, dw_buf):
        def x_load(i):
            slot = odd(i)
            return pltpu.make_async_copy(x_all.at[:, lanes(i * n1, n1)], x_buf.at[slot], x_sem.at[slot])

        def dw_store(i):
            slot = odd(i)
            return pltpu.make_async_copy(dw_buf.at[slot], dw_in.at[rows(i * n1, n1)], dw_sem.at[slot])

        def tiles(a, b, midway=None):
            @pl.loop(a, b)
            def _(i):
                slot = odd(i)
                x_load(i).wait()

                @pl.when(i >= 2)
                def _():
                    dw_store(i - 2).wait()

                @pl.loop(0, 2)
                def _(h):
                    if midway is not None:
                        @pl.when(h == 1)
                        def _():
                            midway()

                    part = lanes(h * (ff // 2), ff // 2)
                    dw_buf[slot, :, part] = dot(x_buf[slot], right[:, part], TN).astype(BF16)

                dw_store(i).start()

                @pl.when(i + 2 < HELD)
                def _():
                    x_load(i + 2).start()

        def fill2(i):
            turn, on = lax.div(i + 1, 3), lax.div(lax.rem(i, 3), 2)
            tiles(turn, turn + on * turn)

        def fill3(i):
            turn, on = lax.div(i + 1, 3), lax.div(lax.rem(i, 3), 2)
            tiles(4 + turn, 4 + turn + on)

        def early(out1):
            def prepare(i):
                for n in (5, 6):
                    @pl.when(i == 6 * n - 27)
                    def _():
                        gather_x.act(n)

                @pl.when(i == 12)
                def _():
                    gather_x.shared_own()
                    gather_x.shared_all(OTHERS, 0)
                    x_load(0).start()
                    x_load(1).start()
                    go(loads2[2] + loads3[2])

                @pl.when(i == 15)
                def _():
                    go(loads2[0] + loads3[0])

            def between(midway):
                go(loads2[1] + loads3[1])
                right_load.wait()
                tiles(0, 1, midway)

            def prepare2(i):
                for p in range(3):
                    @pl.when(i == p)
                    def _():
                        wait(loads2[p] + loads3[p])

            stage(0, 16, out1, between, prepare=prepare)
            stage(1, 8, out2, lambda midway: tiles(4, 5, midway), prepare=prepare2, filler=fill2)
            for i in range(16):
                onward(0, i, 4, narrow(i)[0], lanes(narrow(i)[2], n1), 0, out1.at[i]).wait_send()

        pl.run_scoped(early, pltpu.VMEM((16, 4 * shard, n1), BF16))

        def late(out3, keep):
            stage(2, 8, out3, lambda midway: tiles(7, 8, midway), filler=fill3, keep=keep)
            pl.run_scoped(functools.partial(final, keep), pltpu.VMEM((8, shard, n2), BF16), pltpu.VMEM((4, 4, shard, n2), BF16))
            for i in range(8):
                onward(1, i, 2, wide(i)[0], lanes(wide(i)[2], n2), 16, out2.at[i]).wait_send()
                onward(2, i, 1, wide(i)[0], lanes(wide(i)[2], n2), 24, out3.at[i]).wait_send()

        def final(keep, out4, staged):
            def columns(i):
                return lanes(wide(i)[2], n2)

            def sources(i):
                views = [d2d.at[pl.ds(7 * shard, shard), columns(i)]]
                views += [ici.at[pl.ds(n * shard, shard), columns(i)] for n in (0, 4, 6)]
                slot = lax.rem(i, 4)
                return [pltpu.make_async_copy(view, staged.at[slot, n], stage_sem.at[4 * slot + n]) for n, view in enumerate(views)]

            def store(i):
                return pltpu.make_async_copy(out4.at[i], dx.at[:, columns(i)], dx_sem.at[i])

            @pl.loop(0, 8 + 3)
            def _(i):
                @pl.when(i >= 3)
                def _():
                    j = i - 3
                    wait(sources(j))
                    total = keep[j]
                    for n in range(4):
                        total = total + staged[lax.rem(j, 4), n].astype(F32)
                    out4[j] = total.astype(BF16)
                    store(j).start()

                @pl.when(i < 8)
                def _():
                    view = ici.at[pl.ds(0, shard), columns(i)]
                    remote(view, view, ici_send.at[24 + i], ici_recv.at[24 + i], place.sibling).wait_recv()
                    go(sources(i))

            dw_store(HELD - 2).wait()
            dw_store(HELD - 1).wait()
            for i in range(8):
                store(i).wait()

        pl.run_scoped(late, pltpu.VMEM((8, shard, n2), BF16), pltpu.VMEM((8, shard, n2), F32))

    pl.run_scoped(
        main,
        pltpu.VMEM((8, 2 * shard, n2), BF16),
        pltpu.VMEM((2, tokens, n1), BF16),
        pltpu.VMEM((2, n1, ff), BF16),
    )


def backward(x, dy, pre, w_in, w_down):
    shard, width = dy.shape
    tokens, ff = pre.shape
    dma = pltpu.SemaphoreType.DMA

    def shape(*size):
        return jax.ShapeDtypeStruct(size, BF16)

    x_all, _, d_pre, _, dw_down, dx, dw_in, _, _ = pl.pallas_call(
        backward_kernel,
        in_specs=[ANY] * 5,
        out_specs=[ANY] * 9,
        out_shape=[
            shape(tokens, width),
            shape(tokens, width),
            shape(tokens, ff),
            shape(tokens, ff),
            shape(ff, width),
            shape(shard, width),
            shape(HELD * width // 16, ff),
            shape(7 * shard, width),
            shape(8 * shard, width),
        ],
        scratch_shapes=[dma((n,)) for n in [72] * 4 + [4] + [12] * 4 + [2] + [32] * 4 + [4, 48, 16, 8, 2, 2, 1]],
        compiler_params=pltpu.CompilerParams(collective_id=0, has_side_effects=True, vmem_limit_bytes=VMEM_LIMIT),
        cost_estimate=pl.CostEstimate(flops=7 * tokens * ff * width, bytes_accessed=800_000_000, transcendentals=tokens * ff),
        name="backward",
    )(x, dy, pre, w_down, w_in)
    return x_all, d_pre, dw_down, dx, dw_in


def finish_kernel(x_ref, d_pre_ref, part_ref, down_ref, dx_part, dw_in, dw_down, dx, buf, dx_buf, copy_sem, buf_sem, dx_sem):
    i = pl.program_id(0)
    n, ff = part_ref.shape
    count = pl.num_programs(0)
    slot = lax.rem(i, 2)
    copies = [
        pltpu.make_async_copy(part_ref, dw_in.at[rows(i * n, n)], copy_sem.at[0]),
        pltpu.make_async_copy(down_ref, dw_down.at[rows(i * down_ref.shape[0], down_ref.shape[0])], copy_sem.at[1]),
    ]

    def store(i):
        slot = lax.rem(i, 2)
        return pltpu.make_async_copy(buf.at[slot], dw_in.at[rows((count + i) * n, n)], buf_sem.at[slot])

    for copy in copies:
        copy.start()

    through = [pltpu.make_async_copy(dx_part, dx_buf, dx_sem.at[0]), pltpu.make_async_copy(dx_buf, dx, dx_sem.at[1])]

    @pl.when(i == 0)
    def _():
        through[0].start()

    @pl.when(i == 1)
    def _():
        through[0].wait()
        through[1].start()

    @pl.when(i >= 2)
    def _():
        store(i - 2).wait()

    @pl.loop(0, 2)
    def _(h):
        half = lanes(h * (ff // 2), ff // 2)
        buf[slot, :, half] = dot(x_ref[...], d_pre_ref[:, half], TN).astype(BF16)

    store(i).start()
    for copy in copies:
        copy.wait()

    @pl.when(i == count - 1)
    def _():
        through[1].wait()
        store(i - 1).wait()
        store(i).wait()


def finish(x_all, d_pre, dw_in_part, dw_down_part, dx_part):
    tokens, ff = d_pre.shape
    width = x_all.shape[1]
    n = width // 16
    return pl.pallas_call(
        finish_kernel,
        grid=(8,),
        in_specs=[
            pl.BlockSpec((tokens, n), lambda i: (0, 8 + i)),
            pl.BlockSpec((tokens, ff), lambda i: (0, 0)),
            pl.BlockSpec((n, ff), lambda i: (i, 0)),
            pl.BlockSpec((ff // 8, width), lambda i: (i, 0)),
            ANY,
        ],
        out_specs=[ANY] * 3,
        out_shape=[jax.ShapeDtypeStruct(size, BF16) for size in ((width, ff), (ff, width), dx_part.shape)],
        scratch_shapes=[pltpu.VMEM((2, n, ff), BF16), pltpu.VMEM(dx_part.shape, BF16)] + [pltpu.SemaphoreType.DMA((2,))] * 3,
        compiler_params=pltpu.CompilerParams(dimension_semantics=("arbitrary",), vmem_limit_bytes=VMEM_LIMIT),
        cost_estimate=pl.CostEstimate(flops=tokens * ff * width, bytes_accessed=140_000_000, transcendentals=0),
        name="finish",
    )(x_all, d_pre, dw_in_part, dw_down_part, dx_part)


def solution(mesh):
    def body(x, dy, pre, w_in, w_down):
        x_all, d_pre, dw_down, dx, dw_in = backward(x, dy, pre, w_in, w_down)
        dw_in, dw_down, dx = finish(x_all, d_pre, dw_in, dw_down, dx)
        return dx, dw_in, dw_down

    return jax.shard_map(
        body,
        mesh=mesh,
        in_specs=(P(("dp", "tp")), P(("dp", "tp")), P("dp", "tp"), P(None, "tp"), P("tp", None)),
        out_specs=(P(("dp", "tp")), P("dp", "tp"), P(("dp", "tp"))),
        check_vma=False,
    )
```

```python
import functools

import jax
import jax.numpy as jnp
from jax import lax
from jax.experimental import pallas as pl
from jax.experimental.pallas import tpu as pltpu
from jax.sharding import PartitionSpec as P

VMEM_LIMIT = 67_000_000
WEIGHT = (4, 2, 1)
HELD = 8
F32, BF16 = jnp.float32, jnp.bfloat16
ANY = pl.BlockSpec(memory_space=pl.ANY)


def act(pre):
    return jax.nn.gelu(pre)


def dot(a, b, dims):
    return lax.dot_general(a, b, (dims, ((), ())), preferred_element_type=F32)


NT, TN = ((1,), (1,)), ((0,), (0,))


def odd(i):
    return lax.rem(i, 2)


def rows(start, size):
    return pl.ds(pl.multiple_of(start, 16), size)


def lanes(start, size):
    return pl.ds(pl.multiple_of(start, 128), size)


class Place:
    def __init__(self):
        me = lax.axis_index("tp")
        self.chip, self.core = lax.div(me, 2), lax.rem(me, 2)
        self.step = [w * (1 - 2 * lax.rem(lax.div(self.chip, w), 2)) for w in WEIGHT]
        self.sibling = self.device(self.chip, 1 - self.core)

    def chip_at(self, r):
        return self.chip + sum(self.step[d] * r[d] for d in range(3) if isinstance(r[d], jax.Array) or r[d])

    def device(self, chip, core):
        return {"tp": 2 * chip + core}

    def across(self, d):
        if isinstance(d, int):
            return self.device(self.chip + self.step[d], self.core)
        r = (lax.div(2 - d, 2), lax.rem(d, 2), lax.div(d, 2))
        return self.device(self.chip_at(r), self.core)

    def barrier(self):
        sem = pltpu.get_barrier_semaphore()
        for peer in [self.sibling] + [self.across(d) for d in range(3)]:
            pl.semaphore_signal(sem, inc=1, device_id=peer, device_id_type=pl.DeviceIdType.MESH)
        pl.semaphore_wait(sem, 4)


def remote(src, dst, send, recv, device):
    return pltpu.make_async_remote_copy(src, dst, send, recv, device_id=device, device_id_type=pl.DeviceIdType.MESH)


def order(p):
    return p, (p + 1) % 3, (p + 2) % 3


def across(*dims):
    return tuple(int(d in dims) for d in range(3))


HERE, NEAR, FAR = [across()], [across(d) for d in range(3)], [across(*range(3))]
MIDDLE = [across(*order(d)[:2]) for d in range(3)]
OTHERS = NEAR + MIDDLE + FAR


class Gather:
    def __init__(self, place, src, dst, sems, base, halves, shares):
        self.place, self.src, self.dst, self.halves = place, src, dst, halves
        self.shard, width = src.shape
        self.size = self.shard // halves
        self.send, self.recv, self.out, self.back = (functools.partial(lambda s, i: s.at[base + i], s) for s in sems)
        tiles = width // 128
        ends = [128 * (tiles * sum(shares[:k]) // sum(shares)) for k in range(4)]
        self.columns = [pl.ds(ends[k], ends[k + 1] - ends[k]) for k in range(3)]

    def rows_of(self, r, core, h=None):
        start = (2 * self.place.chip_at(r) + core) * self.shard
        return rows(start, self.shard) if h is None else rows(start + h * self.size, self.size)

    def piece(self, p, r, core, h):
        return self.dst.at[self.rows_of(r, core, h), self.columns[p]]

    @staticmethod
    def index(p, r, h):
        return 24 * h + 8 * p + 4 * r[0] + 2 * r[1] + r[2]

    def hop(self, p, r, h):
        d = [d for d in order(p) if r[d]][-1]
        q = tuple(r[e] * (e != d) for e in range(3))
        dst = self.piece(p, q, self.place.core, h)
        src = dst if any(q) else self.src.at[pl.ds(h * self.size, self.size), self.columns[p]]
        i = self.index(p, r, h)
        return remote(src, dst, self.send(i), self.recv(i), self.place.across(d))

    def arrive(self, p, r, h):
        view, i = self.piece(p, r, self.place.core, h), self.index(p, r, h)
        remote(view, view, self.send(i), self.recv(i), self.place.sibling).wait_recv()

    def share(self, p, r, h):
        view, i = self.piece(p, r, self.place.core, h), self.index(p, r, h)
        return remote(view, view, self.out(i), self.back(i), self.place.sibling)

    def shared(self, p, r, h):
        view, i = self.piece(p, r, 1 - self.place.core, h), self.index(p, r, h)
        remote(view, view, self.out(i), self.back(i), self.place.sibling).wait_recv()

    def share_own(self):
        return remote(self.src, self.dst.at[self.rows_of((0, 0, 0), self.place.core)], self.out(0), self.back(0), self.place.sibling)

    def shared_own(self):
        view = self.dst.at[self.rows_of((0, 0, 0), 1 - self.place.core)]
        remote(view, view, self.out(0), self.back(0), self.place.sibling).wait_recv()

    def shared_all(self, chips, h):
        for p in range(3):
            for r in chips:
                self.shared(p, r, h)

    def begin(self):
        self.share_own().start()
        for h in range(self.halves):
            for k in range(3):
                for d in range(3):
                    self.hop((d - k) % 3, across(d), h).start()

    def act(self, n, h=0):
        for p in range(3):
            a, b, c = order(p)
            seq = [across(a), across(b), across(c), across(a, b), across(a, c), across(b, c), across(a, b, c)]
            follow = {0: [across(a, b), across(a, c)], 1: [across(b, c)], 3: [across(a, b, c)]}
            self.arrive(p, seq[n], h)
            for r in follow.get(n, []):
                self.hop(p, r, h).start()
            self.share(p, seq[n], h).start()

    def drain(self):
        self.share_own().wait_send()
        for h in range(self.halves):
            for p in range(3):
                for r in OTHERS:
                    self.hop(p, r, h).wait_send()
                    self.share(p, r, h).wait_send()


def backward_kernel(x, dy, pre, w_down, w_in, x_all, dy_all, d_pre, hidden, dw_down, dx, dw_in, ici, d2d,
                    send, recv, out, back, w_sem, load_sem, pre_sem, hidden_sem, store_sem, own_sem, *scatter_sems):
    place = Place()
    shard, width = dy.shape
    half = shard // 2
    tokens, ff = pre.shape
    block = ff // 4
    place.barrier()
    sems = (send, recv, out, back)
    gather_dy = Gather(place, dy, dy_all, sems, 0, 2, (22, 21, 21))
    gather_x = Gather(place, x, x_all, sems, 48, 1, (25, 22, 17))
    gather_dy.begin()
    mine = gather_dy.rows_of(HERE[0], place.core)
    batches = [(HERE, None), (NEAR, 0), (NEAR, 1), (MIDDLE, 0), (MIDDLE, 1), (FAR, None)]

    def parts(n):
        chips, h = batches[n]
        size = shard if h is None else half
        cores = (place.core, 1 - place.core)
        return [(gather_dy.rows_of(r, c, h), pl.ds(k * size, size)) for k, (r, c) in enumerate((r, c) for r in chips for c in cores)]

    def rows_in(n):
        return sum(part.size for _, part in parts(n))

    def gradient(weights, lhs, slopes, result, values):
        def load_weights(j):
            part = rows(j * block, block)
            return pltpu.make_async_copy(w_down.at[part], weights.at[part], w_sem.at[j])

        def pre_loads(n):
            return [
                pltpu.make_async_copy(pre.at[src], values.at[n % 2, part], pre_sem.at[6 * (n % 2) + k])
                for k, (src, part) in enumerate(parts(n))
            ]

        def hidden_stores(n):
            return [
                pltpu.make_async_copy(values.at[n % 2, part], hidden.at[dst], hidden_sem.at[6 * (n % 2) + k])
                for k, (dst, part) in enumerate(parts(n))
            ]

        def row_load(n, k):
            src, part = parts(n)[k]
            there = dy if (n == 0 and k == 0) else dy_all.at[src]
            return pltpu.make_async_copy(there, lhs.at[n % 2, part], load_sem.at[6 * (n % 2) + k])

        def stores(n):
            return [
                pltpu.make_async_copy(result.at[n % 2, part], d_pre.at[dst], store_sem.at[6 * (n % 2) + k])
                for k, (dst, part) in enumerate(parts(n))
            ]

        def gelu(n):
            for copy in pre_loads(n):
                copy.wait()
            slot, some = n % 2, 32 if shard >= 64 else 16

            @pl.loop(0, rows_in(n) // some)
            def _(i):
                part = rows(i * some, some)
                value, pull = jax.vjp(act, values[slot, part, :].astype(F32))
                slopes[slot, part, :] = pull(jnp.ones_like(value))[0]
                values[slot, part, :] = value.astype(BF16)

            for copy in hidden_stores(n):
                copy.start()

        first = pl.ds(0, shard)
        own_row = pltpu.make_async_copy(lhs.at[0, first], dy_all.at[mine], own_sem.at[0])
        own_x = [
            pltpu.make_async_copy(x, lhs.at[1, first], own_sem.at[1]),
            pltpu.make_async_copy(lhs.at[1, first], x_all.at[mine], own_sem.at[1]),
        ]

        def arrivals(n):
            chips, h = batches[n]
            if chips is FAR:
                return [(6, 0), (6, 1)]
            return [(k + 3 * (chips is MIDDLE), h) for k in range(3)]

        def row_loads(n, mine):
            return [row_load(n, k) for k in range(1 - mine, len(parts(n)), 2)]

        for copy in pre_loads(0):
            copy.start()
        row_load(0, 0).start()
        load_weights(0).start()
        for copy in pre_loads(1):
            copy.start()
        gelu(0)
        gather_dy.shared_own()
        row_load(0, 1).start()
        for j in range(1, 4):
            load_weights(j).start()
        own_x[0].start()
        row_load(0, 0).wait()
        own_row.start()
        row_load(0, 1).wait()

        for n in range(6):
            if n:
                for copy in row_loads(n, True) + row_loads(n, False):
                    copy.wait()
            if n < 4 and n != 1:
                for copy in hidden_stores(n):
                    copy.wait()
                for copy in pre_loads(n + 2):
                    copy.start()
            if n >= 2:
                for copy in stores(n - 2):
                    copy.wait()
            size, slot = rows_in(n), n % 2
            pieces = arrivals(n + 1) if n < 5 else []

            @pl.loop(0, 4)
            def _(j):
                if n == 0:
                    load_weights(j).wait()
                for at, (k, h) in enumerate(pieces[:2]):
                    @pl.when(j == at + 2)
                    def _():
                        gather_dy.act(k, h)
                        if at + 1 == len(pieces):
                            for copy in row_loads(n + 1, True):
                                copy.start()

                columns = lanes(j * block, block)
                d_hidden = dot(lhs[slot, :size], weights[rows(j * block, block), :], NT)
                result[slot, :size, columns] = (d_hidden * slopes[slot, :size, columns]).astype(BF16)

            for copy in stores(n):
                copy.start()
            if n == 0:
                own_x[0].wait()
                own_x[1].start()
                gelu(1)
                own_x[1].wait()
                for copy in hidden_stores(1):
                    copy.wait()
                for copy in pre_loads(3):
                    copy.start()
            if n == 3:
                gather_x.begin()
            if n < 4:
                gelu(n + 2)
            for k, h in pieces[2:]:
                gather_dy.act(k, h)
            if n < 5:
                if n == 1:
                    own_row.wait()
                for copy in row_loads(n + 1, True) if pieces[2:] else []:
                    copy.start()
                chips, h = batches[n + 1]
                for h in (0, 1) if h is None else (h,):
                    gather_dy.shared_all(chips, h)
                for copy in row_loads(n + 1, False):
                    copy.start()
        for n in (4, 5):
            for copy in hidden_stores(n) + stores(n):
                copy.wait()

    pl.run_scoped(
        gradient,
        pltpu.VMEM((ff, width), BF16),
        pltpu.VMEM((2, 6 * half, width), BF16),
        pltpu.VMEM((2, 6 * half, ff), F32),
        pltpu.VMEM((2, 6 * half, ff), BF16),
        pltpu.VMEM((2, 6 * half, ff), BF16),
    )

    tm, tn = ff // 2, width // 8

    def down(loads):
        def product(h_ref, dy_ref, o_ref):
            at = pl.program_id(0) * pl.num_programs(1) + pl.program_id(1)
            group, place_in = lax.div(at, 3), lax.rem(at, 3)

            @pl.when(place_in == 0)
            def _():
                for n in range(5):
                    @pl.when(group == n + 1)
                    def _():
                        gather_x.act(n)

            @pl.when(place_in == 2)
            def _():
                for n, some in enumerate(loads):
                    @pl.when(group == n)
                    def _():
                        for copy in some:
                            copy.start()

            o_ref[...] = dot(h_ref[...], dy_ref[...], TN).astype(BF16)

        pltpu.emit_pipeline(
            product,
            grid=(2, 8),
            in_specs=[pl.BlockSpec((tokens, tm), lambda i, j: (0, i)), pl.BlockSpec((tokens, tn), lambda i, j: (0, j))],
            out_specs=[pl.BlockSpec((tm, tn), lambda i, j: (i, j))],
        )(hidden, dy_all, dw_down)

    def rest(lhs, weights, right):
        scatter(place, gather_x, down, x_all, d_pre, w_in, dx, dw_in, ici, d2d, lhs, weights, right, *scatter_sems)

    pl.run_scoped(
        rest, pltpu.VMEM((3, 8 * shard, ff), BF16), pltpu.VMEM((width // 4, ff), BF16), pltpu.VMEM((tokens, ff), BF16)
    )
    gather_dy.drain()
    gather_x.drain()


def scatter(place, gather_x, down, x_all, d_pre, w_in, dx, dw_in, ici, d2d, lhs_buf, weights, right,
            ici_send, ici_recv, d2d_send, d2d_recv, w_sem, load_sem, stage_sem, dx_sem, x_sem, dw_sem, right_sem):
    core = place.core
    shard, width = dx.shape
    tokens, ff = d_pre.shape
    n1, n2 = width // 16, width // 8

    def pick(i, group):
        k = lax.div(i, 3 * group)
        p = (1 - k) * lax.rem(i, 3) + k * odd(i)
        t = (1 - k) * lax.div(i, 3) + k * (group + lax.div(i - 3 * group, 2))
        return p, t

    def unpick(p, t, group):
        k = lax.div(t, group)
        return (1 - k) * (3 * t + p) + k * (3 * group + 2 * (t - group) + p)

    def turn(p, k):
        return lax.rem(p + k, 3)

    def narrow(i):
        p, t = pick(i, 4)
        return p, t, p * (3 * n2) + t * n1

    def wide(i):
        p, t = pick(i, 2)
        return p, t, p * (3 * n2) + t * n2

    def narrow_weights(i):
        slot = lax.rem(i, 4)
        return [pltpu.make_async_copy(w_in.at[rows(narrow(i)[2], n1)], weights.at[rows(slot * n1, n1)], w_sem.at[slot])]

    def wide_weights(i):
        start, slot = wide(i)[2], odd(i)
        return [
            pltpu.make_async_copy(w_in.at[rows(start + h * n1, n1)], weights.at[rows(slot * n2 + h * n1, n1)], w_sem.at[2 * slot + h])
            for h in (0, 1)
        ]

    def go(copies):
        for copy in copies:
            copy.start()

    def wait(copies):
        for copy in copies:
            copy.wait()

    def lhs_loads(p, first, chips, base):
        loads = []
        for half, c in enumerate((1 - core, core)):
            for k, r in enumerate(chips):
                src = d_pre.at[rows((2 * place.chip_at(r) + c) * shard, shard)]
                n = half * len(chips) + k
                loads.append(pltpu.make_async_copy(src, lhs_buf.at[p, pl.ds(first + n * shard, shard)], load_sem.at[base + n]))
        return loads

    def exchange(k, i, count, columns, base, part):
        region = (0, 4, 6)[k]
        dst = d2d.at[pl.ds(region * shard, count * shard), columns]
        return remote(part, dst, d2d_send.at[base + i], d2d_recv.at[base + i], place.sibling)

    def onward(k, i, count, p, columns, base, part):
        region = (0, 4, 6)[k]
        dst = ici.at[pl.ds(region * shard, count * shard), columns]
        return remote(part, dst, ici_send.at[base + i], ici_recv.at[base + i], place.across(turn(p, k)))

    def stage_chips(p, k):
        a, b, c = order(p)
        tail = [(0, 0), (0, 1), (1, 0), (1, 1)]
        if k == 0:
            return [tuple(across(a)[d] + s * across(b)[d] + t * across(c)[d] for d in range(3)) for s, t in tail]
        if k == 1:
            return [across(b), across(b, c)]
        return [across(c)] + HERE

    def stage(k, items, out, between, prepare=None, filler=None, keep=None, lag_b=1, lag_c=3):
        count, moved = (4, 2, 1)[k], (4, 2, 2)[k]
        size = n1 if k == 0 else n2
        base = (0, 16, 24)[k]
        locate = narrow if k == 0 else wide
        slots, n_term, n_staged = lag_c, 2, lag_c
        n_in = 1 + k
        from_ici = [(), ((2, 4),), ((1, 2), (5, 6))][k]

        def body(acc, term, staged):
            def columns(i):
                return lanes(locate(i)[2], size)

            def sources(i):
                region = (0, 4, 6)[k]
                views = [d2d.at[pl.ds(region * shard, count * shard), columns(i)]]
                views += [ici.at[pl.ds(a * shard, (b - a) * shard), columns(i)] for a, b in from_ici]
                slot = lax.rem(i, n_staged)
                return [
                    pltpu.make_async_copy(view, staged.at[slot, n], stage_sem.at[slot * n_in + n]) for n, view in enumerate(views)
                ]

            def send(i):
                return exchange(k, i, moved, columns(i), base, term.at[lax.rem(i, n_term)])

            def leave(i):
                return onward(k, i, count, locate(i)[0], columns(i), base, out.at[i])

            def fetch(j):
                view = d2d.at[pl.ds(0, moved * shard), columns(j)]
                remote(view, view, d2d_send.at[base + j], d2d_recv.at[base + j], place.sibling).wait_recv()
                p, t, start = locate(j)
                if k == 1:
                    for h in range(2):
                        n = unpick(p, 2 * t + h, 4)
                        view = ici.at[pl.ds(0, 4 * shard), lanes(start + h * n1, n1)]
                        remote(view, view, ici_send.at[n], ici_recv.at[n], place.sibling).wait_recv()
                elif k == 2:
                    n = 16 + j
                    view = ici.at[pl.ds(0, 2 * shard), columns(j)]
                    remote(view, view, ici_send.at[n], ici_recv.at[n], place.sibling).wait_recv()
                go(sources(j))

            def add(j, slot, there):
                total = acc[slot]
                for n in range(n_in):
                    total = total + staged[there, n].astype(F32)
                out[j] = total.astype(BF16)

            @pl.loop(0, items)
            def _(i):
                p, _, start = locate(i)
                slot = lax.rem(i, slots)
                wait(narrow_weights(i) if k == 0 else wide_weights(i))
                if prepare is not None:
                    prepare(i)

                @pl.when(i >= n_term)
                def _():
                    send(i - n_term).wait_send()

                @pl.when(i >= lag_c)
                def _():
                    wait(sources(i - lag_c))

                add(lax.max(i - lag_c, 0), slot, lax.rem(i, n_staged))
                if k == 0:
                    w = weights[rows(lax.rem(i, 4) * n1, n1), :]
                else:
                    w = weights[rows(odd(i) * n2, n2), :]
                value = dot(lhs_buf[p, pl.ds((k // 2) * 4 * shard, 2 * moved * shard)], w, NT)
                term[lax.rem(i, n_term)] = value[: moved * shard].astype(BF16)
                acc[slot] = value[moved * shard : (moved + count) * shard]
                if k == 2:
                    keep[i] = value[(moved + count) * shard :]
                send(i).start()

                @pl.when(i >= lag_c)
                def _():
                    leave(i - lag_c).start()

                if k == 0:
                    @pl.when(i + 4 < items)
                    def _():
                        go(narrow_weights(i + 4))

                    @pl.when(i == items - 3)
                    def _():
                        go(wide_weights(0))

                    @pl.when(i == items - 1)
                    def _():
                        go(wide_weights(1))
                elif k == 1:
                    go(wide_weights(lax.rem(i + 2, items)))
                else:
                    @pl.when(i + 2 < items)
                    def _():
                        go(wide_weights(i + 2))

                if filler is not None:
                    filler(i)

                @pl.when(i >= lag_b)
                def _():
                    fetch(i - lag_b)

            def close(j):
                wait(sources(j))
                add(j, j % slots, j % n_staged)
                leave(j).start()

            def midway():
                fetch(items - 1)
                close(items - 2)

            close(items - 3)
            between(midway)
            close(items - 1)

            for i in range(items - n_term, items):
                send(i).wait_send()

        pl.run_scoped(
            body,
            pltpu.VMEM((slots, count * shard, size), F32),
            pltpu.VMEM((n_term, moved * shard, size), BF16),
            pltpu.VMEM((n_staged, n_in, count * shard, size), BF16),
        )

    loads1 = [lhs_loads(p, 0, stage_chips(p, 0), 8 * p) for p in range(3)]
    loads2 = [lhs_loads(p, 0, stage_chips(p, 1), 24 + 4 * p) for p in range(3)]
    loads3 = [lhs_loads(p, 4 * shard, stage_chips(p, 2), 36 + 4 * p) for p in range(3)]
    right_load = pltpu.make_async_copy(d_pre, right, right_sem.at[0])
    down([[copy for i in range(4) for copy in narrow_weights(i)], *loads1, [right_load]])
    for some in loads1:
        wait(some)

    def main(out2, x_buf, dw_buf):
        def x_load(i):
            slot = odd(i)
            return pltpu.make_async_copy(x_all.at[:, lanes(i * n1, n1)], x_buf.at[slot], x_sem.at[slot])

        def dw_store(i):
            slot = odd(i)
            return pltpu.make_async_copy(dw_buf.at[slot], dw_in.at[rows(i * n1, n1)], dw_sem.at[slot])

        def tiles(a, b, midway=None):
            @pl.loop(a, b)
            def _(i):
                slot = odd(i)
                x_load(i).wait()

                @pl.when(i >= 2)
                def _():
                    dw_store(i - 2).wait()

                @pl.loop(0, 2)
                def _(h):
                    if midway is not None:
                        @pl.when(h == 1)
                        def _():
                            midway()

                    part = lanes(h * (ff // 2), ff // 2)
                    dw_buf[slot, :, part] = dot(x_buf[slot], right[:, part], TN).astype(BF16)

                dw_store(i).start()

                @pl.when(i + 2 < HELD)
                def _():
                    x_load(i + 2).start()

        def fill2(i):
            turn, on = lax.div(i + 1, 3), lax.div(lax.rem(i, 3), 2)
            tiles(turn, turn + on * turn)

        def fill3(i):
            turn, on = lax.div(i + 1, 3), lax.div(lax.rem(i, 3), 2)
            tiles(4 + turn, 4 + turn + on)

        def early(out1):
            def prepare(i):
                for n in (5, 6):
                    @pl.when(i == 6 * n - 27)
                    def _():
                        gather_x.act(n)

                @pl.when(i == 12)
                def _():
                    gather_x.shared_own()
                    gather_x.shared_all(OTHERS, 0)
                    x_load(0).start()
                    x_load(1).start()
                    go(loads2[2] + loads3[2])

                @pl.when(i == 15)
                def _():
                    go(loads2[0] + loads3[0])

            def between(midway):
                go(loads2[1] + loads3[1])
                right_load.wait()
                tiles(0, 1, midway)

            def prepare2(i):
                for p in range(3):
                    @pl.when(i == p)
                    def _():
                        wait(loads2[p] + loads3[p])

            stage(0, 16, out1, between, prepare=prepare)
            stage(1, 8, out2, lambda midway: tiles(4, 5, midway), prepare=prepare2, filler=fill2)
            for i in range(16):
                onward(0, i, 4, narrow(i)[0], lanes(narrow(i)[2], n1), 0, out1.at[i]).wait_send()

        pl.run_scoped(early, pltpu.VMEM((16, 4 * shard, n1), BF16))

        def late(out3, keep):
            stage(2, 8, out3, lambda midway: tiles(7, 8, midway), filler=fill3, keep=keep)
            pl.run_scoped(functools.partial(final, keep), pltpu.VMEM((8, shard, n2), BF16), pltpu.VMEM((4, 4, shard, n2), BF16))
            for i in range(8):
                onward(1, i, 2, wide(i)[0], lanes(wide(i)[2], n2), 16, out2.at[i]).wait_send()
                onward(2, i, 1, wide(i)[0], lanes(wide(i)[2], n2), 24, out3.at[i]).wait_send()

        def final(keep, out4, staged):
            def columns(i):
                return lanes(wide(i)[2], n2)

            def sources(i):
                views = [d2d.at[pl.ds(7 * shard, shard), columns(i)]]
                views += [ici.at[pl.ds(n * shard, shard), columns(i)] for n in (0, 4, 6)]
                slot = lax.rem(i, 4)
                return [pltpu.make_async_copy(view, staged.at[slot, n], stage_sem.at[4 * slot + n]) for n, view in enumerate(views)]

            def store(i):
                return pltpu.make_async_copy(out4.at[i], dx.at[:, columns(i)], dx_sem.at[i])

            @pl.loop(0, 8 + 3)
            def _(i):
                @pl.when(i >= 3)
                def _():
                    j = i - 3
                    wait(sources(j))
                    total = keep[j]
                    for n in range(4):
                        total = total + staged[lax.rem(j, 4), n].astype(F32)
                    out4[j] = total.astype(BF16)
                    store(j).start()

                @pl.when(i < 8)
                def _():
                    view = ici.at[pl.ds(0, shard), columns(i)]
                    remote(view, view, ici_send.at[24 + i], ici_recv.at[24 + i], place.sibling).wait_recv()
                    go(sources(i))

            dw_store(HELD - 2).wait()
            dw_store(HELD - 1).wait()
            for i in range(8):
                store(i).wait()

        pl.run_scoped(late, pltpu.VMEM((8, shard, n2), BF16), pltpu.VMEM((8, shard, n2), F32))

    pl.run_scoped(
        main,
        pltpu.VMEM((8, 2 * shard, n2), BF16),
        pltpu.VMEM((2, tokens, n1), BF16),
        pltpu.VMEM((2, n1, ff), BF16),
    )


def backward(x, dy, pre, w_in, w_down):
    shard, width = dy.shape
    tokens, ff = pre.shape
    dma = pltpu.SemaphoreType.DMA

    def shape(*size):
        return jax.ShapeDtypeStruct(size, BF16)

    x_all, _, d_pre, _, dw_down, dx, dw_in, _, _ = pl.pallas_call(
        backward_kernel,
        in_specs=[ANY] * 5,
        out_specs=[ANY] * 9,
        out_shape=[
            shape(tokens, width),
            shape(tokens, width),
            shape(tokens, ff),
            shape(tokens, ff),
            shape(ff, width),
            shape(shard, width),
            shape(HELD * width // 16, ff),
            shape(7 * shard, width),
            shape(8 * shard, width),
        ],
        scratch_shapes=[dma((n,)) for n in [72] * 4 + [4] + [12] * 4 + [2] + [32] * 4 + [4, 48, 16, 8, 2, 2, 1]],
        compiler_params=pltpu.CompilerParams(collective_id=0, has_side_effects=True, vmem_limit_bytes=VMEM_LIMIT),
        cost_estimate=pl.CostEstimate(flops=7 * tokens * ff * width, bytes_accessed=800_000_000, transcendentals=tokens * ff),
        name="backward",
    )(x, dy, pre, w_down, w_in)
    return x_all, d_pre, dw_down, dx, dw_in


def finish_kernel(x_ref, d_pre_ref, part_ref, down_ref, dx_part, dw_in, dw_down, dx, buf, dx_buf, copy_sem, buf_sem, dx_sem):
    i = pl.program_id(0)
    n, ff = part_ref.shape
    count = pl.num_programs(0)
    slot = lax.rem(i, 2)
    copies = [
        pltpu.make_async_copy(part_ref, dw_in.at[rows(i * n, n)], copy_sem.at[0]),
        pltpu.make_async_copy(down_ref, dw_down.at[rows(i * down_ref.shape[0], down_ref.shape[0])], copy_sem.at[1]),
    ]

    def store(i):
        slot = lax.rem(i, 2)
        return pltpu.make_async_copy(buf.at[slot], dw_in.at[rows((count + i) * n, n)], buf_sem.at[slot])

    for copy in copies:
        copy.start()

    through = [pltpu.make_async_copy(dx_part, dx_buf, dx_sem.at[0]), pltpu.make_async_copy(dx_buf, dx, dx_sem.at[1])]

    @pl.when(i == 0)
    def _():
        through[0].start()

    @pl.when(i == 1)
    def _():
        through[0].wait()
        through[1].start()

    @pl.when(i >= 2)
    def _():
        store(i - 2).wait()

    @pl.loop(0, 2)
    def _(h):
        half = lanes(h * (ff // 2), ff // 2)
        buf[slot, :, half] = dot(x_ref[...], d_pre_ref[:, half], TN).astype(BF16)

    store(i).start()
    for copy in copies:
        copy.wait()

    @pl.when(i == count - 1)
    def _():
        through[1].wait()
        store(i - 1).wait()
        store(i).wait()


def finish(x_all, d_pre, dw_in_part, dw_down_part, dx_part):
    tokens, ff = d_pre.shape
    width = x_all.shape[1]
    n = width // 16
    return pl.pallas_call(
        finish_kernel,
        grid=(8,),
        in_specs=[
            pl.BlockSpec((tokens, n), lambda i: (0, 8 + i)),
            pl.BlockSpec((tokens, ff), lambda i: (0, 0)),
            pl.BlockSpec((n, ff), lambda i: (i, 0)),
            pl.BlockSpec((ff // 8, width), lambda i: (i, 0)),
            ANY,
        ],
        out_specs=[ANY] * 3,
        out_shape=[jax.ShapeDtypeStruct(size, BF16) for size in ((width, ff), (ff, width), dx_part.shape)],
        scratch_shapes=[pltpu.VMEM((2, n, ff), BF16), pltpu.VMEM(dx_part.shape, BF16)] + [pltpu.SemaphoreType.DMA((2,))] * 3,
        compiler_params=pltpu.CompilerParams(dimension_semantics=("arbitrary",), vmem_limit_bytes=VMEM_LIMIT),
        cost_estimate=pl.CostEstimate(flops=tokens * ff * width, bytes_accessed=140_000_000, transcendentals=0),
        name="finish",
    )(x_all, d_pre, dw_in_part, dw_down_part, dx_part)


def solution(mesh):
    def body(x, dy, pre, w_in, w_down):
        x_all, d_pre, dw_down, dx, dw_in = backward(x, dy, pre, w_in, w_down)
        dw_in, dw_down, dx = finish(x_all, d_pre, dw_in, dw_down, dx)
        return dx, dw_in, dw_down

    return jax.shard_map(
        body,
        mesh=mesh,
        in_specs=(P(("dp", "tp")), P(("dp", "tp")), P("dp", "tp"), P(None, "tp"), P("tp", None)),
        out_specs=(P(("dp", "tp")), P("dp", "tp"), P(("dp", "tp"))),
        check_vma=False,
    )
```
